16 devices in a mesh: dp: 4 (over z, y), tp: 4 (over x, core).
Axes of the slice: x: 2, y: 2, z: 2, core: 2. Of those that a mesh axis runs over, the one named last changes fastest.
Arguments:
- hidden: bfloat16 [128, 4096], P('dp'), parts along dimension 0
- cache_len: int32 [128], P('dp'), parts along dimension 0
- lin_state: float32 [128, 32, 128, 128], P('dp', 'tp'), parts along dimension 0
- k_cache: bfloat16 [128, 8, 512, 128], P('dp', 'tp'), parts along dimension 0
- v_cache: bfloat16 [128, 8, 512, 128], P('dp', 'tp'), parts along dimension 0
- norm_first: float32 [4096], replicated
- w_qkv: bfloat16 [4096, 3, 32, 128], P(None, None, 'tp')
- w_gate: bfloat16 [4096, 32, 128], P(None, 'tp')
- slopes: float32 [32], P('tp')
- out_norm: float32 [32, 128], P('tp')
- w_out_lin: bfloat16 [32, 128, 4096], P('tp')
- norm_second: float32 [4096], replicated
- w_attn: bfloat16 [4096, 8, 6, 128], P(None, 'tp')
- w_out_attn: bfloat16 [32, 128, 4096], P('tp')
- mix_alpha: float32 [2], replicated
- mix_beta: float32 [2], replicated
Outputs:
- output 1: bfloat16 [128, 4096], P('dp'), parts along dimension 0
- output 2: float32 [128, 32, 128, 128], P('dp', 'tp'), parts along dimension 0
- output 3: bfloat16 [128, 8, 512, 128], P('dp', 'tp'), parts along dimension 0
- output 4: bfloat16 [128, 8, 512, 128], P('dp', 'tp'), parts along dimension 0
There are 4 independent parts. The reference program is written for one: setup_inputs(seed, part) draws one part's arguments, and reference() takes and returns one part's arrays. A program takes and returns all parts, laid end to end along the dimension named above; an argument that names none is the same for every part.
All inputs are finite; a program needn't handle non-finite values.
Results may differ from the reference program's by a relative error of at most 0.0114328.
Values sent between devices are 32-bit elements.
A program may use at most 1 GiB of HBM per device.

```python
import math
import jax
import jax.numpy as jnp
from jax import lax

D = 4096
HEADS = 32
KV_HEADS = 8
HEAD = 128
BATCH = 32
TMAX = 512

GROUP = HEADS // KV_HEADS
WIDTH = HEADS * HEAD
LEN_MIN = TMAX // 16
EPS = 1e-5
ROPE_BASE = 10000000.0


def setup_inputs(seed: int = 0, part: int = 0) -> dict:
    shared_keys = jax.random.split(jax.random.key(seed), 11)
    own_keys = jax.random.split(jax.random.fold_in(jax.random.key(seed), part), 8)
    hidden = jax.random.normal(own_keys[0], (BATCH, D), jnp.float32).astype(jnp.bfloat16)
    cache_len = jax.random.randint(own_keys[1], (BATCH,), LEN_MIN, TMAX, jnp.int32)
    cache_len = cache_len.at[0].set(TMAX - 1).at[1].set(LEN_MIN)
    head_scale = jnp.exp(jax.random.uniform(own_keys[2], (BATCH, HEADS, 1, 1), jnp.float32, -1.0, 1.0))
    lin_state = 2.0 * head_scale * jax.random.normal(own_keys[3], (BATCH, HEADS, HEAD, HEAD), jnp.float32)
    key_scale = math.sqrt(math.log(TMAX / 32.0))
    k_cache = (key_scale * jax.random.normal(own_keys[4], (BATCH, KV_HEADS, TMAX, HEAD), jnp.float32)).astype(jnp.bfloat16)
    pos_ramp = (2.0 * jnp.arange(TMAX, dtype=jnp.float32) / TMAX - 1.0)[None, None, :, None]
    v_base = jax.random.normal(own_keys[5], (BATCH, KV_HEADS, 1, HEAD), jnp.float32)
    v_slope = jax.random.normal(own_keys[6], (BATCH, KV_HEADS, 1, HEAD), jnp.float32)
    v_noise = jax.random.normal(own_keys[7], (BATCH, KV_HEADS, TMAX, HEAD), jnp.float32)
    v_cache = (0.5 * v_base + 0.5 * v_slope * pos_ramp + v_noise).astype(jnp.bfloat16)
    norm_first = jax.random.uniform(shared_keys[0], (D,), jnp.float32, 0.5, 1.5)
    w_qkv = (jax.random.normal(shared_keys[1], (D, 3, HEADS, HEAD), jnp.float32) * D ** -0.5).astype(jnp.bfloat16)
    w_gate = (jax.random.normal(shared_keys[2], (D, HEADS, HEAD), jnp.float32) * D ** -0.5).astype(jnp.bfloat16)
    slopes = jax.random.uniform(shared_keys[3], (HEADS,), jnp.float32, 0.02, 0.3)
    out_norm = jax.random.uniform(shared_keys[4], (HEADS, HEAD), jnp.float32, 0.5, 1.5)
    w_out_lin = (jax.random.normal(shared_keys[5], (HEADS, HEAD, D), jnp.float32) * WIDTH ** -0.5).astype(jnp.bfloat16)
    norm_second = jax.random.uniform(shared_keys[6], (D,), jnp.float32, 0.5, 1.5)
    w_attn = (jax.random.normal(shared_keys[7], (D, KV_HEADS, GROUP + 2, HEAD), jnp.float32) * D ** -0.5).astype(jnp.bfloat16)
    w_out_attn = (jax.random.normal(shared_keys[8], (HEADS, HEAD, D), jnp.float32) * WIDTH ** -0.5).astype(jnp.bfloat16)
    mix_alpha = jax.random.uniform(shared_keys[9], (2,), jnp.float32, 0.5, 1.5)
    mix_beta = jax.random.uniform(shared_keys[10], (2,), jnp.float32, 0.5, 1.5)
    return dict(hidden=hidden, cache_len=cache_len, lin_state=lin_state, k_cache=k_cache, v_cache=v_cache,
                norm_first=norm_first, w_qkv=w_qkv, w_gate=w_gate, slopes=slopes, out_norm=out_norm,
                w_out_lin=w_out_lin, norm_second=norm_second, w_attn=w_attn, w_out_attn=w_out_attn,
                mix_alpha=mix_alpha, mix_beta=mix_beta)


def rms_norm(values, gain_vec):
    wide_vals = values.astype(jnp.float32)
    mean_sq = jnp.mean(wide_vals * wide_vals, axis=-1, keepdims=True)
    return wide_vals * lax.rsqrt(mean_sq + EPS) * gain_vec


def rotary(values, positions):
    rot_dim = values.shape[-1] // 2
    half_dim = rot_dim // 2
    inv_freq = ROPE_BASE ** (-2.0 * jnp.arange(half_dim, dtype=jnp.float32) / rot_dim)
    angles = positions.astype(jnp.float32)[:, None] * inv_freq[None, :]
    cosine = jnp.cos(angles)[:, None, None, :]
    sine_val = jnp.sin(angles)[:, None, None, :]
    rot_first = values[..., :half_dim]
    rot_second = values[..., half_dim:rot_dim]
    return jnp.concatenate([rot_first * cosine - rot_second * sine_val,
                            rot_second * cosine + rot_first * sine_val,
                            values[..., rot_dim:]], axis=-1)


def lightning_layer(h_first, lin_state, w_qkv, w_gate, slopes, out_norm, w_out_lin):
    proj_lin = jnp.dot(h_first, w_qkv.reshape(D, 3 * WIDTH), preferred_element_type=jnp.float32)
    proj_lin = jax.nn.silu(proj_lin).astype(jnp.bfloat16).astype(jnp.float32).reshape(BATCH, 3, HEADS, HEAD)
    query_lin = proj_lin[:, 0]
    key_lin = proj_lin[:, 1]
    value_lin = proj_lin[:, 2]
    decay_rate = jnp.exp(-slopes)[None, :, None, None]
    state_out = decay_rate * lin_state + jnp.einsum('bhk,bhv->bhkv', key_lin, value_lin)
    lin_attn = jnp.einsum('bhk,bhkv->bhv', query_lin, state_out)
    mean_sq = jnp.mean(lin_attn * lin_attn, axis=(1, 2), keepdims=True)
    normed = (lin_attn * lax.rsqrt(mean_sq + EPS) * out_norm).reshape(BATCH, WIDTH)
    gate_val = jax.nn.sigmoid(jnp.dot(h_first, w_gate.reshape(D, WIDTH), preferred_element_type=jnp.float32))
    gated_out = (normed * gate_val).astype(jnp.bfloat16)
    lin_out = jnp.dot(gated_out, w_out_lin.reshape(WIDTH, D), preferred_element_type=jnp.float32)
    return lin_out, state_out


def softmax_layer(h_second, cache_len, k_cache, v_cache, w_attn, w_out_attn):
    proj_attn = jnp.dot(h_second, w_attn.reshape(D, KV_HEADS * (GROUP + 2) * HEAD), preferred_element_type=jnp.float32)
    proj_attn = proj_attn.reshape(BATCH, KV_HEADS, GROUP + 2, HEAD)
    turned = rotary(proj_attn[:, :, :GROUP + 1], cache_len).astype(jnp.bfloat16)
    query_new = turned[:, :, :GROUP]
    key_new = turned[:, :, GROUP]
    value_new = proj_attn[:, :, GROUP + 1].astype(jnp.bfloat16)
    positions = jnp.arange(TMAX, dtype=jnp.int32)
    write_mask = (positions[None, :] == cache_len[:, None])[:, None, :, None]
    k_out = jnp.where(write_mask, key_new[:, :, None, :], k_cache)
    v_out = jnp.where(write_mask, value_new[:, :, None, :], v_cache)

    def one_row(row_args):
        query_row, key_row, value_row, length = row_args
        scores = jnp.einsum('kgc,ktc->kgt', query_row.astype(jnp.float32), key_row.astype(jnp.float32)) * HEAD ** -0.5
        scores = jnp.where(positions[None, None, :] <= length, scores, -jnp.inf)
        probs_row = jax.nn.softmax(scores, axis=-1).astype(jnp.bfloat16)
        return jnp.einsum('kgt,ktc->kgc', probs_row.astype(jnp.float32), value_row.astype(jnp.float32)).astype(jnp.bfloat16)

    attn_rows = lax.map(one_row, (query_new, k_out, v_out, cache_len))
    attn_out = jnp.dot(attn_rows.reshape(BATCH, WIDTH), w_out_attn.reshape(WIDTH, D), preferred_element_type=jnp.float32)
    return attn_out, k_out, v_out


def reference(hidden, cache_len, lin_state, k_cache, v_cache, norm_first, w_qkv, w_gate, slopes, out_norm,
              w_out_lin, norm_second, w_attn, w_out_attn, mix_alpha, mix_beta):
    h_first = rms_norm(hidden, norm_first).astype(jnp.bfloat16)
    lin_out, state_out = lightning_layer(h_first, lin_state, w_qkv, w_gate, slopes, out_norm, w_out_lin)
    mid_hidden = (mix_alpha[0] * h_first.astype(jnp.float32) + mix_beta[0] * lin_out).astype(jnp.bfloat16)
    h_second = rms_norm(mid_hidden, norm_second).astype(jnp.bfloat16)
    attn_out, k_out, v_out = softmax_layer(h_second, cache_len, k_cache, v_cache, w_attn, w_out_attn)
    hidden_out = (mix_alpha[1] * h_second.astype(jnp.float32) + mix_beta[1] * attn_out).astype(jnp.bfloat16)
    return hidden_out, state_out, k_out, v_out
```

```python
import functools
import math

import jax
import jax.numpy as jnp
from jax import lax
from jax.experimental import pallas as pl
from jax.experimental.pallas import tpu as pltpu
from jax.sharding import PartitionSpec as P

EPS = 1e-5
ROPE_BASE = 10000000.0
MESH = pl.DeviceIdType.MESH
F32 = jnp.float32
BF16 = jnp.bfloat16
VMEM_LIMIT = 62 * 1024 * 1024

B = 32
D = 4096
HL = 8
HD = 128
KV = 2
GQ = 4
T = 512
NC = D // HD

DCH = 128
STEPS = D // DCH
RING = 8


def any_spec():
    return pl.BlockSpec(memory_space=pl.ANY)


def vmem_spec():
    return pl.BlockSpec(memory_space=pltpu.VMEM)


def smem_spec():
    return pl.BlockSpec(memory_space=pltpu.SMEM)


def dot(a, b):
    return jnp.dot(a, b, preferred_element_type=F32)


def lightning_kernel(hid_ref, g1_ref, slopes_ref, onorm_ref, state_ref, wqkv_ref, wgate_ref,
                     sout_ref, og_ref, ss_ref, h1_ref,
                     wbuf, sbuf, ebuf, lbuf, acc, qk_t, v_s, o_s, wsem, ssem, osem):
    def w_copies(step, slot):
        rows = pl.ds(step * DCH, DCH)
        out = [pltpu.make_async_copy(wqkv_ref.at[rows, c], wbuf.at[slot, c], wsem.at[slot, c]) for c in range(3)]
        out.append(pltpu.make_async_copy(wgate_ref.at[rows], wbuf.at[slot, 3], wsem.at[slot, 3]))
        return out

    def s_copy(b):
        return pltpu.make_async_copy(state_ref.at[b], sbuf.at[b], ssem.at[b])

    def o_copy(b):
        return pltpu.make_async_copy(sbuf.at[b], sout_ref.at[b], osem.at[b])

    for i in range(RING):
        for cp in w_copies(i, i):
            cp.start()

    sq = jnp.zeros((B, HD), F32)
    for c in range(NC):
        x = hid_ref[:, c * HD:(c + 1) * HD].astype(F32)
        sq = sq + x * x
    inv = lax.rsqrt(jnp.sum(sq, axis=1, keepdims=True) / D + EPS)
    rr = lax.broadcasted_iota(jnp.int32, (HD, 256), 1)
    dd = lax.broadcasted_iota(jnp.int32, (HD, 256), 0)
    for c in range(NC):
        x = hid_ref[:, c * HD:(c + 1) * HD].astype(F32)
        h1 = (x * inv * g1_ref[c:c + 1, :]).astype(BF16)
        h1_ref[:, c * HD:(c + 1) * HD] = h1
        lbuf[c * B:(c + 1) * B, 0:HD] = h1
    for n in range(4):
        spread = jnp.where(rr // 8 + 32 * n == dd, 1.0, 0.0).astype(BF16)
        for c in range(NC // 8):
            e = dot(lbuf[c * 256:(c + 1) * 256, 0:HD], spread).astype(BF16)
            for k in range(8):
                ebuf[c * 8 + k, :, n * 256:(n + 1) * 256] = e[k * B:(k + 1) * B, :]

    acc[...] = jnp.zeros_like(acc)
    lane = lax.broadcasted_iota(jnp.int32, (B, 1024), 1) % 8

    def step_fn(i, carry):
        slot = lax.rem(i, RING)
        s_copy(i).start()
        e = ebuf[i]
        for h in range(HL):
            keep = jnp.where(lane == h, 1.0, 0.0).astype(BF16)
            lbuf[h * B:(h + 1) * B, :] = e * keep
        for cp in w_copies(i, slot):
            cp.wait()
        left = lbuf[0:HL * B, :]
        for pair in range(2):
            right = jnp.concatenate([wbuf[slot, 2 * pair].reshape(DCH * HL, HD),
                                     wbuf[slot, 2 * pair + 1].reshape(DCH * HL, HD)], axis=1)
            acc[pair] += dot(left, right)

        @pl.when(i + RING < STEPS)
        def _():
            for cp in w_copies(i + RING, slot):
                cp.start()
        return carry

    lax.fori_loop(0, STEPS, step_fn, 0)

    for h in range(HL):
        rows = slice(h * B, (h + 1) * B)
        q = jax.nn.silu(acc[0, rows, 0:HD]).astype(BF16)
        k = jax.nn.silu(acc[0, rows, HD:2 * HD]).astype(BF16)
        v = jax.nn.silu(acc[1, rows, 0:HD]).astype(BF16)
        qk = jnp.concatenate([k, q], axis=0).astype(F32)
        qk_t[h] = jnp.transpose(qk).astype(BF16)
        v_s[h] = v

    def row_fn(b, carry):
        s_copy(b).wait()
        row_i = lax.broadcasted_iota(jnp.int32, (B, HD), 0)
        hit = row_i == b
        ones = jnp.where(hit, 1.0, 0.0).astype(BF16)
        zero = jnp.zeros((B, HD), BF16)
        for h in range(HL):
            top = jnp.concatenate([v_s[h] * ones, zero], axis=1)
            bot = jnp.concatenate([zero, ones], axis=1)
            prod = dot(qk_t[h], jnp.concatenate([top, bot], axis=0))
            decay = jnp.exp(jnp.full((1, HD), -slopes_ref[h], F32))
            new = decay * sbuf[b, h] + prod[:, 0:HD]
            sbuf[b, h] = new
            o_s[b, h:h + 1, :] = jnp.sum(prod[:, HD:] * new, axis=0, keepdims=True)
        o_copy(b).start()
        return carry

    lax.fori_loop(0, B, row_fn, 0)

    ss = jnp.zeros((B, HD), F32)
    for h in range(HL):
        o = o_s[:, h, :]
        ss = ss + o * o
        gate = jax.nn.sigmoid(acc[1, h * B:(h + 1) * B, HD:2 * HD])
        og_ref[:, h * HD:(h + 1) * HD] = o * onorm_ref[h:h + 1, :] * gate
    ss_ref[...] = jnp.broadcast_to(jnp.sum(ss, axis=1, keepdims=True), (B, HD))

    def drain(b, carry):
        o_copy(b).wait()
        return carry

    lax.fori_loop(0, B, drain, 0)


def lightning(hidden, g1, slopes, out_norm, lin_state, w_qkv, w_gate):
    return pl.pallas_call(
        lightning_kernel,
        out_shape=[jax.ShapeDtypeStruct((B, HL, HD, HD), F32), jax.ShapeDtypeStruct((B, HL * HD), F32),
                   jax.ShapeDtypeStruct((B, HD), F32), jax.ShapeDtypeStruct((B, D), BF16)],
        in_specs=[vmem_spec(), vmem_spec(), smem_spec(), vmem_spec(), any_spec(), any_spec(), any_spec()],
        out_specs=[any_spec(), vmem_spec(), vmem_spec(), vmem_spec()],
        scratch_shapes=[
            pltpu.VMEM((RING, 4, DCH, HL, HD), BF16),
            pltpu.VMEM((B, HL, HD, HD), F32),
            pltpu.VMEM((STEPS, B, DCH * HL), BF16),
            pltpu.VMEM((1024, 1024), BF16),
            pltpu.VMEM((2, HL * B, 2 * HD), F32),
            pltpu.VMEM((HL, HD, 2 * B), BF16),
            pltpu.VMEM((HL, B, HD), BF16),
            pltpu.VMEM((B, HL, HD), F32),
            pltpu.SemaphoreType.DMA((RING, 4)),
            pltpu.SemaphoreType.DMA((B,)),
            pltpu.SemaphoreType.DMA((B,)),
        ],
        compiler_params=pltpu.CompilerParams(vmem_limit_bytes=VMEM_LIMIT),
        name="lightning",
    )(hidden, g1, slopes, out_norm, lin_state, w_qkv, w_gate)


NCH = 4
CW = D // 2 // NCH


def peers():
    dp = lax.axis_index("dp")
    me = lax.axis_index("tp")
    core = lax.rem(me, 2)
    chip = me // 2
    mate = (dp, chip * 2 + (1 - core))
    across = (dp, (1 - chip) * 2 + core)
    diag = (dp, (1 - chip) * 2 + (1 - core))
    return core, mate, across, diag


def entry_barrier(targets):
    barrier = pltpu.get_barrier_semaphore()
    for dev in targets:
        pl.semaphore_signal(barrier, inc=1, device_id=dev, device_id_type=MESH)
    pl.semaphore_wait(barrier, len(targets))


def rcopy(src, dst, send, recv, dev):
    return pltpu.make_async_remote_copy(src_ref=src, dst_ref=dst, send_sem=send, recv_sem=recv,
                                        device_id=dev, device_id_type=MESH)


def exchange(left, wbuf, wwait, mid_work, core, mate, across,
             a_send, a_recv, b_send, b_recv, total, sems):
    sa, ra, sb, rb, sc, rc = sems
    per = CW // HD

    def product(half, j):
        base = half * (NC // 2) + j * per
        cols = []
        for p in range(per // 2):
            w = jnp.concatenate([wbuf[base + 2 * p], wbuf[base + 2 * p + 1]], axis=1)
            cols.append(dot(left, w))
        return jnp.concatenate(cols, axis=1)

    a_copies, b_copies, c_copies = [], [], []
    for j in range(NCH):
        wwait(1 - core, j)
        a_send[j] = product(1 - core, j)
        cp = rcopy(a_send.at[j], a_recv.at[j], sa.at[j], ra.at[j], mate)
        cp.start()
        a_copies.append(cp)
        wwait(core, j)
        b_send[j] = product(core, j)
        if j >= 1:
            send_across(j - 1, a_copies, b_copies, a_recv, b_send, b_recv, sb, rb, across)
    send_across(NCH - 1, a_copies, b_copies, a_recv, b_send, b_recv, sb, rb, across)
    mid_work()
    for j in range(NCH):
        b_copies[j].wait_recv()
        total[core, j] = b_send[j] + b_recv[j]
        cp = rcopy(total.at[core, j], total.at[core, j], sc.at[j], rc.at[j], mate)
        cp.start()
        c_copies.append(cp)
    for j in range(NCH):
        c_copies[j].wait_recv()
    for j in range(NCH):
        a_copies[j].wait_send()
        b_copies[j].wait_send()
        c_copies[j].wait_send()


def send_across(j, a_copies, b_copies, a_recv, b_send, b_recv, sb, rb, across):
    a_copies[j].wait_recv()
    b_send[j] = b_send[j] + a_recv[j]
    cp = rcopy(b_send.at[j], b_recv.at[j], sb.at[j], rb.at[j], across)
    cp.start()
    b_copies.append(cp)


def exchange_scratch():
    return [
        pltpu.VMEM((NC, HL * HD, HD), BF16),
        pltpu.VMEM((NCH, B, CW), F32),
        pltpu.VMEM((NCH, B, CW), F32),
        pltpu.VMEM((NCH, B, CW), F32),
        pltpu.VMEM((NCH, B, CW), F32),
        pltpu.VMEM((2, NCH, B, CW), F32),
        pltpu.SemaphoreType.DMA((NC,)),
        pltpu.SemaphoreType.DMA((NCH,)),
        pltpu.SemaphoreType.DMA((NCH,)),
        pltpu.SemaphoreType.DMA((NCH,)),
        pltpu.SemaphoreType.DMA((NCH,)),
        pltpu.SemaphoreType.DMA((NCH,)),
        pltpu.SemaphoreType.DMA((NCH,)),
    ]


def out_weights(w_ref, wbuf, wsem, core):
    per = CW // HD

    def copy(c):
        cols = pl.ds(pl.multiple_of(c * HD, HD), HD)
        return pltpu.make_async_copy(w_ref.at[:, cols], wbuf.at[c], wsem.at[c])

    def start():
        for j in range(NCH):
            for half in (1 - core, core):
                for p in range(per):
                    copy(half * (NC // 2) + j * per + p).start()

    def wait(half, j):
        for p in range(per):
            copy(half * (NC // 2) + j * per + p).wait()

    return start, wait


WA_ROWS = D * KV * (GQ + 2)
WA_CH = 32
WA_STEP = WA_ROWS // WA_CH
NJ = KV * (GQ + 2)


def mid_kernel(og_ref, ss_ref, h1_ref, g2_ref, alpha_ref, beta_ref, len_ref, wout_ref, wattn_ref,
               q_ref, kn_ref, vn_ref, h2_ref,
               wbuf, a_send, a_recv, b_send, b_recv, total, wsem, sa, ra, sb, rb, sc, rc,
               wraw, wide, w2, ss_recv, wasem, ss_s, ss_r):
    core, mate, across, diag = peers()
    start_w, wait_w = out_weights(wout_ref, wbuf, wsem, core)
    start_w()

    def wa_copy(i):
        return pltpu.make_async_copy(wattn_ref.at[pl.ds(i * WA_STEP, WA_STEP)], wraw.at[i], wasem.at[i])

    def wa_start(i, carry):
        wa_copy(i).start()
        return carry

    lax.fori_loop(0, WA_CH, wa_start, 0)
    entry_barrier((mate, across, diag))
    ss_copies = []
    for n, dev in enumerate((mate, across, diag)):
        cp = rcopy(ss_ref, ss_recv.at[n], ss_s.at[n], ss_r.at[n], dev)
        cp.start()
        ss_copies.append(cp)
    for cp in ss_copies:
        cp.wait_recv()
    ssum = (ss_ref[...] + ss_recv[0]) + (ss_recv[1] + ss_recv[2])
    inv = lax.rsqrt(ssum[:, 0:1] / D + EPS)
    left = (og_ref[...] * inv).astype(BF16)

    def relayout():
        def body(i, carry):
            wa_copy(i).wait()
            wide[...] = wraw[i].astype(F32)
            for j in range(NJ):
                w2[j, pl.ds(pl.multiple_of(i * HD, HD), HD), :] = wide[pl.ds(j, HD, stride=NJ), :].astype(BF16)
            return carry
        lax.fori_loop(0, WA_CH, body, 0)

    exchange(left, wbuf, wait_w, relayout, core, mate, across, a_send, a_recv, b_send, b_recv, total,
             (sa, ra, sb, rb, sc, rc))
    for cp in ss_copies:
        cp.wait_send()

    per = CW // HD
    alpha = alpha_ref[0]
    beta = beta_ref[0]
    sq = jnp.zeros((B, HD), F32)
    mids = []
    for c in range(NC):
        a1 = total[c // (NC // 2), (c % (NC // 2)) // per, :, (c % per) * HD:(c % per + 1) * HD]
        m = (alpha * h1_ref[:, c * HD:(c + 1) * HD].astype(F32) + beta * a1).astype(BF16)
        h2_ref[:, c * HD:(c + 1) * HD] = m
        x = m.astype(F32)
        sq = sq + x * x
    inv2 = lax.rsqrt(jnp.sum(sq, axis=1, keepdims=True) / D + EPS)
    for c in range(NC):
        m = h2_ref[:, c * HD:(c + 1) * HD].astype(F32)
        h2_ref[:, c * HD:(c + 1) * HD] = (m * inv2 * g2_ref[c:c + 1, :]).astype(BF16)

    pos = jnp.zeros((B, HD), F32)
    row_i = lax.broadcasted_iota(jnp.int32, (B, HD), 0)
    for b in range(B):
        pos = jnp.where(row_i == b, jnp.full((B, HD), len_ref[b]).astype(F32), pos)
    lane = lax.broadcasted_iota(jnp.int32, (B, HD), 1)
    freq = jnp.exp((lane % 32).astype(F32) * (-2.0 * math.log(ROPE_BASE) / 64))
    ang = pos * freq
    rot = lane < 64
    cosv = jnp.where(rot, jnp.cos(ang), 1.0)
    sinv = jnp.sin(ang)
    sin_lo = jnp.where(lane < 32, -sinv, 0.0)
    sin_hi = jnp.where((lane >= 32) & rot, sinv, 0.0)

    def turn(x):
        return x * cosv + pltpu.roll(x, HD - 32, 1) * sin_lo + pltpu.roll(x, 32, 1) * sin_hi

    h2 = h2_ref[...]
    for j in range(GQ + 2):
        w = jnp.concatenate([w2[2 * j], w2[2 * j + 1]], axis=1)
        pr = dot(h2, w)
        for kv in range(KV):
            x = pr[:, kv * HD:(kv + 1) * HD]
            if j < GQ:
                q_ref[pl.ds(kv * GQ + j, B, stride=8), :] = turn(x).astype(BF16).astype(F32)
            elif j == GQ:
                kn_ref[kv] = turn(x).astype(BF16).astype(F32)
            else:
                vn_ref[kv] = x.astype(BF16).astype(F32)


def middle(og, ss, h1, g2, alpha, beta, cache_len, w_out, w_attn):
    return pl.pallas_call(
        mid_kernel,
        out_shape=[jax.ShapeDtypeStruct((B * 8, HD), F32), jax.ShapeDtypeStruct((KV, B, HD), F32),
                   jax.ShapeDtypeStruct((KV, B, HD), F32), jax.ShapeDtypeStruct((B, D), BF16)],
        in_specs=[vmem_spec(), vmem_spec(), vmem_spec(), vmem_spec(), smem_spec(), smem_spec(), smem_spec(),
                  any_spec(), any_spec()],
        out_specs=[vmem_spec()] * 4,
        scratch_shapes=exchange_scratch() + [
            pltpu.VMEM((WA_CH, WA_STEP, HD), BF16),
            pltpu.VMEM((WA_STEP, HD), F32),
            pltpu.VMEM((NJ, D, HD), BF16),
            pltpu.VMEM((3, B, HD), F32),
            pltpu.SemaphoreType.DMA((WA_CH,)),
            pltpu.SemaphoreType.DMA((3,)),
            pltpu.SemaphoreType.DMA((3,)),
        ],
        compiler_params=pltpu.CompilerParams(vmem_limit_bytes=VMEM_LIMIT, collective_id=0, has_side_effects=True),
        name="middle",
    )(og, ss, h1, g2, alpha, beta, cache_len, w_out, w_attn)


def attention_kernel(len_ref, q_ref, kn_ref, vn_ref, k_ref, v_ref, at_ref, ko_ref, vo_ref,
                     kbuf, vbuf, isem, osem):
    def ins(b):
        return (pltpu.make_async_copy(k_ref.at[b], kbuf.at[b], isem.at[0, b]),
                pltpu.make_async_copy(v_ref.at[b], vbuf.at[b], isem.at[1, b]))

    def outs(b):
        return (pltpu.make_async_copy(kbuf.at[b], ko_ref.at[b], osem.at[0, b]),
                pltpu.make_async_copy(vbuf.at[b], vo_ref.at[b], osem.at[1, b]))

    def start_in(b, carry):
        for cp in ins(b):
            cp.start()
        return carry

    lax.fori_loop(0, B, start_in, 0)
    row8 = lax.broadcasted_iota(jnp.int32, (8, HD), 0)
    row16 = lax.broadcasted_iota(jnp.int32, (16, HD), 0)
    tpos = lax.broadcasted_iota(jnp.int32, (8, T), 1)

    def body(b, carry):
        for cp in ins(b):
            cp.wait()
        p = len_ref[b]
        base = pl.multiple_of((p // 16) * 16, 16)
        hit = row16 == p - base
        for kv in range(KV):
            kn = kn_ref[kv, pl.ds(b, 1), :]
            vn = vn_ref[kv, pl.ds(b, 1), :]
            old_k = kbuf[b, kv, pl.ds(base, 16), :].astype(F32)
            old_v = vbuf[b, kv, pl.ds(base, 16), :].astype(F32)
            kbuf[b, kv, pl.ds(base, 16), :] = jnp.where(hit, kn, old_k).astype(BF16)
            vbuf[b, kv, pl.ds(base, 16), :] = jnp.where(hit, vn, old_v).astype(BF16)
        for cp in outs(b):
            cp.start()
        q = q_ref[pl.ds(b * 8, 8), :]
        q2 = jnp.concatenate([jnp.where(row8 < 4, q, 0.0), jnp.where(row8 < 4, 0.0, q)], axis=1).astype(BF16)
        k2 = jnp.concatenate([kbuf[b, 0], kbuf[b, 1]], axis=1)
        s = lax.dot_general(q2, k2, (((1,), (1,)), ((), ())), preferred_element_type=F32) * HD ** -0.5
        s = jnp.where(tpos <= p, s, -jnp.inf)
        e = jnp.exp(s - jnp.max(s, axis=1, keepdims=True))
        pr = (e / jnp.sum(e, axis=1, keepdims=True)).astype(BF16)
        v2 = jnp.concatenate([vbuf[b, 0], vbuf[b, 1]], axis=1)
        o = dot(pr, v2)
        at_ref[pl.ds(b * 8, 8), :] = jnp.where(row8 < 4, o[:, 0:HD], o[:, HD:])
        return carry

    lax.fori_loop(0, B, body, 0)

    def drain(b, carry):
        for cp in outs(b):
            cp.wait()
        return carry

    lax.fori_loop(0, B, drain, 0)


def attention(cache_len, q, kn, vn, k_cache, v_cache):
    return pl.pallas_call(
        attention_kernel,
        out_shape=[jax.ShapeDtypeStruct((B * 8, HD), F32), jax.ShapeDtypeStruct((B, KV, T, HD), BF16),
                   jax.ShapeDtypeStruct((B, KV, T, HD), BF16)],
        in_specs=[smem_spec(), vmem_spec(), vmem_spec(), vmem_spec(), any_spec(), any_spec()],
        out_specs=[vmem_spec(), any_spec(), any_spec()],
        scratch_shapes=[
            pltpu.VMEM((B, KV, T, HD), BF16),
            pltpu.VMEM((B, KV, T, HD), BF16),
            pltpu.SemaphoreType.DMA((2, B)),
            pltpu.SemaphoreType.DMA((2, B)),
        ],
        compiler_params=pltpu.CompilerParams(vmem_limit_bytes=VMEM_LIMIT),
        name="attention",
    )(cache_len, q, kn, vn, k_cache, v_cache)


def last_kernel(at_ref, h2_ref, alpha_ref, beta_ref, wout_ref, out_ref,
                wbuf, a_send, a_recv, b_send, b_recv, total, wsem, sa, ra, sb, rb, sc, rc):
    core, mate, across, diag = peers()
    start_w, wait_w = out_weights(wout_ref, wbuf, wsem, core)
    start_w()
    entry_barrier((mate, across))
    left = jnp.concatenate([at_ref[pl.ds(j, B, stride=8), :].astype(BF16) for j in range(8)], axis=1)
    exchange(left, wbuf, wait_w, lambda: None, core, mate, across, a_send, a_recv, b_send, b_recv, total,
             (sa, ra, sb, rb, sc, rc))
    per = CW // HD
    alpha = alpha_ref[1]
    beta = beta_ref[1]
    for c in range(NC):
        a2 = total[c // (NC // 2), (c % (NC // 2)) // per, :, (c % per) * HD:(c % per + 1) * HD]
        cols = slice(c * HD, (c + 1) * HD)
        out_ref[:, cols] = (alpha * h2_ref[:, cols].astype(F32) + beta * a2).astype(BF16)


def last(at, h2, alpha, beta, w_out):
    return pl.pallas_call(
        last_kernel,
        out_shape=jax.ShapeDtypeStruct((B, D), BF16),
        in_specs=[vmem_spec(), vmem_spec(), smem_spec(), smem_spec(), any_spec()],
        out_specs=vmem_spec(),
        scratch_shapes=exchange_scratch(),
        compiler_params=pltpu.CompilerParams(vmem_limit_bytes=VMEM_LIMIT, collective_id=1, has_side_effects=True),
        name="last",
    )(at, h2, alpha, beta, w_out)


def solution(mesh):
    row_spec = P('dp', None)
    cache_spec = P('dp', 'tp', None, None)
    in_specs = (row_spec, P('dp'), cache_spec, cache_spec, cache_spec, P(None), P(None, None, 'tp', None),
                P(None, 'tp', None), P('tp'), P('tp', None), P('tp', None, None), P(None),
                P(None, 'tp', None, None), P('tp', None, None), P(None), P(None))
    out_specs = (row_spec, cache_spec, cache_spec, cache_spec)

    def local_step(hidden, cache_len, lin_state, k_cache, v_cache, norm_first, w_qkv, w_gate, slopes, out_norm,
                   w_out_lin, norm_second, w_attn, w_out_attn, mix_alpha, mix_beta):
        g1 = norm_first.reshape(NC, HD)
        g2 = norm_second.reshape(NC, HD)
        wa = jnp.transpose(w_attn, (0, 2, 1, 3)).reshape(WA_ROWS, HD)
        state_out, og, ss, h1 = lightning(hidden, g1, slopes, out_norm, lin_state, w_qkv, w_gate)
        q, kn, vn, h2 = middle(og, ss, h1, g2, mix_alpha, mix_beta, cache_len, w_out_lin.reshape(HL * HD, D), wa)
        at, k_out, v_out = attention(cache_len, q, kn, vn, k_cache, v_cache)
        hidden_out = last(at, h2, mix_alpha, mix_beta, w_out_attn.reshape(HL * HD, D))
        return hidden_out, state_out, k_out, v_out

    return jax.shard_map(local_step, mesh=mesh, in_specs=in_specs, out_specs=out_specs, check_vma=False)
```

```python
import functools
import math

import jax
import jax.numpy as jnp
from jax import lax
from jax.experimental import pallas as pl
from jax.experimental.pallas import tpu as pltpu
from jax.sharding import PartitionSpec as P

EPS = 1e-5
ROPE_BASE = 10000000.0
MESH = pl.DeviceIdType.MESH
F32 = jnp.float32
BF16 = jnp.bfloat16
MIB = 1024 * 1024

B = 32
D = 4096
HL = 8
HD = 128
KV = 2
GQ = 4
T = 512
NC = D // HD

DCH = 256
STEPS = D // DCH
RING = 4


def any_spec():
    return pl.BlockSpec(memory_space=pl.ANY)


def vmem_spec():
    return pl.BlockSpec(memory_space=pltpu.VMEM)


def smem_spec():
    return pl.BlockSpec(memory_space=pltpu.SMEM)


def dot(a, b):
    return jnp.dot(a, b, preferred_element_type=F32)


def lightning_kernel(hid_ref, g1_ref, slopes_ref, onorm_ref, state_ref, wqkv_ref, wgate_ref,
                     sout_ref, og_ref, ss_ref, h1_ref,
                     wbuf, sbuf, hstack, ebuf, lbuf, acc, qk_t, v_s, o_s, wsem, ssem, osem):
    def w_copies(step, slot):
        rows = pl.ds(step * DCH, DCH)
        out = [pltpu.make_async_copy(wqkv_ref.at[rows, c], wbuf.at[slot, c], wsem.at[slot, c]) for c in range(3)]
        out.append(pltpu.make_async_copy(wgate_ref.at[rows], wbuf.at[slot, 3], wsem.at[slot, 3]))
        return out

    def s_copy(b):
        return pltpu.make_async_copy(state_ref.at[b], sbuf.at[b], ssem.at[b])

    def o_copy(b):
        return pltpu.make_async_copy(sbuf.at[b], sout_ref.at[b], osem.at[b])

    for i in range(RING):
        for cp in w_copies(i, i):
            cp.start()

    sq = jnp.zeros((B, HD), F32)
    for c in range(NC):
        x = hid_ref[:, c * HD:(c + 1) * HD].astype(F32)
        sq = sq + x * x
    inv = lax.rsqrt(jnp.sum(sq, axis=1, keepdims=True) / D + EPS)
    rr = lax.broadcasted_iota(jnp.int32, (HD, 256), 1)
    dd = lax.broadcasted_iota(jnp.int32, (HD, 256), 0)
    for c in range(NC):
        x = hid_ref[:, c * HD:(c + 1) * HD].astype(F32)
        h1 = (x * inv * g1_ref[c:c + 1, :]).astype(BF16)
        h1_ref[:, c * HD:(c + 1) * HD] = h1
        hstack[c * B:(c + 1) * B, :] = h1
    for n in range(4):
        spread = jnp.where(rr // 8 + 32 * n == dd, 1.0, 0.0).astype(BF16)
        for c in range(NC // 8):
            e = dot(hstack[c * 256:(c + 1) * 256, :], spread).astype(BF16)
            for k in range(8):
                cc = c * 8 + k
                off = (cc % (DCH // HD)) * 1024 + n * 256
                ebuf[cc // (DCH // HD), :, off:off + 256] = e[k * B:(k + 1) * B, :]

    acc[...] = jnp.zeros_like(acc)
    lane = lax.broadcasted_iota(jnp.int32, (B, DCH * HL), 1) % 8

    def step_fn(i, carry):
        slot = lax.rem(i, RING)
        for k in range(B // STEPS):
            s_copy(i * (B // STEPS) + k).start()
        e = ebuf[i]
        for h in range(HL):
            keep = jnp.where(lane == h, 1.0, 0.0).astype(BF16)
            lbuf[h * B:(h + 1) * B, :] = e * keep
        for cp in w_copies(i, slot):
            cp.wait()
        left = lbuf[...]
        for pair in range(2):
            right = jnp.concatenate([wbuf[slot, 2 * pair].reshape(DCH * HL, HD),
                                     wbuf[slot, 2 * pair + 1].reshape(DCH * HL, HD)], axis=1)
            acc[pair] += dot(left, right)

        @pl.when(i + RING < STEPS)
        def _():
            for cp in w_copies(i + RING, slot):
                cp.start()
        return carry

    lax.fori_loop(0, STEPS, step_fn, 0)

    for h in range(HL):
        rows = slice(h * B, (h + 1) * B)
        q = jax.nn.silu(acc[0, rows, 0:HD]).astype(BF16)
        k = jax.nn.silu(acc[0, rows, HD:2 * HD]).astype(BF16)
        v = jax.nn.silu(acc[1, rows, 0:HD]).astype(BF16)
        qk = jnp.concatenate([k, q], axis=0).astype(F32)
        qk_t[h] = jnp.transpose(qk).astype(BF16)
        v_s[h] = v

    def row_fn(b, carry):
        s_copy(b).wait()
        row_i = lax.broadcasted_iota(jnp.int32, (B, HD), 0)
        hit = row_i == b
        ones = jnp.where(hit, 1.0, 0.0).astype(BF16)
        zero = jnp.zeros((B, HD), BF16)
        for h in range(HL):
            top = jnp.concatenate([v_s[h] * ones, zero], axis=1)
            bot = jnp.concatenate([zero, ones], axis=1)
            prod = dot(qk_t[h], jnp.concatenate([top, bot], axis=0))
            decay = jnp.exp(jnp.full((1, HD), -slopes_ref[h], F32))
            new = decay * sbuf[b, h] + prod[:, 0:HD]
            sbuf[b, h] = new
            o_s[b, h:h + 1, :] = jnp.sum(prod[:, HD:] * new, axis=0, keepdims=True)
        o_copy(b).start()
        return carry

    lax.fori_loop(0, B, row_fn, 0)

    ss = jnp.zeros((B, HD), F32)
    for h in range(HL):
        o = o_s[:, h, :]
        ss = ss + o * o
        gate = jax.nn.sigmoid(acc[1, h * B:(h + 1) * B, HD:2 * HD])
        og_ref[:, h * HD:(h + 1) * HD] = o * onorm_ref[h:h + 1, :] * gate
    ss_ref[...] = jnp.broadcast_to(jnp.sum(ss, axis=1, keepdims=True), (B, HD))

    def drain(b, carry):
        o_copy(b).wait()
        return carry

    lax.fori_loop(0, B, drain, 0)


def lightning(hidden, g1, slopes, out_norm, lin_state, w_qkv, w_gate):
    return pl.pallas_call(
        lightning_kernel,
        out_shape=[jax.ShapeDtypeStruct((B, HL, HD, HD), F32), jax.ShapeDtypeStruct((B, HL * HD), F32),
                   jax.ShapeDtypeStruct((B, HD), F32), jax.ShapeDtypeStruct((B, D), BF16)],
        in_specs=[vmem_spec(), vmem_spec(), smem_spec(), vmem_spec(), any_spec(), any_spec(), any_spec()],
        out_specs=[any_spec(), vmem_spec(), vmem_spec(), vmem_spec()],
        scratch_shapes=[
            pltpu.VMEM((RING, 4, DCH, HL, HD), BF16),
            pltpu.VMEM((B, HL, HD, HD), F32),
            pltpu.VMEM((NC * B, HD), BF16),
            pltpu.VMEM((STEPS, B, DCH * HL), BF16),
            pltpu.VMEM((HL * B, DCH * HL), BF16),
            pltpu.VMEM((2, HL * B, 2 * HD), F32),
            pltpu.VMEM((HL, HD, 2 * B), BF16),
            pltpu.VMEM((HL, B, HD), BF16),
            pltpu.VMEM((B, HL, HD), F32),
            pltpu.SemaphoreType.DMA((RING, 4)),
            pltpu.SemaphoreType.DMA((B,)),
            pltpu.SemaphoreType.DMA((B,)),
        ],
        compiler_params=pltpu.CompilerParams(vmem_limit_bytes=40 * MIB),
        name="lightning",
    )(hidden, g1, slopes, out_norm, lin_state, w_qkv, w_gate)


NCH = 4
CW = D // 2 // NCH


def peers():
    dp = lax.axis_index("dp")
    me = lax.axis_index("tp")
    core = lax.rem(me, 2)
    chip = me // 2
    mate = (dp, chip * 2 + (1 - core))
    across = (dp, (1 - chip) * 2 + core)
    diag = (dp, (1 - chip) * 2 + (1 - core))
    return core, mate, across, diag


def entry_barrier(targets):
    barrier = pltpu.get_barrier_semaphore()
    for dev in targets:
        pl.semaphore_signal(barrier, inc=1, device_id=dev, device_id_type=MESH)
    pl.semaphore_wait(barrier, len(targets))


def rcopy(src, dst, send, recv, dev):
    return pltpu.make_async_remote_copy(src_ref=src, dst_ref=dst, send_sem=send, recv_sem=recv,
                                        device_id=dev, device_id_type=MESH)


def exchange(left, wbuf, wwait, mid_work, core, mate, across,
             a_send, a_recv, b_send, b_recv, total, sems):
    sa, ra, sb, rb, sc, rc = sems
    per = CW // HD

    def product(half, j):
        base = half * (NC // 2) + j * per
        cols = []
        for p in range(per // 2):
            w = jnp.concatenate([wbuf[base + 2 * p], wbuf[base + 2 * p + 1]], axis=1)
            cols.append(dot(left, w))
        return jnp.concatenate(cols, axis=1)

    a_copies, b_copies, c_copies = [], [], []
    for j in range(NCH):
        wwait(1 - core, j)
        a_send[j] = product(1 - core, j)
        cp = rcopy(a_send.at[j], a_recv.at[j], sa.at[j], ra.at[j], mate)
        cp.start()
        a_copies.append(cp)
        wwait(core, j)
        b_send[j] = product(core, j)
        if j >= 1:
            send_across(j - 1, a_copies, b_copies, a_recv, b_send, b_recv, sb, rb, across)
    send_across(NCH - 1, a_copies, b_copies, a_recv, b_send, b_recv, sb, rb, across)
    mid_work()
    for j in range(NCH):
        b_copies[j].wait_recv()
        total[core, j] = b_send[j] + b_recv[j]
        cp = rcopy(total.at[core, j], total.at[core, j], sc.at[j], rc.at[j], mate)
        cp.start()
        c_copies.append(cp)
    for j in range(NCH):
        c_copies[j].wait_recv()
    for j in range(NCH):
        a_copies[j].wait_send()
        b_copies[j].wait_send()
        c_copies[j].wait_send()


def send_across(j, a_copies, b_copies, a_recv, b_send, b_recv, sb, rb, across):
    a_copies[j].wait_recv()
    b_send[j] = b_send[j] + a_recv[j]
    cp = rcopy(b_send.at[j], b_recv.at[j], sb.at[j], rb.at[j], across)
    cp.start()
    b_copies.append(cp)


def exchange_scratch():
    return [
        pltpu.VMEM((NC, HL * HD, HD), BF16),
        pltpu.VMEM((NCH, B, CW), F32),
        pltpu.VMEM((NCH, B, CW), F32),
        pltpu.VMEM((NCH, B, CW), F32),
        pltpu.VMEM((NCH, B, CW), F32),
        pltpu.VMEM((2, NCH, B, CW), F32),
        pltpu.SemaphoreType.DMA((NC,)),
        pltpu.SemaphoreType.DMA((NCH,)),
        pltpu.SemaphoreType.DMA((NCH,)),
        pltpu.SemaphoreType.DMA((NCH,)),
        pltpu.SemaphoreType.DMA((NCH,)),
        pltpu.SemaphoreType.DMA((NCH,)),
        pltpu.SemaphoreType.DMA((NCH,)),
    ]


def out_weights(w_ref, wbuf, wsem, core):
    per = CW // HD

    def copy(c):
        cols = pl.ds(pl.multiple_of(c * HD, HD), HD)
        return pltpu.make_async_copy(w_ref.at[:, cols], wbuf.at[c], wsem.at[c])

    def start():
        for j in range(NCH):
            for half in (1 - core, core):
                for p in range(per):
                    copy(half * (NC // 2) + j * per + p).start()

    def wait(half, j):
        for p in range(per):
            copy(half * (NC // 2) + j * per + p).wait()

    return start, wait


WA_ROWS = D * KV * (GQ + 2)
WA_CH = 32
WA_STEP = WA_ROWS // WA_CH
NJ = KV * (GQ + 2)


def mid_kernel(og_ref, ss_ref, h1_ref, g2_ref, alpha_ref, beta_ref, len_ref, wout_ref, wattn_ref,
               k_ref, v_ref, q_ref, kn_ref, vn_ref, h2_ref, kbuf, vbuf,
               wbuf, a_send, a_recv, b_send, b_recv, total, wsem, sa, ra, sb, rb, sc, rc,
               wraw, wide, w2, ss_recv, wasem, ss_s, ss_r, csem):
    core, mate, across, diag = peers()
    start_w, wait_w = out_weights(wout_ref, wbuf, wsem, core)
    start_w()

    def wa_copy(i):
        return pltpu.make_async_copy(wattn_ref.at[pl.ds(i * WA_STEP, WA_STEP)], wraw.at[i], wasem.at[i])

    def wa_start(i, carry):
        wa_copy(i).start()
        return carry

    lax.fori_loop(0, WA_CH, wa_start, 0)
    caches = [pltpu.make_async_copy(k_ref, kbuf, csem.at[0]), pltpu.make_async_copy(v_ref, vbuf, csem.at[1])]
    for cp in caches:
        cp.start()
    entry_barrier((mate, across, diag))
    ss_copies = []
    for n, dev in enumerate((mate, across, diag)):
        cp = rcopy(ss_ref, ss_recv.at[n], ss_s.at[n], ss_r.at[n], dev)
        cp.start()
        ss_copies.append(cp)
    for cp in ss_copies:
        cp.wait_recv()
    ssum = (ss_ref[...] + ss_recv[0]) + (ss_recv[1] + ss_recv[2])
    inv = lax.rsqrt(ssum[:, 0:1] / D + EPS)
    left = (og_ref[...] * inv).astype(BF16)

    def relayout():
        def body(i, carry):
            wa_copy(i).wait()
            wide[...] = wraw[i].astype(F32)
            for j in range(NJ):
                w2[j, pl.ds(pl.multiple_of(i * HD, HD), HD), :] = wide[pl.ds(j, HD, stride=NJ), :].astype(BF16)
            return carry
        lax.fori_loop(0, WA_CH, body, 0)

    exchange(left, wbuf, wait_w, relayout, core, mate, across, a_send, a_recv, b_send, b_recv, total,
             (sa, ra, sb, rb, sc, rc))
    for cp in ss_copies:
        cp.wait_send()

    per = CW // HD
    alpha = alpha_ref[0]
    beta = beta_ref[0]
    sq = jnp.zeros((B, HD), F32)
    mids = []
    for c in range(NC):
        a1 = total[c // (NC // 2), (c % (NC // 2)) // per, :, (c % per) * HD:(c % per + 1) * HD]
        m = (alpha * h1_ref[:, c * HD:(c + 1) * HD].astype(F32) + beta * a1).astype(BF16)
        h2_ref[:, c * HD:(c + 1) * HD] = m
        x = m.astype(F32)
        sq = sq + x * x
    inv2 = lax.rsqrt(jnp.sum(sq, axis=1, keepdims=True) / D + EPS)
    for c in range(NC):
        m = h2_ref[:, c * HD:(c + 1) * HD].astype(F32)
        h2_ref[:, c * HD:(c + 1) * HD] = (m * inv2 * g2_ref[c:c + 1, :]).astype(BF16)

    pos = jnp.zeros((B, HD), F32)
    row_i = lax.broadcasted_iota(jnp.int32, (B, HD), 0)
    for b in range(B):
        pos = jnp.where(row_i == b, jnp.full((B, HD), len_ref[b]).astype(F32), pos)
    lane = lax.broadcasted_iota(jnp.int32, (B, HD), 1)
    freq = jnp.exp((lane % 32).astype(F32) * (-2.0 * math.log(ROPE_BASE) / 64))
    ang = pos * freq
    rot = lane < 64
    cosv = jnp.where(rot, jnp.cos(ang), 1.0)
    sinv = jnp.sin(ang)
    sin_lo = jnp.where(lane < 32, -sinv, 0.0)
    sin_hi = jnp.where((lane >= 32) & rot, sinv, 0.0)

    def turn(x):
        return x * cosv + pltpu.roll(x, HD - 32, 1) * sin_lo + pltpu.roll(x, 32, 1) * sin_hi

    h2 = h2_ref[...]
    for j in range(GQ + 2):
        w = jnp.concatenate([w2[2 * j], w2[2 * j + 1]], axis=1)
        pr = dot(h2, w)
        for kv in range(KV):
            x = pr[:, kv * HD:(kv + 1) * HD]
            if j < GQ:
                q_ref[pl.ds(kv * GQ + j, B, stride=8), :] = turn(x).astype(BF16).astype(F32)
            elif j == GQ:
                kn_ref[kv] = turn(x).astype(BF16).astype(F32)
            else:
                vn_ref[kv] = x.astype(BF16).astype(F32)
    for cp in caches:
        cp.wait()


def middle(og, ss, h1, g2, alpha, beta, cache_len, w_out, w_attn, k_cache, v_cache):
    return pl.pallas_call(
        mid_kernel,
        out_shape=[jax.ShapeDtypeStruct((B * 8, HD), F32), jax.ShapeDtypeStruct((KV, B, HD), F32),
                   jax.ShapeDtypeStruct((KV, B, HD), F32), jax.ShapeDtypeStruct((B, D), BF16),
                   pltpu.VMEM((B, KV, T, HD), BF16), pltpu.VMEM((B, KV, T, HD), BF16)],
        in_specs=[vmem_spec(), vmem_spec(), vmem_spec(), vmem_spec(), smem_spec(), smem_spec(), smem_spec(),
                  any_spec(), any_spec(), any_spec(), any_spec()],
        out_specs=[vmem_spec()] * 6,
        scratch_shapes=exchange_scratch() + [
            pltpu.VMEM((WA_CH, WA_STEP, HD), BF16),
            pltpu.VMEM((WA_STEP, HD), F32),
            pltpu.VMEM((NJ, D, HD), BF16),
            pltpu.VMEM((3, B, HD), F32),
            pltpu.SemaphoreType.DMA((WA_CH,)),
            pltpu.SemaphoreType.DMA((3,)),
            pltpu.SemaphoreType.DMA((3,)),
            pltpu.SemaphoreType.DMA((2,)),
        ],
        compiler_params=pltpu.CompilerParams(vmem_limit_bytes=37 * MIB, collective_id=0, has_side_effects=True),
        name="middle",
    )(og, ss, h1, g2, alpha, beta, cache_len, w_out, w_attn, k_cache, v_cache)


ROWS = 4


def attention_kernel(len_ref, q_ref, kn_ref, vn_ref, kin_ref, vin_ref, at_ref, ko_ref, vo_ref, kbuf, vbuf, osem):
    def outs(b):
        return (pltpu.make_async_copy(kbuf.at[b], ko_ref.at[b], osem.at[0, b]),
                pltpu.make_async_copy(vbuf.at[b], vo_ref.at[b], osem.at[1, b]))

    row8 = lax.broadcasted_iota(jnp.int32, (8, HD), 0)
    row16 = lax.broadcasted_iota(jnp.int32, (16, HD), 0)
    tpos = lax.broadcasted_iota(jnp.int32, (8, T), 1)

    def body(i, carry):
        rows = [i * ROWS + r for r in range(ROWS)]
        lens = [len_ref[b] for b in rows]
        for b, p in zip(rows, lens):
            base = pl.multiple_of((p // 16) * 16, 16)
            hit = row16 == p - base
            for kv in range(KV):
                for buf, new in ((kbuf, kn_ref), (vbuf, vn_ref)):
                    old = buf[b, kv, pl.ds(base, 16), :].astype(F32)
                    buf[b, kv, pl.ds(base, 16), :] = jnp.where(hit, new[kv, pl.ds(b, 1), :], old).astype(BF16)
        for b in rows:
            for cp in outs(b):
                cp.start()
        scores = []
        for b, p in zip(rows, lens):
            q = q_ref[pl.ds(b * 8, 8), :]
            q2 = jnp.concatenate([jnp.where(row8 < 4, q, 0.0), jnp.where(row8 < 4, 0.0, q)], axis=1).astype(BF16)
            k2 = jnp.concatenate([kbuf[b, 0], kbuf[b, 1]], axis=1)
            s = lax.dot_general(q2, k2, (((1,), (1,)), ((), ())), preferred_element_type=F32) * HD ** -0.5
            scores.append(jnp.where(tpos <= p, s, -jnp.inf))
        tops = [jnp.max(s, axis=1, keepdims=True) for s in scores]
        es = [jnp.exp(s - m) for s, m in zip(scores, tops)]
        sums = [jnp.sum(e, axis=1, keepdims=True) for e in es]
        prs = [(e / z).astype(BF16) for e, z in zip(es, sums)]
        for b, pr in zip(rows, prs):
            o = dot(pr, jnp.concatenate([vbuf[b, 0], vbuf[b, 1]], axis=1))
            at_ref[pl.ds(b * 8, 8), :] = jnp.where(row8 < 4, o[:, 0:HD], o[:, HD:])
        return carry

    lax.fori_loop(0, B // ROWS, body, 0)

    def drain(b, carry):
        for cp in outs(b):
            cp.wait()
        return carry

    lax.fori_loop(0, B, drain, 0)


def attention(cache_len, q, kn, vn, kbuf, vbuf):
    return pl.pallas_call(
        attention_kernel,
        out_shape=[jax.ShapeDtypeStruct((B * 8, HD), F32), pltpu.HBM((B, KV, T, HD), BF16),
                   pltpu.HBM((B, KV, T, HD), BF16), pltpu.VMEM((B, KV, T, HD), BF16), pltpu.VMEM((B, KV, T, HD), BF16)],
        in_specs=[smem_spec(), vmem_spec(), vmem_spec(), vmem_spec(), vmem_spec(), vmem_spec()],
        out_specs=[vmem_spec(), any_spec(), any_spec(), vmem_spec(), vmem_spec()],
        input_output_aliases={4: 3, 5: 4},
        scratch_shapes=[pltpu.SemaphoreType.DMA((2, B))],
        compiler_params=pltpu.CompilerParams(vmem_limit_bytes=4 * MIB),
        name="attention",
    )(cache_len, q, kn, vn, kbuf, vbuf)[:3]


def last_kernel(at_ref, h2_ref, alpha_ref, beta_ref, wout_ref, out_ref,
                wbuf, a_send, a_recv, b_send, b_recv, total, wsem, sa, ra, sb, rb, sc, rc):
    core, mate, across, diag = peers()
    start_w, wait_w = out_weights(wout_ref, wbuf, wsem, core)
    start_w()
    entry_barrier((mate, across))
    left = jnp.concatenate([at_ref[pl.ds(j, B, stride=8), :].astype(BF16) for j in range(8)], axis=1)
    exchange(left, wbuf, wait_w, lambda: None, core, mate, across, a_send, a_recv, b_send, b_recv, total,
             (sa, ra, sb, rb, sc, rc))
    per = CW // HD
    alpha = alpha_ref[1]
    beta = beta_ref[1]
    for c in range(NC):
        a2 = total[c // (NC // 2), (c % (NC // 2)) // per, :, (c % per) * HD:(c % per + 1) * HD]
        cols = slice(c * HD, (c + 1) * HD)
        out_ref[:, cols] = (alpha * h2_ref[:, cols].astype(F32) + beta * a2).astype(BF16)


def last(at, h2, alpha, beta, w_out):
    return pl.pallas_call(
        last_kernel,
        out_shape=jax.ShapeDtypeStruct((B, D), BF16),
        in_specs=[vmem_spec(), vmem_spec(), smem_spec(), smem_spec(), any_spec()],
        out_specs=vmem_spec(),
        scratch_shapes=exchange_scratch(),
        compiler_params=pltpu.CompilerParams(vmem_limit_bytes=16 * MIB, collective_id=1, has_side_effects=True),
        name="last",
    )(at, h2, alpha, beta, w_out)


def solution(mesh):
    row_spec = P('dp', None)
    cache_spec = P('dp', 'tp', None, None)
    in_specs = (row_spec, P('dp'), cache_spec, cache_spec, cache_spec, P(None), P(None, None, 'tp', None),
                P(None, 'tp', None), P('tp'), P('tp', None), P('tp', None, None), P(None),
                P(None, 'tp', None, None), P('tp', None, None), P(None), P(None))
    out_specs = (row_spec, cache_spec, cache_spec, cache_spec)

    def local_step(hidden, cache_len, lin_state, k_cache, v_cache, norm_first, w_qkv, w_gate, slopes, out_norm,
                   w_out_lin, norm_second, w_attn, w_out_attn, mix_alpha, mix_beta):
        def hbm(x):
            return pltpu.with_memory_space_constraint(x, pltpu.HBM)

        g1 = norm_first.reshape(NC, HD)
        g2 = norm_second.reshape(NC, HD)
        wa = jnp.transpose(w_attn, (0, 2, 1, 3)).reshape(WA_ROWS, HD)
        state_out, og, ss, h1 = lightning(hidden, g1, slopes, out_norm, hbm(lin_state), hbm(w_qkv), hbm(w_gate))
        q, kn, vn, h2, kbuf, vbuf = middle(og, ss, h1, g2, mix_alpha, mix_beta, cache_len,
                                           hbm(w_out_lin.reshape(HL * HD, D)), hbm(wa), hbm(k_cache), hbm(v_cache))
        at, k_out, v_out = attention(cache_len, q, kn, vn, kbuf, vbuf)
        hidden_out = last(at, h2, mix_alpha, mix_beta, hbm(w_out_attn.reshape(HL * HD, D)))
        return hidden_out, state_out, k_out, v_out

    return jax.shard_map(local_step, mesh=mesh, in_specs=in_specs, out_specs=out_specs, check_vma=False)
```

```python
import functools
import math

import jax
import jax.numpy as jnp
from jax import lax
from jax.experimental import pallas as pl
from jax.experimental.pallas import tpu as pltpu
from jax.sharding import PartitionSpec as P

EPS = 1e-5
ROPE_BASE = 10000000.0
MESH = pl.DeviceIdType.MESH
F32 = jnp.float32
BF16 = jnp.bfloat16
MIB = 1024 * 1024

B = 32
D = 4096
HL = 8
HD = 128
KV = 2
GQ = 4
T = 512
NC = D // HD

DCH = 256
STEPS = D // DCH
RING = 4
EARLY = 24


def any_spec():
    return pl.BlockSpec(memory_space=pl.ANY)


def vmem_spec():
    return pl.BlockSpec(memory_space=pltpu.VMEM)


def smem_spec():
    return pl.BlockSpec(memory_space=pltpu.SMEM)


def dot(a, b):
    return jnp.dot(a, b, preferred_element_type=F32)


def lightning_kernel(hid_hbm, g1_hbm, slopes_hbm, onorm_hbm, state_ref, wqkv_ref, wgate_ref,
                     sout_ref, og_ref, ss_ref, h1_ref, hid_ref, g1_ref, onorm_ref, slopes_ref,
                     wbuf, gbuf, sbuf, hstack, ebuf, lbuf, acc, qk_t, v_s, o_s, psem, wsem, ssem, osem):
    def w_copies(step, slot):
        rows = pl.ds(step * DCH, DCH)
        return (pltpu.make_async_copy(wqkv_ref.at[rows], wbuf.at[slot], wsem.at[slot, 0]),
                pltpu.make_async_copy(wgate_ref.at[rows], gbuf.at[slot], wsem.at[slot, 1]))

    def s_copy(b):
        return pltpu.make_async_copy(state_ref.at[b], sbuf.at[b], ssem.at[b])

    def o_copy(b):
        return pltpu.make_async_copy(sbuf.at[b], sout_ref.at[b], osem.at[b])

    small = [pltpu.make_async_copy(src, dst, psem.at[n]) for n, (src, dst) in enumerate(
        ((hid_hbm, hid_ref), (g1_hbm, g1_ref), (onorm_hbm, onorm_ref), (slopes_hbm, slopes_ref)))]
    for cp in small:
        cp.start()
    for i in range(RING):
        for cp in w_copies(i, i):
            cp.start()
    for cp in small:
        cp.wait()

    sq = jnp.zeros((B, HD), F32)
    for c in range(NC):
        x = hid_ref[:, c * HD:(c + 1) * HD].astype(F32)
        sq = sq + x * x
    inv = lax.rsqrt(jnp.sum(sq, axis=1, keepdims=True) / D + EPS)
    rr = lax.broadcasted_iota(jnp.int32, (HD, 256), 1)
    dd = lax.broadcasted_iota(jnp.int32, (HD, 256), 0)
    for c in range(NC):
        x = hid_ref[:, c * HD:(c + 1) * HD].astype(F32)
        h1 = (x * inv * g1_ref[c:c + 1, :]).astype(BF16)
        h1_ref[:, c * HD:(c + 1) * HD] = h1
        hstack[c * B:(c + 1) * B, :] = h1
    for n in range(4):
        spread = jnp.where(rr // 8 + 32 * n == dd, 1.0, 0.0).astype(BF16)
        for c in range(NC // 8):
            e = dot(hstack[c * 256:(c + 1) * 256, :], spread).astype(BF16)
            for k in range(8):
                cc = c * 8 + k
                off = (cc % (DCH // HD)) * 1024 + n * 256
                ebuf[cc // (DCH // HD), :, off:off + 256] = e[k * B:(k + 1) * B, :]

    acc[...] = jnp.zeros_like(acc)
    lane = lax.broadcasted_iota(jnp.int32, (B, DCH * HL), 1) % 8

    def step_fn(i, carry):
        slot = lax.rem(i, RING)
        @pl.when(i >= STEPS - EARLY // 2)
        def _():
            for k in range(2):
                s_copy((i - (STEPS - EARLY // 2)) * 2 + k).start()

        e = ebuf[i]
        for h in range(HL):
            keep = jnp.where(lane == h, 1.0, 0.0).astype(BF16)
            lbuf[h * B:(h + 1) * B, :] = e * keep
        for cp in w_copies(i, slot):
            cp.wait()
        left = lbuf[...]
        for pair in range(2):
            second = wbuf[slot, :, 1] if pair == 0 else gbuf[slot]
            right = jnp.concatenate([wbuf[slot, :, 2 * pair].reshape(DCH * HL, HD), second.reshape(DCH * HL, HD)], axis=1)
            acc[pair] += dot(left, right)

        @pl.when(i + RING < STEPS)
        def _():
            for cp in w_copies(i + RING, slot):
                cp.start()
        return carry

    lax.fori_loop(0, STEPS, step_fn, 0)
    for b in range(EARLY, B):
        s_copy(b).start()

    for h in range(HL):
        rows = slice(h * B, (h + 1) * B)
        q = jax.nn.silu(acc[0, rows, 0:HD]).astype(BF16)
        k = jax.nn.silu(acc[0, rows, HD:2 * HD]).astype(BF16)
        v = jax.nn.silu(acc[1, rows, 0:HD]).astype(BF16)
        qk = jnp.concatenate([k, q], axis=0).astype(F32)
        qk_t[h] = jnp.transpose(qk).astype(BF16)
        v_s[h] = v

    def row_fn(b, carry):
        s_copy(b).wait()
        row_i = lax.broadcasted_iota(jnp.int32, (B, HD), 0)
        hit = row_i == b
        ones = jnp.where(hit, 1.0, 0.0).astype(BF16)
        zero = jnp.zeros((B, HD), BF16)
        for h in range(HL):
            top = jnp.concatenate([v_s[h] * ones, zero], axis=1)
            bot = jnp.concatenate([zero, ones], axis=1)
            prod = dot(qk_t[h], jnp.concatenate([top, bot], axis=0))
            decay = jnp.exp(jnp.full((1, HD), -slopes_ref[h], F32))
            new = decay * sbuf[b, h] + prod[:, 0:HD]
            sbuf[b, h] = new
            o_s[b, h:h + 1, :] = jnp.sum(prod[:, HD:] * new, axis=0, keepdims=True)
        o_copy(b).start()
        return carry

    lax.fori_loop(0, B, row_fn, 0)

    ss = jnp.zeros((B, HD), F32)
    for h in range(HL):
        o = o_s[:, h, :]
        ss = ss + o * o
    ss = jnp.sum(ss, axis=1, keepdims=True)
    ss_ref[...] = jnp.broadcast_to(ss, (B, HD))
    inv_own = lax.rsqrt(ss / (HL * HD) + EPS)
    for h in range(HL):
        gate = jax.nn.sigmoid(acc[1, h * B:(h + 1) * B, HD:2 * HD])
        og_ref[:, h * HD:(h + 1) * HD] = (o_s[:, h, :] * inv_own * onorm_ref[h:h + 1, :] * gate).astype(BF16)

    def drain(b, carry):
        o_copy(b).wait()
        return carry

    lax.fori_loop(0, B, drain, 0)


def lightning(hidden, g1, slopes, out_norm, lin_state, w_qkv, w_gate):
    return pl.pallas_call(
        lightning_kernel,
        out_shape=[jax.ShapeDtypeStruct((B, HL, HD, HD), F32), jax.ShapeDtypeStruct((B, HL * HD), BF16),
                   jax.ShapeDtypeStruct((B, HD), F32), jax.ShapeDtypeStruct((B, D), BF16)],
        in_specs=[any_spec()] * 7,
        out_specs=[any_spec(), vmem_spec(), vmem_spec(), vmem_spec()],
        scratch_shapes=[
            pltpu.VMEM((B, D), BF16),
            pltpu.VMEM((NC, HD), F32),
            pltpu.VMEM((HL, HD), F32),
            pltpu.SMEM((HL,), F32),
            pltpu.VMEM((RING, DCH, 3, HL, HD), BF16),
            pltpu.VMEM((RING, DCH, HL, HD), BF16),
            pltpu.VMEM((B, HL, HD, HD), F32),
            pltpu.VMEM((NC * B, HD), BF16),
            pltpu.VMEM((STEPS, B, DCH * HL), BF16),
            pltpu.VMEM((HL * B, DCH * HL), BF16),
            pltpu.VMEM((2, HL * B, 2 * HD), F32),
            pltpu.VMEM((HL, HD, 2 * B), BF16),
            pltpu.VMEM((HL, B, HD), BF16),
            pltpu.VMEM((B, HL, HD), F32),
            pltpu.SemaphoreType.DMA((4,)),
            pltpu.SemaphoreType.DMA((RING, 2)),
            pltpu.SemaphoreType.DMA((B,)),
            pltpu.SemaphoreType.DMA((B,)),
        ],
        compiler_params=pltpu.CompilerParams(vmem_limit_bytes=40 * MIB),
        name="lightning",
    )(hidden, g1, slopes, out_norm, lin_state, w_qkv, w_gate)


NCH = 4
CW = D // 2 // NCH


def peers():
    dp = lax.axis_index("dp")
    me = lax.axis_index("tp")
    core = lax.rem(me, 2)
    chip = me // 2
    mate = (dp, chip * 2 + (1 - core))
    across = (dp, (1 - chip) * 2 + core)
    return core, mate, across


def say_here(targets):
    barrier = pltpu.get_barrier_semaphore()
    for dev in targets:
        pl.semaphore_signal(barrier, inc=1, device_id=dev, device_id_type=MESH)


def await_peers(count):
    pl.semaphore_wait(pltpu.get_barrier_semaphore(), count)


def rcopy(src, dst, send, recv, dev):
    return pltpu.make_async_remote_copy(src_ref=src, dst_ref=dst, send_sem=send, recv_sem=recv,
                                        device_id=dev, device_id_type=MESH)


def exchange(left, wbuf, wwait, before_sends, pair_scale, mid_work, cross_scale, core, mate, across,
             a_send, a_recv, b_send, b_recv, total, sems):
    sa, ra, sb, rb, sc, rc = sems

    def product(half, j):
        wwait(half, j)
        at = half * NCH + j
        return jnp.concatenate([dot(left, wbuf[at, :, c:c + 2 * HD]) for c in range(0, CW, 2 * HD)], axis=1)

    a_copies = [rcopy(a_send.at[j], a_recv.at[j], sa.at[j], ra.at[j], mate) for j in range(NCH)]
    b_copies = [rcopy(b_send.at[j], b_recv.at[j], sb.at[j], rb.at[j], across) for j in range(NCH)]
    c_copies = [rcopy(total.at[core, j], total.at[core, j], sc.at[j], rc.at[j], mate) for j in range(NCH)]

    def send_across(j, scale):
        a_copies[j].wait_recv()
        b_send[j] = b_send[j] * scale[0] + a_recv[j] * scale[1] if scale else b_send[j] + a_recv[j]
        b_copies[j].start()

    scale = None
    for j in range(NCH):
        a_send[j] = product(1 - core, j)
        if j == 0:
            before_sends()
        a_copies[j].start()
        b_send[j] = product(core, j)
        if j == 1:
            scale = pair_scale()
        if j >= 1:
            send_across(j - 1, scale)
    send_across(NCH - 1, scale)
    mid_work()
    scale = cross_scale()
    for j in range(NCH):
        b_copies[j].wait_recv()
        total[core, j] = b_send[j] * scale[0] + b_recv[j] * scale[1] if scale else b_send[j] + b_recv[j]
        c_copies[j].start()
    for j in range(NCH):
        c_copies[j].wait_recv()
    for cp in a_copies + b_copies + c_copies:
        cp.wait_send()


def exchange_scratch():
    return [
        pltpu.VMEM((2 * NCH, HL * HD, CW), BF16),
        pltpu.VMEM((NCH, B, CW), F32),
        pltpu.VMEM((NCH, B, CW), F32),
        pltpu.VMEM((NCH, B, CW), F32),
        pltpu.VMEM((NCH, B, CW), F32),
        pltpu.VMEM((2, NCH, B, CW), F32),
        pltpu.SemaphoreType.DMA((2 * NCH,)),
        pltpu.SemaphoreType.DMA((NCH,)),
        pltpu.SemaphoreType.DMA((NCH,)),
        pltpu.SemaphoreType.DMA((NCH,)),
        pltpu.SemaphoreType.DMA((NCH,)),
        pltpu.SemaphoreType.DMA((NCH,)),
        pltpu.SemaphoreType.DMA((NCH,)),
    ]


def out_weights(w_ref, wbuf, wsem, core):
    def copy(half, j):
        at = half * NCH + j
        cols = pl.ds(pl.multiple_of(at * CW, CW), CW)
        return pltpu.make_async_copy(w_ref.at[:, cols], wbuf.at[at], wsem.at[at])

    def start():
        for j in range(NCH):
            copy(1 - core, j).start()
            copy(core, j).start()

    def wait(half, j):
        copy(half, j).wait()

    return start, wait


WA_ROWS = D * KV * (GQ + 2)
WA_CH = 32
WA_STEP = WA_ROWS // WA_CH
NJ = KV * (GQ + 2)


def mid_kernel(og_ref, ss_ref, h1_ref, g2_ref, alpha_ref, beta_ref, len_ref, wout_ref, wattn_ref,
               k_ref, v_ref, q_ref, kn_ref, vn_ref, h2_ref, kbuf, vbuf,
               wbuf, a_send, a_recv, b_send, b_recv, total, wsem, sa, ra, sb, rb, sc, rc,
               wraw, wide, w2, ss_recv, ss_chip, wasem, ss_s, ss_r, csem):
    core, mate, across = peers()
    start_w, wait_w = out_weights(wout_ref, wbuf, wsem, core)
    start_w()

    def wa_copy(i):
        return pltpu.make_async_copy(wattn_ref.at[pl.ds(i * WA_STEP, WA_STEP)], wraw.at[i], wasem.at[i])

    def wa_start(i, carry):
        wa_copy(i).start()
        return carry

    lax.fori_loop(0, WA_CH, wa_start, 0)
    caches = [pltpu.make_async_copy(k_ref, kbuf, csem.at[0]), pltpu.make_async_copy(v_ref, vbuf, csem.at[1])]
    for cp in caches:
        cp.start()
    say_here((mate, across))
    ss_mate = rcopy(ss_ref, ss_recv.at[0], ss_s.at[0], ss_r.at[0], mate)
    ss_across = rcopy(ss_chip, ss_recv.at[1], ss_s.at[1], ss_r.at[1], across)

    def before_sends():
        await_peers(2)
        ss_mate.start()

    def root(total_sq, count):
        return jnp.minimum(jnp.sqrt(total_sq[:, 0:1] / count + EPS), 3e38)

    def pair_scale():
        ss_mate.wait_recv()
        both = ss_ref[...] + ss_recv[0]
        ss_chip[...] = both
        ss_across.start()
        inv = lax.rsqrt(both[:, 0:1] / (D // 2) + EPS)
        return root(ss_ref[...], D // 4) * inv, root(ss_recv[0], D // 4) * inv

    def cross_scale():
        ss_across.wait_recv()
        inv = lax.rsqrt((ss_chip[:, 0:1] + ss_recv[1, :, 0:1]) / D + EPS)
        return root(ss_chip[...], D // 2) * inv, root(ss_recv[1], D // 2) * inv

    def relayout():
        def body(i, carry):
            wa_copy(i).wait()
            wide[...] = wraw[i].astype(F32)
            for j in range(NJ):
                w2[j, pl.ds(pl.multiple_of(i * HD, HD), HD), :] = wide[pl.ds(j, HD, stride=NJ), :].astype(BF16)
            return carry
        lax.fori_loop(0, WA_CH, body, 0)

    exchange(og_ref[...], wbuf, wait_w, before_sends, pair_scale, relayout, cross_scale, core, mate, across,
             a_send, a_recv, b_send, b_recv, total, (sa, ra, sb, rb, sc, rc))
    ss_mate.wait_send()
    ss_across.wait_send()

    per = CW // HD
    alpha = alpha_ref[0]
    beta = beta_ref[0]
    sq = jnp.zeros((B, HD), F32)
    mids = []
    for c in range(NC):
        a1 = total[c // (NC // 2), (c % (NC // 2)) // per, :, (c % per) * HD:(c % per + 1) * HD]
        m = (alpha * h1_ref[:, c * HD:(c + 1) * HD].astype(F32) + beta * a1).astype(BF16)
        h2_ref[:, c * HD:(c + 1) * HD] = m
        x = m.astype(F32)
        sq = sq + x * x
    inv2 = lax.rsqrt(jnp.sum(sq, axis=1, keepdims=True) / D + EPS)
    for c in range(NC):
        m = h2_ref[:, c * HD:(c + 1) * HD].astype(F32)
        h2_ref[:, c * HD:(c + 1) * HD] = (m * inv2 * g2_ref[c:c + 1, :]).astype(BF16)

    pos = jnp.zeros((B, HD), F32)
    row_i = lax.broadcasted_iota(jnp.int32, (B, HD), 0)
    for b in range(B):
        pos = jnp.where(row_i == b, jnp.full((B, HD), len_ref[b]).astype(F32), pos)
    lane = lax.broadcasted_iota(jnp.int32, (B, HD), 1)
    freq = jnp.exp((lane % 32).astype(F32) * (-2.0 * math.log(ROPE_BASE) / 64))
    ang = pos * freq
    rot = lane < 64
    cosv = jnp.where(rot, jnp.cos(ang), 1.0)
    sinv = jnp.sin(ang)
    sin_lo = jnp.where(lane < 32, -sinv, 0.0)
    sin_hi = jnp.where((lane >= 32) & rot, sinv, 0.0)

    def turn(x):
        return x * cosv + pltpu.roll(x, HD - 32, 1) * sin_lo + pltpu.roll(x, 32, 1) * sin_hi

    h2 = h2_ref[...]
    for j in range(GQ + 2):
        w = jnp.concatenate([w2[2 * j], w2[2 * j + 1]], axis=1)
        pr = dot(h2, w)
        for kv in range(KV):
            x = pr[:, kv * HD:(kv + 1) * HD]
            if j < GQ:
                q_ref[pl.ds(kv * GQ + j, B, stride=8), :] = turn(x).astype(BF16).astype(F32)
            elif j == GQ:
                kn_ref[kv] = turn(x).astype(BF16).astype(F32)
            else:
                vn_ref[kv] = x.astype(BF16).astype(F32)
    for cp in caches:
        cp.wait()


def middle(og, ss, h1, g2, alpha, beta, cache_len, w_out, w_attn, k_cache, v_cache):
    return pl.pallas_call(
        mid_kernel,
        out_shape=[jax.ShapeDtypeStruct((B * 8, HD), F32), jax.ShapeDtypeStruct((KV, B, HD), F32),
                   jax.ShapeDtypeStruct((KV, B, HD), F32), jax.ShapeDtypeStruct((B, D), BF16),
                   pltpu.VMEM((B, KV, T, HD), BF16), pltpu.VMEM((B, KV, T, HD), BF16)],
        in_specs=[vmem_spec(), vmem_spec(), vmem_spec(), vmem_spec(), smem_spec(), smem_spec(), smem_spec(),
                  any_spec(), any_spec(), any_spec(), any_spec()],
        out_specs=[vmem_spec()] * 6,
        scratch_shapes=exchange_scratch() + [
            pltpu.VMEM((WA_CH, WA_STEP, HD), BF16),
            pltpu.VMEM((WA_STEP, HD), F32),
            pltpu.VMEM((NJ, D, HD), BF16),
            pltpu.VMEM((2, B, HD), F32),
            pltpu.VMEM((B, HD), F32),
            pltpu.SemaphoreType.DMA((WA_CH,)),
            pltpu.SemaphoreType.DMA((2,)),
            pltpu.SemaphoreType.DMA((2,)),
            pltpu.SemaphoreType.DMA((2,)),
        ],
        compiler_params=pltpu.CompilerParams(vmem_limit_bytes=37 * MIB, collective_id=0, has_side_effects=True),
        name="middle",
    )(og, ss, h1, g2, alpha, beta, cache_len, w_out, w_attn, k_cache, v_cache)


ROWS = 4


def attention_kernel(len_ref, q_ref, kn_ref, vn_ref, kin_ref, vin_ref, at_ref, ko_ref, vo_ref, kbuf, vbuf, osem):
    def outs(b):
        return (pltpu.make_async_copy(kbuf.at[b], ko_ref.at[b], osem.at[0, b]),
                pltpu.make_async_copy(vbuf.at[b], vo_ref.at[b], osem.at[1, b]))

    row8 = lax.broadcasted_iota(jnp.int32, (8, HD), 0)
    row16 = lax.broadcasted_iota(jnp.int32, (16, HD), 0)
    tpos = lax.broadcasted_iota(jnp.int32, (8, T), 1)

    def insert(i, carry):
        rows = [i * ROWS + r for r in range(ROWS)]
        for b in rows:
            p = len_ref[b]
            base = pl.multiple_of((p // 16) * 16, 16)
            hit = row16 == p - base
            for kv in range(KV):
                for buf, new in ((kbuf, kn_ref), (vbuf, vn_ref)):
                    old = buf[b, kv, pl.ds(base, 16), :].astype(F32)
                    buf[b, kv, pl.ds(base, 16), :] = jnp.where(hit, new[kv, pl.ds(b, 1), :], old).astype(BF16)
        for b in rows:
            for cp in outs(b):
                cp.start()
        return carry

    lax.fori_loop(0, B // ROWS, insert, 0)

    def body(i, carry):
        rows = [i * ROWS + r for r in range(ROWS)]
        lens = [len_ref[b] for b in rows]
        scores = []
        for b, p in zip(rows, lens):
            q = q_ref[pl.ds(b * 8, 8), :]
            q2 = jnp.concatenate([jnp.where(row8 < 4, q, 0.0), jnp.where(row8 < 4, 0.0, q)], axis=1).astype(BF16)
            k2 = jnp.concatenate([kbuf[b, 0], kbuf[b, 1]], axis=1)
            s = lax.dot_general(q2, k2, (((1,), (1,)), ((), ())), preferred_element_type=F32) * HD ** -0.5
            scores.append(jnp.where(tpos <= p, s, -jnp.inf))
        tops = [jnp.max(s, axis=1, keepdims=True) for s in scores]
        es = [jnp.exp(s - m) for s, m in zip(scores, tops)]
        sums = [jnp.sum(e, axis=1, keepdims=True) for e in es]
        prs = [(e / z).astype(BF16) for e, z in zip(es, sums)]
        for b, pr in zip(rows, prs):
            o = dot(pr, jnp.concatenate([vbuf[b, 0], vbuf[b, 1]], axis=1))
            at_ref[pl.ds(b * 8, 8), :] = jnp.where(row8 < 4, o[:, 0:HD], o[:, HD:])
        return carry

    lax.fori_loop(0, B // ROWS, body, 0)

    def drain(b, carry):
        for cp in outs(b):
            cp.wait()
        return carry

    lax.fori_loop(0, B, drain, 0)


def attention(cache_len, q, kn, vn, kbuf, vbuf):
    return pl.pallas_call(
        attention_kernel,
        out_shape=[jax.ShapeDtypeStruct((B * 8, HD), F32), pltpu.HBM((B, KV, T, HD), BF16),
                   pltpu.HBM((B, KV, T, HD), BF16), pltpu.VMEM((B, KV, T, HD), BF16), pltpu.VMEM((B, KV, T, HD), BF16)],
        in_specs=[smem_spec(), vmem_spec(), vmem_spec(), vmem_spec(), vmem_spec(), vmem_spec()],
        out_specs=[vmem_spec(), any_spec(), any_spec(), vmem_spec(), vmem_spec()],
        input_output_aliases={4: 3, 5: 4},
        scratch_shapes=[pltpu.SemaphoreType.DMA((2, B))],
        compiler_params=pltpu.CompilerParams(vmem_limit_bytes=4 * MIB),
        name="attention",
    )(cache_len, q, kn, vn, kbuf, vbuf)[:3]


def last_kernel(at_ref, h2_ref, alpha_ref, beta_ref, wout_ref, out_ref,
                wbuf, a_send, a_recv, b_send, b_recv, total, wsem, sa, ra, sb, rb, sc, rc):
    core, mate, across = peers()
    start_w, wait_w = out_weights(wout_ref, wbuf, wsem, core)
    start_w()
    say_here((mate, across))
    left = jnp.concatenate([at_ref[pl.ds(j, B, stride=8), :].astype(BF16) for j in range(8)], axis=1)
    exchange(left, wbuf, wait_w, lambda: await_peers(2), lambda: None, lambda: None, lambda: None, core, mate, across,
             a_send, a_recv, b_send, b_recv, total, (sa, ra, sb, rb, sc, rc))
    per = CW // HD
    alpha = alpha_ref[1]
    beta = beta_ref[1]
    for c in range(NC):
        a2 = total[c // (NC // 2), (c % (NC // 2)) // per, :, (c % per) * HD:(c % per + 1) * HD]
        cols = slice(c * HD, (c + 1) * HD)
        out_ref[:, cols] = (alpha * h2_ref[:, cols].astype(F32) + beta * a2).astype(BF16)


def last(at, h2, alpha, beta, w_out):
    return pl.pallas_call(
        last_kernel,
        out_shape=jax.ShapeDtypeStruct((B, D), BF16),
        in_specs=[vmem_spec(), vmem_spec(), smem_spec(), smem_spec(), any_spec()],
        out_specs=vmem_spec(),
        scratch_shapes=exchange_scratch(),
        compiler_params=pltpu.CompilerParams(vmem_limit_bytes=16 * MIB, collective_id=1, has_side_effects=True),
        name="last",
    )(at, h2, alpha, beta, w_out)


def solution(mesh):
    row_spec = P('dp', None)
    cache_spec = P('dp', 'tp', None, None)
    in_specs = (row_spec, P('dp'), cache_spec, cache_spec, cache_spec, P(None), P(None, None, 'tp', None),
                P(None, 'tp', None), P('tp'), P('tp', None), P('tp', None, None), P(None),
                P(None, 'tp', None, None), P('tp', None, None), P(None), P(None))
    out_specs = (row_spec, cache_spec, cache_spec, cache_spec)

    def local_step(hidden, cache_len, lin_state, k_cache, v_cache, norm_first, w_qkv, w_gate, slopes, out_norm,
                   w_out_lin, norm_second, w_attn, w_out_attn, mix_alpha, mix_beta):
        def hbm(x):
            return pltpu.with_memory_space_constraint(x, pltpu.HBM)

        g1 = norm_first.reshape(NC, HD)
        g2 = norm_second.reshape(NC, HD)
        wa = jnp.transpose(w_attn, (0, 2, 1, 3)).reshape(WA_ROWS, HD)
        state_out, og, ss, h1 = lightning(hbm(hidden), hbm(g1), hbm(slopes), hbm(out_norm), hbm(lin_state), hbm(w_qkv), hbm(w_gate))
        q, kn, vn, h2, kbuf, vbuf = middle(og, ss, h1, g2, mix_alpha, mix_beta, cache_len,
                                           hbm(w_out_lin.reshape(HL * HD, D)), hbm(wa), hbm(k_cache), hbm(v_cache))
        at, k_out, v_out = attention(cache_len, q, kn, vn, kbuf, vbuf)
        hidden_out = last(at, h2, mix_alpha, mix_beta, hbm(w_out_attn.reshape(HL * HD, D)))
        return hidden_out, state_out, k_out, v_out

    return jax.shard_map(local_step, mesh=mesh, in_specs=in_specs, out_specs=out_specs, check_vma=False)
```

```python
import functools
import math

import jax
import jax.numpy as jnp
from jax import lax
from jax.experimental import pallas as pl
from jax.experimental.pallas import tpu as pltpu
from jax.sharding import PartitionSpec as P

EPS = 1e-5
ROPE_BASE = 10000000.0
MESH = pl.DeviceIdType.MESH
F32 = jnp.float32
BF16 = jnp.bfloat16
MIB = 1024 * 1024

B = 32
D = 4096
HL = 8
HD = 128
KV = 2
GQ = 4
T = 512
NC = D // HD

DCH = 256
STEPS = D // DCH
RING = 4
EARLY = 12


def any_spec():
    return pl.BlockSpec(memory_space=pl.ANY)


def vmem_spec():
    return pl.BlockSpec(memory_space=pltpu.VMEM)


def smem_spec():
    return pl.BlockSpec(memory_space=pltpu.SMEM)


def dot(a, b):
    return jnp.dot(a, b, preferred_element_type=F32)


def lightning_kernel(hid_hbm, g1_hbm, slopes_hbm, onorm_hbm, state_ref, wqkv_ref, wgate_ref,
                     sout_ref, og_ref, ss_ref, h1_ref, hid_ref, g1_ref, onorm_ref, slopes_ref,
                     wbuf, gbuf, sbuf, hstack, ebuf, lbuf_a, lbuf_b, acc, kq_t, v_s, o_s, psem, wsem, ssem, osem):
    def w_copies(step, slot):
        rows = pl.ds(step * DCH, DCH)
        return (pltpu.make_async_copy(wqkv_ref.at[rows], wbuf.at[slot], wsem.at[slot, 0]),
                pltpu.make_async_copy(wgate_ref.at[rows], gbuf.at[slot], wsem.at[slot, 1]))

    def s_copy(b):
        return pltpu.make_async_copy(state_ref.at[b], sbuf.at[b], ssem.at[b])

    def o_copy(b):
        return pltpu.make_async_copy(sbuf.at[b], sout_ref.at[b], osem.at[b])

    small = [pltpu.make_async_copy(src, dst, psem.at[n]) for n, (src, dst) in enumerate(
        ((hid_hbm, hid_ref), (g1_hbm, g1_ref), (onorm_hbm, onorm_ref), (slopes_hbm, slopes_ref)))]
    for cp in small:
        cp.start()
    for i in range(RING):
        for cp in w_copies(i, i):
            cp.start()
    for cp in small:
        cp.wait()

    sq = jnp.zeros((B, HD), F32)
    for c in range(NC):
        x = hid_ref[:, c * HD:(c + 1) * HD].astype(F32)
        sq = sq + x * x
    inv = lax.rsqrt(jnp.sum(sq, axis=1, keepdims=True) / D + EPS)
    rr = lax.broadcasted_iota(jnp.int32, (HD, 256), 1)
    dd = lax.broadcasted_iota(jnp.int32, (HD, 256), 0)
    for c in range(NC):
        x = hid_ref[:, c * HD:(c + 1) * HD].astype(F32)
        h1 = (x * inv * g1_ref[c:c + 1, :]).astype(BF16)
        h1_ref[:, c * HD:(c + 1) * HD] = h1
        hstack[c * B:(c + 1) * B, :] = h1
    for n in range(4):
        spread = jnp.where(rr // 8 + 32 * n == dd, 1.0, 0.0).astype(BF16)
        for c in range(NC // 8):
            e = dot(hstack[c * 256:(c + 1) * 256, :], spread).astype(BF16)
            for k in range(8):
                cc = c * 8 + k
                off = (cc % (DCH // HD)) * 1024 + n * 256
                ebuf[cc // (DCH // HD), :, off:off + 256] = e[k * B:(k + 1) * B, :]

    acc[...] = jnp.zeros_like(acc)
    half = DCH * HL // 2
    lane = lax.broadcasted_iota(jnp.int32, (B, half), 1) % 8

    def spread_heads(dst, i, part):
        e = ebuf[i, :, part * half:(part + 1) * half]
        for h in range(HL):
            keep = jnp.where(lane == h, 1.0, 0.0).astype(BF16)
            dst[h * B:(h + 1) * B, :] = e * keep

    spread_heads(lbuf_a, 0, 0)

    def step_fn(i, carry):
        slot = lax.rem(i, RING)

        @pl.when(i >= STEPS - EARLY // 2)
        def _():
            for k in range(2):
                s_copy((i - (STEPS - EARLY // 2)) * 2 + k).start()

        for cp in w_copies(i, slot):
            cp.wait()

        def product(left, part, pair):
            rows = slice(part * DCH // 2, (part + 1) * DCH // 2)
            second = wbuf[slot, rows, 1] if pair == 0 else gbuf[slot, rows]
            right = jnp.concatenate([wbuf[slot, rows, 2 * pair].reshape(half, HD), second.reshape(half, HD)], axis=1)
            return dot(left, right)

        spread_heads(lbuf_b, i, 1)
        left_a = lbuf_a[...]
        first = [product(left_a, 0, pair) for pair in range(2)]
        spread_heads(lbuf_a, jnp.minimum(i + 1, STEPS - 1), 0)
        left_b = lbuf_b[...]
        for pair in range(2):
            acc[pair] += first[pair] + product(left_b, 1, pair)

        @pl.when(i + RING < STEPS)
        def _():
            for cp in w_copies(i + RING, slot):
                cp.start()
        return carry

    lax.fori_loop(0, STEPS, step_fn, 0)
    for b in range(EARLY, B):
        s_copy(b).start()

    for h in range(HL):
        rows = slice(h * B, (h + 1) * B)
        q = jax.nn.silu(acc[0, rows, 0:HD]).astype(BF16)
        k = jax.nn.silu(acc[0, rows, HD:2 * HD]).astype(BF16)
        v = jax.nn.silu(acc[1, rows, 0:HD]).astype(BF16)
        qk = jnp.concatenate([k, q], axis=0).astype(F32)
        both = jnp.transpose(qk).astype(BF16)
        kq_t[h] = jnp.concatenate([both[:, 0:B], both[:, B:]], axis=0)
        v_s[h] = v.astype(F32)

    brow = lax.broadcasted_iota(jnp.int32, (B, 2 * HD), 0)
    bcol = lax.broadcasted_iota(jnp.int32, (B, 2 * HD), 1) // HD

    def row_fn(i, carry):
        for r in range(2):
            s_copy(2 * i + r).wait()
        pick = jnp.where(brow == 2 * i + bcol, 1.0, 0.0).astype(BF16)
        for h in range(HL):
            kq = dot(kq_t[h], pick)
            decay = jnp.exp(jnp.full((1, HD), -slopes_ref[h], F32))
            for r in range(2):
                b = 2 * i + r
                lanes = slice(r * HD, (r + 1) * HD)
                new = decay * sbuf[b, h] + kq[0:HD, lanes] * v_s[h, pl.ds(b, 1), :]
                sbuf[b, h] = new
                o_s[b, h:h + 1, :] = jnp.sum(kq[HD:, lanes] * new, axis=0, keepdims=True)
        for r in range(2):
            o_copy(2 * i + r).start()
        return carry

    lax.fori_loop(0, B // 2, row_fn, 0)

    ss = jnp.zeros((B, HD), F32)
    for h in range(HL):
        o = o_s[:, h, :]
        ss = ss + o * o
    ss = jnp.sum(ss, axis=1, keepdims=True)
    ss_ref[...] = jnp.broadcast_to(ss, (B, HD))
    inv_own = lax.rsqrt(ss / (HL * HD) + EPS)
    for h in range(HL):
        gate = jax.nn.sigmoid(acc[1, h * B:(h + 1) * B, HD:2 * HD])
        og_ref[:, h * HD:(h + 1) * HD] = (o_s[:, h, :] * inv_own * onorm_ref[h:h + 1, :] * gate).astype(BF16)

    def drain(b, carry):
        o_copy(b).wait()
        return carry

    lax.fori_loop(0, B, drain, 0)


def lightning(hidden, g1, slopes, out_norm, lin_state, w_qkv, w_gate):
    return pl.pallas_call(
        lightning_kernel,
        out_shape=[jax.ShapeDtypeStruct((B, HL, HD, HD), F32), jax.ShapeDtypeStruct((B, HL * HD), BF16),
                   jax.ShapeDtypeStruct((B, HD), F32), jax.ShapeDtypeStruct((B, D), BF16)],
        in_specs=[any_spec()] * 7,
        out_specs=[any_spec(), vmem_spec(), vmem_spec(), vmem_spec()],
        scratch_shapes=[
            pltpu.VMEM((B, D), BF16),
            pltpu.VMEM((NC, HD), F32),
            pltpu.VMEM((HL, HD), F32),
            pltpu.SMEM((HL,), F32),
            pltpu.VMEM((RING, DCH, 3, HL, HD), BF16),
            pltpu.VMEM((RING, DCH, HL, HD), BF16),
            pltpu.VMEM((B, HL, HD, HD), F32),
            pltpu.VMEM((NC * B, HD), BF16),
            pltpu.VMEM((STEPS, B, DCH * HL), BF16),
            pltpu.VMEM((HL * B, DCH * HL // 2), BF16),
            pltpu.VMEM((HL * B, DCH * HL // 2), BF16),
            pltpu.VMEM((2, HL * B, 2 * HD), F32),
            pltpu.VMEM((HL, 2 * HD, B), BF16),
            pltpu.VMEM((HL, B, HD), F32),
            pltpu.VMEM((B, HL, HD), F32),
            pltpu.SemaphoreType.DMA((4,)),
            pltpu.SemaphoreType.DMA((RING, 2)),
            pltpu.SemaphoreType.DMA((B,)),
            pltpu.SemaphoreType.DMA((B,)),
        ],
        compiler_params=pltpu.CompilerParams(vmem_limit_bytes=40 * MIB),
        name="lightning",
    )(hidden, g1, slopes, out_norm, lin_state, w_qkv, w_gate)


NCH = 4
CW = D // 2 // NCH


def peers():
    dp = lax.axis_index("dp")
    me = lax.axis_index("tp")
    core = lax.rem(me, 2)
    chip = me // 2
    mate = (dp, chip * 2 + (1 - core))
    across = (dp, (1 - chip) * 2 + core)
    return core, mate, across


def say_here(targets):
    barrier = pltpu.get_barrier_semaphore()
    for dev in targets:
        pl.semaphore_signal(barrier, inc=1, device_id=dev, device_id_type=MESH)


def await_peers(count):
    pl.semaphore_wait(pltpu.get_barrier_semaphore(), count)


def rcopy(src, dst, send, recv, dev):
    return pltpu.make_async_remote_copy(src_ref=src, dst_ref=dst, send_sem=send, recv_sem=recv,
                                        device_id=dev, device_id_type=MESH)


def exchange(left, wbuf, wwait, before_sends, pair_scale, mid_work, cross_scale, core, mate, across,
             a_send, a_recv, b_send, b_recv, total, sems, first=None):
    sa, ra, sb, rb, sc, rc = sems

    def product(half, j):
        wwait(half, j)
        buf, at = (wbuf, half * NCH + j) if first is None or j > 0 else (first, half)
        return jnp.concatenate([dot(left, buf[at, :, c:c + 2 * HD]) for c in range(0, CW, 2 * HD)], axis=1)

    a_copies = [rcopy(a_send.at[j], a_recv.at[j], sa.at[j], ra.at[j], mate) for j in range(NCH)]
    b_copies = [rcopy(b_send.at[j], b_recv.at[j], sb.at[j], rb.at[j], across) for j in range(NCH)]
    c_copies = [rcopy(total.at[core, j], total.at[core, j], sc.at[j], rc.at[j], mate) for j in range(NCH)]

    def send_across(j, scale):
        a_copies[j].wait_recv()
        b_send[j] = b_send[j] * scale[0] + a_recv[j] * scale[1] if scale else b_send[j] + a_recv[j]
        b_copies[j].start()

    scale = None
    for j in range(NCH):
        a_send[j] = product(1 - core, j)
        if j == 0:
            before_sends()
        a_copies[j].start()
        b_send[j] = product(core, j)
        if j == 1:
            scale = pair_scale()
        if j >= 1:
            send_across(j - 1, scale)
    send_across(NCH - 1, scale)
    mid_work()
    scale = cross_scale()
    for j in range(NCH):
        b_copies[j].wait_recv()
        total[core, j] = b_send[j] * scale[0] + b_recv[j] * scale[1] if scale else b_send[j] + b_recv[j]
        c_copies[j].start()
    for j in range(NCH):
        c_copies[j].wait_recv()
    for cp in a_copies + b_copies + c_copies:
        cp.wait_send()


def exchange_scratch():
    return [
        pltpu.VMEM((2 * NCH, HL * HD, CW), BF16),
        pltpu.VMEM((NCH, B, CW), F32),
        pltpu.VMEM((NCH, B, CW), F32),
        pltpu.VMEM((NCH, B, CW), F32),
        pltpu.VMEM((NCH, B, CW), F32),
        pltpu.VMEM((2, NCH, B, CW), F32),
        pltpu.SemaphoreType.DMA((2 * NCH,)),
        pltpu.SemaphoreType.DMA((NCH,)),
        pltpu.SemaphoreType.DMA((NCH,)),
        pltpu.SemaphoreType.DMA((NCH,)),
        pltpu.SemaphoreType.DMA((NCH,)),
        pltpu.SemaphoreType.DMA((NCH,)),
        pltpu.SemaphoreType.DMA((NCH,)),
    ]


def out_weights(w_ref, wbuf, wsem, core, begin=0):
    def copy(half, j):
        at = half * NCH + j
        cols = pl.ds(pl.multiple_of(at * CW, CW), CW)
        return pltpu.make_async_copy(w_ref.at[:, cols], wbuf.at[at], wsem.at[at])

    def start():
        for j in range(begin, NCH):
            copy(1 - core, j).start()
            copy(core, j).start()

    def wait(half, j):
        if j >= begin:
            copy(half, j).wait()

    return start, wait


WA_ROWS = D * KV * (GQ + 2)
WA_CH = 32
WA_STEP = WA_ROWS // WA_CH
NJ = KV * (GQ + 2)


def mid_kernel(og_ref, ss_ref, h1_ref, g2_ref, alpha_ref, beta_ref, len_ref, wout_ref, wattn_ref,
               k_ref, v_ref, wnext_ref, q_ref, kn_ref, vn_ref, h2_ref, kbuf, vbuf, wnext,
               wbuf, a_send, a_recv, b_send, b_recv, total, wsem, sa, ra, sb, rb, sc, rc,
               wraw, wide, w2, ss_recv, ss_chip, wasem, ss_s, ss_r, csem):
    core, mate, across = peers()
    say_here((mate, across))
    start_w, wait_w = out_weights(wout_ref, wbuf, wsem, core)
    start_w()

    def wa_copy(i):
        return pltpu.make_async_copy(wattn_ref.at[pl.ds(i * WA_STEP, WA_STEP)], wraw.at[i], wasem.at[i])

    def wa_start(i, carry):
        wa_copy(i).start()
        return carry

    lax.fori_loop(0, WA_CH, wa_start, 0)
    caches = [pltpu.make_async_copy(k_ref, kbuf, csem.at[0]), pltpu.make_async_copy(v_ref, vbuf, csem.at[1])]
    caches += [pltpu.make_async_copy(wnext_ref.at[:, pl.ds(h * (D // 2), CW)], wnext.at[h], csem.at[2 + h]) for h in range(2)]
    for cp in caches:
        cp.start()
    ss_mate = rcopy(ss_ref, ss_recv.at[0], ss_s.at[0], ss_r.at[0], mate)
    ss_across = rcopy(ss_chip, ss_recv.at[1], ss_s.at[1], ss_r.at[1], across)

    def before_sends():
        await_peers(2)
        ss_mate.start()

    def root(total_sq, count):
        return jnp.minimum(jnp.sqrt(total_sq[:, 0:1] / count + EPS), 3e38)

    def pair_scale():
        ss_mate.wait_recv()
        both = ss_ref[...] + ss_recv[0]
        ss_chip[...] = both
        ss_across.start()
        inv = lax.rsqrt(both[:, 0:1] / (D // 2) + EPS)
        return root(ss_ref[...], D // 4) * inv, root(ss_recv[0], D // 4) * inv

    def cross_scale():
        ss_across.wait_recv()
        inv = lax.rsqrt((ss_chip[:, 0:1] + ss_recv[1, :, 0:1]) / D + EPS)
        return root(ss_chip[...], D // 2) * inv, root(ss_recv[1], D // 2) * inv

    def relayout():
        def body(i, carry):
            wa_copy(i).wait()
            wide[...] = wraw[i].astype(F32)
            for j in range(NJ):
                w2[j, pl.ds(pl.multiple_of(i * HD, HD), HD), :] = wide[pl.ds(j, HD, stride=NJ), :].astype(BF16)
            return carry
        lax.fori_loop(0, WA_CH, body, 0)

    exchange(og_ref[...], wbuf, wait_w, before_sends, pair_scale, relayout, cross_scale, core, mate, across,
             a_send, a_recv, b_send, b_recv, total, (sa, ra, sb, rb, sc, rc))
    ss_mate.wait_send()
    ss_across.wait_send()

    per = CW // HD
    alpha = alpha_ref[0]
    beta = beta_ref[0]
    sq = jnp.zeros((B, HD), F32)
    mids = []
    for c in range(NC):
        a1 = total[c // (NC // 2), (c % (NC // 2)) // per, :, (c % per) * HD:(c % per + 1) * HD]
        m = (alpha * h1_ref[:, c * HD:(c + 1) * HD].astype(F32) + beta * a1).astype(BF16)
        h2_ref[:, c * HD:(c + 1) * HD] = m
        x = m.astype(F32)
        sq = sq + x * x
    inv2 = lax.rsqrt(jnp.sum(sq, axis=1, keepdims=True) / D + EPS)
    for c in range(NC):
        m = h2_ref[:, c * HD:(c + 1) * HD].astype(F32)
        h2_ref[:, c * HD:(c + 1) * HD] = (m * inv2 * g2_ref[c:c + 1, :]).astype(BF16)

    pos = jnp.zeros((B, HD), F32)
    row_i = lax.broadcasted_iota(jnp.int32, (B, HD), 0)
    for b in range(B):
        pos = jnp.where(row_i == b, jnp.full((B, HD), len_ref[b]).astype(F32), pos)
    lane = lax.broadcasted_iota(jnp.int32, (B, HD), 1)
    freq = jnp.exp((lane % 32).astype(F32) * (-2.0 * math.log(ROPE_BASE) / 64))
    ang = pos * freq
    rot = lane < 64
    cosv = jnp.where(rot, jnp.cos(ang), 1.0)
    sinv = jnp.sin(ang)
    sin_lo = jnp.where(lane < 32, -sinv, 0.0)
    sin_hi = jnp.where((lane >= 32) & rot, sinv, 0.0)

    def turn(x):
        return x * cosv + pltpu.roll(x, HD - 32, 1) * sin_lo + pltpu.roll(x, 32, 1) * sin_hi

    h2 = h2_ref[...]
    for j in range(GQ + 2):
        w = jnp.concatenate([w2[2 * j], w2[2 * j + 1]], axis=1)
        pr = dot(h2, w)
        for kv in range(KV):
            x = pr[:, kv * HD:(kv + 1) * HD]
            if j < GQ:
                q_ref[pl.ds(kv * GQ + j, B, stride=8), :] = turn(x).astype(BF16).astype(F32)
            elif j == GQ:
                kn_ref[kv] = turn(x).astype(BF16).astype(F32)
            else:
                vn_ref[kv] = x.astype(BF16).astype(F32)
    for cp in caches:
        cp.wait()


def middle(og, ss, h1, g2, alpha, beta, cache_len, w_out, w_attn, k_cache, v_cache, w_next):
    return pl.pallas_call(
        mid_kernel,
        out_shape=[jax.ShapeDtypeStruct((B * 8, HD), F32), jax.ShapeDtypeStruct((KV, B, HD), F32),
                   jax.ShapeDtypeStruct((KV, B, HD), F32), jax.ShapeDtypeStruct((B, D), BF16),
                   pltpu.VMEM((B, KV, T, HD), BF16), pltpu.VMEM((B, KV, T, HD), BF16),
                   pltpu.VMEM((2, HL * HD, CW), BF16)],
        in_specs=[vmem_spec(), vmem_spec(), vmem_spec(), vmem_spec(), smem_spec(), smem_spec(), smem_spec(),
                  any_spec(), any_spec(), any_spec(), any_spec(), any_spec()],
        out_specs=[vmem_spec()] * 7,
        scratch_shapes=exchange_scratch() + [
            pltpu.VMEM((WA_CH, WA_STEP, HD), BF16),
            pltpu.VMEM((WA_STEP, HD), F32),
            pltpu.VMEM((NJ, D, HD), BF16),
            pltpu.VMEM((2, B, HD), F32),
            pltpu.VMEM((B, HD), F32),
            pltpu.SemaphoreType.DMA((WA_CH,)),
            pltpu.SemaphoreType.DMA((2,)),
            pltpu.SemaphoreType.DMA((2,)),
            pltpu.SemaphoreType.DMA((4,)),
        ],
        compiler_params=pltpu.CompilerParams(vmem_limit_bytes=37 * MIB, collective_id=0, has_side_effects=True),
        name="middle",
    )(og, ss, h1, g2, alpha, beta, cache_len, w_out, w_attn, k_cache, v_cache, w_next)


ROWS = 4


def attention_kernel(len_ref, q_ref, kn_ref, vn_ref, kin_ref, vin_ref, at_ref, ko_ref, vo_ref, kbuf, vbuf, osem):
    def outs(b):
        return (pltpu.make_async_copy(kbuf.at[b], ko_ref.at[b], osem.at[0, b]),
                pltpu.make_async_copy(vbuf.at[b], vo_ref.at[b], osem.at[1, b]))

    row8 = lax.broadcasted_iota(jnp.int32, (8, HD), 0)
    row16 = lax.broadcasted_iota(jnp.int32, (16, HD), 0)
    tpos = lax.broadcasted_iota(jnp.int32, (8, T), 1)

    def insert(i, carry):
        rows = [i * ROWS + r for r in range(ROWS)]
        for b in rows:
            p = len_ref[b]
            base = pl.multiple_of((p // 16) * 16, 16)
            hit = row16 == p - base
            for kv in range(KV):
                for buf, new in ((kbuf, kn_ref), (vbuf, vn_ref)):
                    old = buf[b, kv, pl.ds(base, 16), :].astype(F32)
                    buf[b, kv, pl.ds(base, 16), :] = jnp.where(hit, new[kv, pl.ds(b, 1), :], old).astype(BF16)
        for b in rows:
            for cp in outs(b):
                cp.start()
        return carry

    lax.fori_loop(0, B // ROWS, insert, 0)

    def body(i, carry):
        rows = [i * ROWS + r for r in range(ROWS)]
        lens = [len_ref[b] for b in rows]
        scores = []
        for b, p in zip(rows, lens):
            q = q_ref[pl.ds(b * 8, 8), :]
            q2 = jnp.concatenate([jnp.where(row8 < 4, q, 0.0), jnp.where(row8 < 4, 0.0, q)], axis=1).astype(BF16)
            k2 = jnp.concatenate([kbuf[b, 0], kbuf[b, 1]], axis=1)
            s = lax.dot_general(q2, k2, (((1,), (1,)), ((), ())), preferred_element_type=F32) * HD ** -0.5
            scores.append(jnp.where(tpos <= p, s, -jnp.inf))
        tops = [jnp.max(s, axis=1, keepdims=True) for s in scores]
        es = [jnp.exp(s - m) for s, m in zip(scores, tops)]
        sums = [jnp.sum(e, axis=1, keepdims=True) for e in es]
        prs = [(e / z).astype(BF16) for e, z in zip(es, sums)]
        for b, pr in zip(rows, prs):
            o = dot(pr, jnp.concatenate([vbuf[b, 0], vbuf[b, 1]], axis=1))
            at_ref[pl.ds(b * 8, 8), :] = jnp.where(row8 < 4, o[:, 0:HD], o[:, HD:])
        return carry

    lax.fori_loop(0, B // ROWS, body, 0)

    def drain(b, carry):
        for cp in outs(b):
            cp.wait()
        return carry

    lax.fori_loop(0, B, drain, 0)


def attention(cache_len, q, kn, vn, kbuf, vbuf):
    return pl.pallas_call(
        attention_kernel,
        out_shape=[jax.ShapeDtypeStruct((B * 8, HD), F32), pltpu.HBM((B, KV, T, HD), BF16),
                   pltpu.HBM((B, KV, T, HD), BF16), pltpu.VMEM((B, KV, T, HD), BF16), pltpu.VMEM((B, KV, T, HD), BF16)],
        in_specs=[smem_spec(), vmem_spec(), vmem_spec(), vmem_spec(), vmem_spec(), vmem_spec()],
        out_specs=[vmem_spec(), any_spec(), any_spec(), vmem_spec(), vmem_spec()],
        input_output_aliases={4: 3, 5: 4},
        scratch_shapes=[pltpu.SemaphoreType.DMA((2, B))],
        compiler_params=pltpu.CompilerParams(vmem_limit_bytes=4 * MIB),
        name="attention",
    )(cache_len, q, kn, vn, kbuf, vbuf)[:3]


def last_kernel(at_ref, h2_ref, alpha_ref, beta_ref, wout_ref, first_ref, out_ref,
                wbuf, a_send, a_recv, b_send, b_recv, total, wsem, sa, ra, sb, rb, sc, rc):
    core, mate, across = peers()
    say_here((mate, across))
    start_w, wait_w = out_weights(wout_ref, wbuf, wsem, core, begin=1)
    start_w()
    left = jnp.concatenate([at_ref[pl.ds(j, B, stride=8), :].astype(BF16) for j in range(8)], axis=1)
    exchange(left, wbuf, wait_w, lambda: await_peers(2), lambda: None, lambda: None, lambda: None, core, mate, across,
             a_send, a_recv, b_send, b_recv, total, (sa, ra, sb, rb, sc, rc), first=first_ref)
    per = CW // HD
    alpha = alpha_ref[1]
    beta = beta_ref[1]
    for c in range(NC):
        a2 = total[c // (NC // 2), (c % (NC // 2)) // per, :, (c % per) * HD:(c % per + 1) * HD]
        cols = slice(c * HD, (c + 1) * HD)
        out_ref[:, cols] = (alpha * h2_ref[:, cols].astype(F32) + beta * a2).astype(BF16)


def last(at, h2, alpha, beta, w_out, w_first):
    return pl.pallas_call(
        last_kernel,
        out_shape=jax.ShapeDtypeStruct((B, D), BF16),
        in_specs=[vmem_spec(), vmem_spec(), smem_spec(), smem_spec(), any_spec(), vmem_spec()],
        out_specs=vmem_spec(),
        scratch_shapes=exchange_scratch(),
        compiler_params=pltpu.CompilerParams(vmem_limit_bytes=16 * MIB, collective_id=1, has_side_effects=True),
        name="last",
    )(at, h2, alpha, beta, w_out, w_first)


def solution(mesh):
    row_spec = P('dp', None)
    cache_spec = P('dp', 'tp', None, None)
    in_specs = (row_spec, P('dp'), cache_spec, cache_spec, cache_spec, P(None), P(None, None, 'tp', None),
                P(None, 'tp', None), P('tp'), P('tp', None), P('tp', None, None), P(None),
                P(None, 'tp', None, None), P('tp', None, None), P(None), P(None))
    out_specs = (row_spec, cache_spec, cache_spec, cache_spec)

    def local_step(hidden, cache_len, lin_state, k_cache, v_cache, norm_first, w_qkv, w_gate, slopes, out_norm,
                   w_out_lin, norm_second, w_attn, w_out_attn, mix_alpha, mix_beta):
        def hbm(x):
            return pltpu.with_memory_space_constraint(x, pltpu.HBM)

        g1 = norm_first.reshape(NC, HD)
        g2 = norm_second.reshape(NC, HD)
        wa = jnp.transpose(w_attn, (0, 2, 1, 3)).reshape(WA_ROWS, HD)
        state_out, og, ss, h1 = lightning(hbm(hidden), hbm(g1), hbm(slopes), hbm(out_norm), hbm(lin_state), hbm(w_qkv), hbm(w_gate))
        w_last = hbm(w_out_attn.reshape(HL * HD, D))
        q, kn, vn, h2, kbuf, vbuf, w_first = middle(og, ss, h1, g2, mix_alpha, mix_beta, cache_len,
                                                    hbm(w_out_lin.reshape(HL * HD, D)), hbm(wa), hbm(k_cache),
                                                    hbm(v_cache), w_last)
        at, k_out, v_out = attention(cache_len, q, kn, vn, kbuf, vbuf)
        hidden_out = last(at, h2, mix_alpha, mix_beta, w_last, w_first)
        return hidden_out, state_out, k_out, v_out

    return jax.shard_map(local_step, mesh=mesh, in_specs=in_specs, out_specs=out_specs, check_vma=False)
```

```python
import functools
import math

import jax
import jax.numpy as jnp
from jax import lax
from jax.experimental import pallas as pl
from jax.experimental.pallas import tpu as pltpu
from jax.sharding import PartitionSpec as P

EPS = 1e-5
ROPE_BASE = 10000000.0
MESH = pl.DeviceIdType.MESH
F32 = jnp.float32
BF16 = jnp.bfloat16
MIB = 1024 * 1024

B = 32
D = 4096
HL = 8
HD = 128
KV = 2
GQ = 4
T = 512
NC = D // HD

DCH = 256
STEPS = D // DCH
RING = 4
EARLY = 16


def any_spec():
    return pl.BlockSpec(memory_space=pl.ANY)


def vmem_spec():
    return pl.BlockSpec(memory_space=pltpu.VMEM)


def smem_spec():
    return pl.BlockSpec(memory_space=pltpu.SMEM)


def dot(a, b):
    return jnp.dot(a, b, preferred_element_type=F32)


def lightning_kernel(hid_hbm, g1_hbm, slopes_hbm, onorm_hbm, state_ref, wqkv_ref, wgate_ref,
                     sout_ref, og_ref, ss_ref, h1_ref, hid_ref, g1_ref, onorm_ref, slopes_ref,
                     wbuf, gbuf, sbuf, hstack, ebuf, lbuf_a, lbuf_b, acc, kq_t, v_s, o_s, psem, wsem, ssem, osem):
    def w_copies(step, slot):
        rows = pl.ds(step * DCH, DCH)
        return (pltpu.make_async_copy(wqkv_ref.at[rows], wbuf.at[slot], wsem.at[slot, 0]),
                pltpu.make_async_copy(wgate_ref.at[rows], gbuf.at[slot], wsem.at[slot, 1]))

    def s_copy(b):
        return pltpu.make_async_copy(state_ref.at[b], sbuf.at[b], ssem.at[b])

    def o_copy(b):
        return pltpu.make_async_copy(sbuf.at[b], sout_ref.at[b], osem.at[b])

    small = [pltpu.make_async_copy(src, dst, psem.at[n]) for n, (src, dst) in enumerate(
        ((hid_hbm, hid_ref), (g1_hbm, g1_ref), (onorm_hbm, onorm_ref), (slopes_hbm, slopes_ref)))]
    for cp in small:
        cp.start()
    for i in range(RING):
        for cp in w_copies(i, i):
            cp.start()
    for cp in small:
        cp.wait()

    sq = jnp.zeros((B, HD), F32)
    for c in range(NC):
        x = hid_ref[:, c * HD:(c + 1) * HD].astype(F32)
        sq = sq + x * x
    inv = lax.rsqrt(jnp.sum(sq, axis=1, keepdims=True) / D + EPS)
    rr = lax.broadcasted_iota(jnp.int32, (HD, 256), 1)
    dd = lax.broadcasted_iota(jnp.int32, (HD, 256), 0)
    for c in range(NC):
        x = hid_ref[:, c * HD:(c + 1) * HD].astype(F32)
        h1 = (x * inv * g1_ref[c:c + 1, :]).astype(BF16)
        h1_ref[:, c * HD:(c + 1) * HD] = h1
        hstack[c * B:(c + 1) * B, :] = h1
    for n in range(4):
        spread = jnp.where(rr // 8 + 32 * n == dd, 1.0, 0.0).astype(BF16)
        for c in range(NC // 8):
            e = dot(hstack[c * 256:(c + 1) * 256, :], spread).astype(BF16)
            for k in range(8):
                cc = c * 8 + k
                off = (cc % (DCH // HD)) * 1024 + n * 256
                ebuf[cc // (DCH // HD), :, off:off + 256] = e[k * B:(k + 1) * B, :]

    acc[...] = jnp.zeros_like(acc)
    half = DCH * HL // 2
    lane = lax.broadcasted_iota(jnp.int32, (B, half), 1) % 8

    def spread_heads(dst, i, part):
        e = ebuf[i, :, part * half:(part + 1) * half]
        for h in range(HL):
            keep = jnp.where(lane == h, 1.0, 0.0).astype(BF16)
            dst[h * B:(h + 1) * B, :] = e * keep

    spread_heads(lbuf_a, 0, 0)

    def step_fn(i, carry):
        slot = lax.rem(i, RING)

        @pl.when(i >= STEPS - RING)
        def _():
            for k in range(EARLY // RING):
                s_copy((i - (STEPS - RING)) * (EARLY // RING) + k).start()

        for cp in w_copies(i, slot):
            cp.wait()

        def product(left, part, pair):
            rows = slice(part * DCH // 2, (part + 1) * DCH // 2)
            second = wbuf[slot, rows, 1] if pair == 0 else gbuf[slot, rows]
            right = jnp.concatenate([wbuf[slot, rows, 2 * pair].reshape(half, HD), second.reshape(half, HD)], axis=1)
            return dot(left, right)

        spread_heads(lbuf_b, i, 1)
        left_a = lbuf_a[...]
        first = [product(left_a, 0, pair) for pair in range(2)]
        spread_heads(lbuf_a, jnp.minimum(i + 1, STEPS - 1), 0)
        left_b = lbuf_b[...]
        for pair in range(2):
            acc[pair] += first[pair] + product(left_b, 1, pair)

        @pl.when(i + RING < STEPS)
        def _():
            for cp in w_copies(i + RING, slot):
                cp.start()
        return carry

    lax.fori_loop(0, STEPS, step_fn, 0)
    for b in range(EARLY, B):
        s_copy(b).start()

    for h in range(HL):
        rows = slice(h * B, (h + 1) * B)
        q = jax.nn.silu(acc[0, rows, 0:HD]).astype(BF16)
        k = jax.nn.silu(acc[0, rows, HD:2 * HD]).astype(BF16)
        v = jax.nn.silu(acc[1, rows, 0:HD]).astype(BF16)
        qk = jnp.concatenate([k, q], axis=0).astype(F32)
        both = jnp.transpose(qk).astype(BF16)
        kq_t[h] = jnp.concatenate([both[:, 0:B], both[:, B:]], axis=0)
        v_s[h] = v.astype(F32)

    brow = lax.broadcasted_iota(jnp.int32, (B, 2 * HD), 0)
    bcol = lax.broadcasted_iota(jnp.int32, (B, 2 * HD), 1) // HD

    def row_fn(i, carry):
        for r in range(2):
            s_copy(2 * i + r).wait()
        pick = jnp.where(brow == 2 * i + bcol, 1.0, 0.0).astype(BF16)
        for h in range(HL):
            kq = dot(kq_t[h], pick)
            decay = jnp.exp(jnp.full((1, HD), -slopes_ref[h], F32))
            for r in range(2):
                b = 2 * i + r
                lanes = slice(r * HD, (r + 1) * HD)
                new = decay * sbuf[b, h] + kq[0:HD, lanes] * v_s[h, pl.ds(b, 1), :]
                sbuf[b, h] = new
                o_s[b, h:h + 1, :] = jnp.sum(kq[HD:, lanes] * new, axis=0, keepdims=True)
        for r in range(2):
            o_copy(2 * i + r).start()
        return carry

    lax.fori_loop(0, B // 2, row_fn, 0)

    ss = jnp.zeros((B, HD), F32)
    for h in range(HL):
        o = o_s[:, h, :]
        ss = ss + o * o
    ss = jnp.sum(ss, axis=1, keepdims=True)
    ss_ref[...] = jnp.broadcast_to(ss, (B, HD))
    inv_own = lax.rsqrt(ss / (HL * HD) + EPS)
    for h in range(HL):
        gate = jax.nn.sigmoid(acc[1, h * B:(h + 1) * B, HD:2 * HD])
        og_ref[:, h * HD:(h + 1) * HD] = (o_s[:, h, :] * inv_own * onorm_ref[h:h + 1, :] * gate).astype(BF16)

    def drain(b, carry):
        o_copy(b).wait()
        return carry

    lax.fori_loop(0, B, drain, 0)


def lightning(hidden, g1, slopes, out_norm, lin_state, w_qkv, w_gate):
    return pl.pallas_call(
        lightning_kernel,
        out_shape=[jax.ShapeDtypeStruct((B, HL, HD, HD), F32), jax.ShapeDtypeStruct((B, HL * HD), BF16),
                   jax.ShapeDtypeStruct((B, HD), F32), jax.ShapeDtypeStruct((B, D), BF16)],
        in_specs=[any_spec()] * 7,
        out_specs=[any_spec(), vmem_spec(), vmem_spec(), vmem_spec()],
        scratch_shapes=[
            pltpu.VMEM((B, D), BF16),
            pltpu.VMEM((NC, HD), F32),
            pltpu.VMEM((HL, HD), F32),
            pltpu.SMEM((HL,), F32),
            pltpu.VMEM((RING, DCH, 3, HL, HD), BF16),
            pltpu.VMEM((RING, DCH, HL, HD), BF16),
            pltpu.VMEM((B, HL, HD, HD), F32),
            pltpu.VMEM((NC * B, HD), BF16),
            pltpu.VMEM((STEPS, B, DCH * HL), BF16),
            pltpu.VMEM((HL * B, DCH * HL // 2), BF16),
            pltpu.VMEM((HL * B, DCH * HL // 2), BF16),
            pltpu.VMEM((2, HL * B, 2 * HD), F32),
            pltpu.VMEM((HL, 2 * HD, B), BF16),
            pltpu.VMEM((HL, B, HD), F32),
            pltpu.VMEM((B, HL, HD), F32),
            pltpu.SemaphoreType.DMA((4,)),
            pltpu.SemaphoreType.DMA((RING, 2)),
            pltpu.SemaphoreType.DMA((B,)),
            pltpu.SemaphoreType.DMA((B,)),
        ],
        compiler_params=pltpu.CompilerParams(vmem_limit_bytes=40 * MIB),
        name="lightning",
    )(hidden, g1, slopes, out_norm, lin_state, w_qkv, w_gate)


NCH = 4
CW = D // 2 // NCH


def peers():
    dp = lax.axis_index("dp")
    me = lax.axis_index("tp")
    core = lax.rem(me, 2)
    chip = me // 2
    mate = (dp, chip * 2 + (1 - core))
    across = (dp, (1 - chip) * 2 + core)
    return core, mate, across


def say_here(targets):
    barrier = pltpu.get_barrier_semaphore()
    for dev in targets:
        pl.semaphore_signal(barrier, inc=1, device_id=dev, device_id_type=MESH)


def await_peers(count):
    pl.semaphore_wait(pltpu.get_barrier_semaphore(), count)


def rcopy(src, dst, send, recv, dev):
    return pltpu.make_async_remote_copy(src_ref=src, dst_ref=dst, send_sem=send, recv_sem=recv,
                                        device_id=dev, device_id_type=MESH)


def exchange(left, wbuf, wwait, before_sends, pair_scale, mid_work, cross_scale, core, mate, across,
             a_send, a_recv, b_send, b_recv, total, sems, first=None):
    sa, ra, sb, rb, sc, rc = sems

    def product(half, j):
        wwait(half, j)
        buf, at = (wbuf, half * NCH + j) if first is None or j > 0 else (first, half)
        return jnp.concatenate([dot(left, buf[at, :, c:c + 2 * HD]) for c in range(0, CW, 2 * HD)], axis=1)

    a_copies = [rcopy(a_send.at[j], a_recv.at[j], sa.at[j], ra.at[j], mate) for j in range(NCH)]
    b_copies = [rcopy(b_send.at[j], b_recv.at[j], sb.at[j], rb.at[j], across) for j in range(NCH)]
    c_copies = [rcopy(total.at[core, j], total.at[core, j], sc.at[j], rc.at[j], mate) for j in range(NCH)]

    def send_across(j, scale):
        a_copies[j].wait_recv()
        b_send[j] = b_send[j] * scale[0] + a_recv[j] * scale[1] if scale else b_send[j] + a_recv[j]
        b_copies[j].start()

    scale = None
    for j in range(NCH):
        a_send[j] = product(1 - core, j)
        if j == 0:
            before_sends()
        a_copies[j].start()
        b_send[j] = product(core, j)
        if j == 1:
            scale = pair_scale()
        if j >= 1:
            send_across(j - 1, scale)
    send_across(NCH - 1, scale)
    mid_work()
    scale = cross_scale()
    for j in range(NCH):
        b_copies[j].wait_recv()
        total[core, j] = b_send[j] * scale[0] + b_recv[j] * scale[1] if scale else b_send[j] + b_recv[j]
        c_copies[j].start()
    for j in range(NCH):
        c_copies[j].wait_recv()
    for cp in a_copies + b_copies + c_copies:
        cp.wait_send()


def exchange_scratch():
    return [
        pltpu.VMEM((2 * NCH, HL * HD, CW), BF16),
        pltpu.VMEM((NCH, B, CW), F32),
        pltpu.VMEM((NCH, B, CW), F32),
        pltpu.VMEM((NCH, B, CW), F32),
        pltpu.VMEM((NCH, B, CW), F32),
        pltpu.VMEM((2, NCH, B, CW), F32),
        pltpu.SemaphoreType.DMA((2 * NCH,)),
        pltpu.SemaphoreType.DMA((NCH,)),
        pltpu.SemaphoreType.DMA((NCH,)),
        pltpu.SemaphoreType.DMA((NCH,)),
        pltpu.SemaphoreType.DMA((NCH,)),
        pltpu.SemaphoreType.DMA((NCH,)),
        pltpu.SemaphoreType.DMA((NCH,)),
    ]


def out_weights(w_ref, wbuf, wsem, core, begin=0):
    def copy(half, j):
        at = half * NCH + j
        cols = pl.ds(pl.multiple_of(at * CW, CW), CW)
        return pltpu.make_async_copy(w_ref.at[:, cols], wbuf.at[at], wsem.at[at])

    def start():
        for j in range(begin, NCH):
            copy(1 - core, j).start()
            copy(core, j).start()

    def wait(half, j):
        if j >= begin:
            copy(half, j).wait()

    return start, wait


WA_ROWS = D * KV * (GQ + 2)
WA_CH = 32
WA_STEP = WA_ROWS // WA_CH
NJ = KV * (GQ + 2)


def mid_kernel(og_ref, ss_ref, h1_ref, g2_ref, alpha_ref, beta_ref, len_ref, wout_ref, wattn_ref,
               k_ref, v_ref, wnext_ref, q_ref, kn_ref, vn_ref, h2_ref, kbuf, vbuf, wnext,
               wbuf, a_send, a_recv, b_send, b_recv, total, wsem, sa, ra, sb, rb, sc, rc,
               wraw, wide, w2, ss_recv, ss_chip, wasem, ss_s, ss_r, csem):
    core, mate, across = peers()
    say_here((mate, across))
    start_w, wait_w = out_weights(wout_ref, wbuf, wsem, core)
    start_w()

    def wa_copy(i):
        return pltpu.make_async_copy(wattn_ref.at[pl.ds(i * WA_STEP, WA_STEP)], wraw.at[i], wasem.at[i])

    def wa_start(i, carry):
        wa_copy(i).start()
        return carry

    lax.fori_loop(0, WA_CH, wa_start, 0)
    caches = [pltpu.make_async_copy(k_ref, kbuf, csem.at[0]), pltpu.make_async_copy(v_ref, vbuf, csem.at[1])]
    caches += [pltpu.make_async_copy(wnext_ref.at[:, pl.ds(h * (D // 2), CW)], wnext.at[h], csem.at[2 + h]) for h in range(2)]
    for cp in caches:
        cp.start()
    ss_mate = rcopy(ss_ref, ss_recv.at[0], ss_s.at[0], ss_r.at[0], mate)
    ss_across = rcopy(ss_chip, ss_recv.at[1], ss_s.at[1], ss_r.at[1], across)

    def before_sends():
        await_peers(2)
        ss_mate.start()

    def root(total_sq, count):
        return jnp.minimum(jnp.sqrt(total_sq[:, 0:1] / count + EPS), 3e38)

    def pair_scale():
        ss_mate.wait_recv()
        both = ss_ref[...] + ss_recv[0]
        ss_chip[...] = both
        ss_across.start()
        inv = lax.rsqrt(both[:, 0:1] / (D // 2) + EPS)
        return root(ss_ref[...], D // 4) * inv, root(ss_recv[0], D // 4) * inv

    def cross_scale():
        ss_across.wait_recv()
        inv = lax.rsqrt((ss_chip[:, 0:1] + ss_recv[1, :, 0:1]) / D + EPS)
        return root(ss_chip[...], D // 2) * inv, root(ss_recv[1], D // 2) * inv

    def relayout():
        def body(i, carry):
            wa_copy(i).wait()
            wide[...] = wraw[i].astype(F32)
            for j in range(NJ):
                w2[j, pl.ds(pl.multiple_of(i * HD, HD), HD), :] = wide[pl.ds(j, HD, stride=NJ), :].astype(BF16)
            return carry
        lax.fori_loop(0, WA_CH, body, 0)

    exchange(og_ref[...], wbuf, wait_w, before_sends, pair_scale, relayout, cross_scale, core, mate, across,
             a_send, a_recv, b_send, b_recv, total, (sa, ra, sb, rb, sc, rc))
    ss_mate.wait_send()
    ss_across.wait_send()

    per = CW // HD
    alpha = alpha_ref[0]
    beta = beta_ref[0]
    sq = jnp.zeros((B, HD), F32)
    mids = []
    for c in range(NC):
        a1 = total[c // (NC // 2), (c % (NC // 2)) // per, :, (c % per) * HD:(c % per + 1) * HD]
        m = (alpha * h1_ref[:, c * HD:(c + 1) * HD].astype(F32) + beta * a1).astype(BF16)
        h2_ref[:, c * HD:(c + 1) * HD] = m
        x = m.astype(F32)
        sq = sq + x * x
    inv2 = lax.rsqrt(jnp.sum(sq, axis=1, keepdims=True) / D + EPS)
    for c in range(NC):
        m = h2_ref[:, c * HD:(c + 1) * HD].astype(F32)
        h2_ref[:, c * HD:(c + 1) * HD] = (m * inv2 * g2_ref[c:c + 1, :]).astype(BF16)

    pos = jnp.zeros((B, HD), F32)
    row_i = lax.broadcasted_iota(jnp.int32, (B, HD), 0)
    for b in range(B):
        pos = jnp.where(row_i == b, jnp.full((B, HD), len_ref[b]).astype(F32), pos)
    lane = lax.broadcasted_iota(jnp.int32, (B, HD), 1)
    freq = jnp.exp((lane % 32).astype(F32) * (-2.0 * math.log(ROPE_BASE) / 64))
    ang = pos * freq
    rot = lane < 64
    cosv = jnp.where(rot, jnp.cos(ang), 1.0)
    sinv = jnp.sin(ang)
    sin_lo = jnp.where(lane < 32, -sinv, 0.0)
    sin_hi = jnp.where((lane >= 32) & rot, sinv, 0.0)

    def turn(x):
        return x * cosv + pltpu.roll(x, HD - 32, 1) * sin_lo + pltpu.roll(x, 32, 1) * sin_hi

    h2 = h2_ref[...]
    for j in range(GQ + 2):
        w = jnp.concatenate([w2[2 * j], w2[2 * j + 1]], axis=1)
        pr = dot(h2, w)
        for kv in range(KV):
            x = pr[:, kv * HD:(kv + 1) * HD]
            if j < GQ:
                q_ref[pl.ds(kv * GQ + j, B, stride=8), :] = turn(x).astype(BF16).astype(F32)
            elif j == GQ:
                kn_ref[kv] = turn(x).astype(BF16).astype(F32)
            else:
                vn_ref[kv] = x.astype(BF16).astype(F32)
    for cp in caches:
        cp.wait()


def middle(og, ss, h1, g2, alpha, beta, cache_len, w_out, w_attn, k_cache, v_cache, w_next):
    return pl.pallas_call(
        mid_kernel,
        out_shape=[jax.ShapeDtypeStruct((B * 8, HD), F32), jax.ShapeDtypeStruct((KV, B, HD), F32),
                   jax.ShapeDtypeStruct((KV, B, HD), F32), jax.ShapeDtypeStruct((B, D), BF16),
                   pltpu.VMEM((B, KV, T, HD), BF16), pltpu.VMEM((B, KV, T, HD), BF16),
                   pltpu.VMEM((2, HL * HD, CW), BF16)],
        in_specs=[vmem_spec(), vmem_spec(), vmem_spec(), vmem_spec(), smem_spec(), smem_spec(), smem_spec(),
                  any_spec(), any_spec(), any_spec(), any_spec(), any_spec()],
        out_specs=[vmem_spec()] * 7,
        scratch_shapes=exchange_scratch() + [
            pltpu.VMEM((WA_CH, WA_STEP, HD), BF16),
            pltpu.VMEM((WA_STEP, HD), F32),
            pltpu.VMEM((NJ, D, HD), BF16),
            pltpu.VMEM((2, B, HD), F32),
            pltpu.VMEM((B, HD), F32),
            pltpu.SemaphoreType.DMA((WA_CH,)),
            pltpu.SemaphoreType.DMA((2,)),
            pltpu.SemaphoreType.DMA((2,)),
            pltpu.SemaphoreType.DMA((4,)),
        ],
        compiler_params=pltpu.CompilerParams(vmem_limit_bytes=35 * MIB, collective_id=0, has_side_effects=True),
        name="middle",
    )(og, ss, h1, g2, alpha, beta, cache_len, w_out, w_attn, k_cache, v_cache, w_next)


ROWS = 4


def attention_kernel(len_ref, q_ref, kn_ref, vn_ref, kin_ref, vin_ref, at_ref, ko_ref, vo_ref, kbuf, vbuf, osem):
    def outs(b):
        return (pltpu.make_async_copy(kbuf.at[b], ko_ref.at[b], osem.at[0, b]),
                pltpu.make_async_copy(vbuf.at[b], vo_ref.at[b], osem.at[1, b]))

    row8 = lax.broadcasted_iota(jnp.int32, (8, HD), 0)
    row16 = lax.broadcasted_iota(jnp.int32, (16, HD), 0)
    tpos = lax.broadcasted_iota(jnp.int32, (8, T), 1)

    def insert(i, carry):
        rows = [i * ROWS + r for r in range(ROWS)]
        for b in rows:
            p = len_ref[b]
            base = pl.multiple_of((p // 16) * 16, 16)
            hit = row16 == p - base
            for kv in range(KV):
                for buf, new in ((kbuf, kn_ref), (vbuf, vn_ref)):
                    old = buf[b, kv, pl.ds(base, 16), :].astype(F32)
                    buf[b, kv, pl.ds(base, 16), :] = jnp.where(hit, new[kv, pl.ds(b, 1), :], old).astype(BF16)
        for b in rows:
            for cp in outs(b):
                cp.start()
        return carry

    lax.fori_loop(0, B // ROWS, insert, 0)

    def body(i, carry):
        rows = [i * ROWS + r for r in range(ROWS)]
        lens = [len_ref[b] for b in rows]
        scores = []
        for b, p in zip(rows, lens):
            q = q_ref[pl.ds(b * 8, 8), :]
            q2 = jnp.concatenate([jnp.where(row8 < 4, q, 0.0), jnp.where(row8 < 4, 0.0, q)], axis=1).astype(BF16)
            k2 = jnp.concatenate([kbuf[b, 0], kbuf[b, 1]], axis=1)
            s = lax.dot_general(q2, k2, (((1,), (1,)), ((), ())), preferred_element_type=F32) * HD ** -0.5
            scores.append(jnp.where(tpos <= p, s, -jnp.inf))
        tops = [jnp.max(s, axis=1, keepdims=True) for s in scores]
        es = [jnp.exp(s - m) for s, m in zip(scores, tops)]
        sums = [jnp.sum(e, axis=1, keepdims=True) for e in es]
        prs = [(e / z).astype(BF16) for e, z in zip(es, sums)]
        for b, pr in zip(rows, prs):
            o = dot(pr, jnp.concatenate([vbuf[b, 0], vbuf[b, 1]], axis=1))
            at_ref[pl.ds(b * 8, 8), :] = jnp.where(row8 < 4, o[:, 0:HD], o[:, HD:])
        return carry

    lax.fori_loop(0, B // ROWS, body, 0)

    def drain(b, carry):
        for cp in outs(b):
            cp.wait()
        return carry

    lax.fori_loop(0, B, drain, 0)


def attention(cache_len, q, kn, vn, kbuf, vbuf):
    return pl.pallas_call(
        attention_kernel,
        out_shape=[jax.ShapeDtypeStruct((B * 8, HD), F32), pltpu.HBM((B, KV, T, HD), BF16),
                   pltpu.HBM((B, KV, T, HD), BF16), pltpu.VMEM((B, KV, T, HD), BF16), pltpu.VMEM((B, KV, T, HD), BF16)],
        in_specs=[smem_spec(), vmem_spec(), vmem_spec(), vmem_spec(), vmem_spec(), vmem_spec()],
        out_specs=[vmem_spec(), any_spec(), any_spec(), vmem_spec(), vmem_spec()],
        input_output_aliases={4: 3, 5: 4},
        scratch_shapes=[pltpu.SemaphoreType.DMA((2, B))],
        compiler_params=pltpu.CompilerParams(vmem_limit_bytes=4 * MIB),
        name="attention",
    )(cache_len, q, kn, vn, kbuf, vbuf)[:3]


def last_kernel(at_ref, h2_ref, alpha_ref, beta_ref, wout_ref, first_ref, out_ref,
                wbuf, a_send, a_recv, b_send, b_recv, total, wsem, sa, ra, sb, rb, sc, rc):
    core, mate, across = peers()
    say_here((mate, across))
    start_w, wait_w = out_weights(wout_ref, wbuf, wsem, core, begin=1)
    start_w()
    left = jnp.concatenate([at_ref[pl.ds(j, B, stride=8), :].astype(BF16) for j in range(8)], axis=1)
    exchange(left, wbuf, wait_w, lambda: await_peers(2), lambda: None, lambda: None, lambda: None, core, mate, across,
             a_send, a_recv, b_send, b_recv, total, (sa, ra, sb, rb, sc, rc), first=first_ref)
    per = CW // HD
    alpha = alpha_ref[1]
    beta = beta_ref[1]
    for c in range(NC):
        a2 = total[c // (NC // 2), (c % (NC // 2)) // per, :, (c % per) * HD:(c % per + 1) * HD]
        cols = slice(c * HD, (c + 1) * HD)
        out_ref[:, cols] = (alpha * h2_ref[:, cols].astype(F32) + beta * a2).astype(BF16)


def last(at, h2, alpha, beta, w_out, w_first):
    return pl.pallas_call(
        last_kernel,
        out_shape=jax.ShapeDtypeStruct((B, D), BF16),
        in_specs=[vmem_spec(), vmem_spec(), smem_spec(), smem_spec(), any_spec(), vmem_spec()],
        out_specs=vmem_spec(),
        scratch_shapes=exchange_scratch(),
        compiler_params=pltpu.CompilerParams(vmem_limit_bytes=16 * MIB, collective_id=1, has_side_effects=True),
        name="last",
    )(at, h2, alpha, beta, w_out, w_first)


def solution(mesh):
    row_spec = P('dp', None)
    cache_spec = P('dp', 'tp', None, None)
    in_specs = (row_spec, P('dp'), cache_spec, cache_spec, cache_spec, P(None), P(None, None, 'tp', None),
                P(None, 'tp', None), P('tp'), P('tp', None), P('tp', None, None), P(None),
                P(None, 'tp', None, None), P('tp', None, None), P(None), P(None))
    out_specs = (row_spec, cache_spec, cache_spec, cache_spec)

    def local_step(hidden, cache_len, lin_state, k_cache, v_cache, norm_first, w_qkv, w_gate, slopes, out_norm,
                   w_out_lin, norm_second, w_attn, w_out_attn, mix_alpha, mix_beta):
        def hbm(x):
            return pltpu.with_memory_space_constraint(x, pltpu.HBM)

        g1 = norm_first.reshape(NC, HD)
        g2 = norm_second.reshape(NC, HD)
        wa = jnp.transpose(w_attn, (0, 2, 1, 3)).reshape(WA_ROWS, HD)
        state_out, og, ss, h1 = lightning(hbm(hidden), hbm(g1), hbm(slopes), hbm(out_norm), hbm(lin_state), hbm(w_qkv), hbm(w_gate))
        w_last = hbm(w_out_attn.reshape(HL * HD, D))
        q, kn, vn, h2, kbuf, vbuf, w_first = middle(og, ss, h1, g2, mix_alpha, mix_beta, cache_len,
                                                    hbm(w_out_lin.reshape(HL * HD, D)), hbm(wa), hbm(k_cache),
                                                    hbm(v_cache), w_last)
        at, k_out, v_out = attention(cache_len, q, kn, vn, kbuf, vbuf)
        hidden_out = last(at, h2, mix_alpha, mix_beta, w_last, w_first)
        return hidden_out, state_out, k_out, v_out

    return jax.shard_map(local_step, mesh=mesh, in_specs=in_specs, out_specs=out_specs, check_vma=False)
```

```python
import functools
import math

import jax
import jax.numpy as jnp
from jax import lax
from jax.experimental import pallas as pl
from jax.experimental.pallas import tpu as pltpu
from jax.sharding import PartitionSpec as P

EPS = 1e-5
ROPE_BASE = 10000000.0
MESH = pl.DeviceIdType.MESH
F32 = jnp.float32
BF16 = jnp.bfloat16
MIB = 1024 * 1024

B = 32
D = 4096
HL = 8
HD = 128
KV = 2
GQ = 4
T = 512
NC = D // HD

DCH = 512
STEPS = D // DCH
LCH = DCH * HL // 2 // HD
RING = 3
EARLY = 24


def any_spec():
    return pl.BlockSpec(memory_space=pl.ANY)


def vmem_spec():
    return pl.BlockSpec(memory_space=pltpu.VMEM)


def smem_spec():
    return pl.BlockSpec(memory_space=pltpu.SMEM)


def dot(a, b):
    return jnp.dot(a, b, preferred_element_type=F32)


def lightning_kernel(hid_hbm, g1_hbm, slopes_hbm, onorm_hbm, state_ref, wqkv_ref, wgate_ref,
                     sout_ref, og_ref, ss_ref, h1_ref, hid_ref, g1_ref, onorm_ref, slopes_ref,
                     wbuf, gbuf, sbuf, hstack, ebuf, lbuf_a, lbuf_b, acc, kq_t, v_s, o_s, psem, wsem, ssem, osem):
    def w_copies(step, slot):
        rows = pl.ds(step * DCH, DCH)
        return (pltpu.make_async_copy(wqkv_ref.at[rows], wbuf.at[slot], wsem.at[slot, 0]),
                pltpu.make_async_copy(wgate_ref.at[rows], gbuf.at[slot], wsem.at[slot, 1]))

    def s_copy(b):
        return pltpu.make_async_copy(state_ref.at[b], sbuf.at[b], ssem.at[b])

    def o_copy(b):
        return pltpu.make_async_copy(sbuf.at[b], sout_ref.at[b], osem.at[b])

    small = [pltpu.make_async_copy(src, dst, psem.at[n]) for n, (src, dst) in enumerate(
        ((hid_hbm, hid_ref), (g1_hbm, g1_ref), (onorm_hbm, onorm_ref), (slopes_hbm, slopes_ref)))]
    for cp in small:
        cp.start()
    for i in range(RING):
        for cp in w_copies(i, i):
            cp.start()
    for cp in small:
        cp.wait()

    sq = jnp.zeros((B, HD), F32)
    for c in range(NC):
        x = hid_ref[:, c * HD:(c + 1) * HD].astype(F32)
        sq = sq + x * x
    inv = lax.rsqrt(jnp.sum(sq, axis=1, keepdims=True) / D + EPS)
    rr = lax.broadcasted_iota(jnp.int32, (HD, 256), 1)
    dd = lax.broadcasted_iota(jnp.int32, (HD, 256), 0)
    for c in range(NC):
        x = hid_ref[:, c * HD:(c + 1) * HD].astype(F32)
        h1 = (x * inv * g1_ref[c:c + 1, :]).astype(BF16)
        h1_ref[:, c * HD:(c + 1) * HD] = h1
        hstack[c * B:(c + 1) * B, :] = h1
    for n in range(4):
        spread = jnp.where(rr // 8 + 32 * n == dd, 1.0, 0.0).astype(BF16)
        for c in range(NC // 8):
            e = dot(hstack[c * 256:(c + 1) * 256, :], spread).astype(BF16)
            for k in range(8):
                for m in range(2):
                    ebuf[(c * 8 + k) * 8 + n * 2 + m] = e[k * B:(k + 1) * B, m * HD:(m + 1) * HD]

    acc[...] = jnp.zeros_like(acc)
    half = DCH * HL // 2
    lane = lax.broadcasted_iota(jnp.int32, (B, HD), 1) % 8

    def spread_heads(dst, part):
        for h in range(HL):
            keep = jnp.where(lane == h, 1.0, 0.0).astype(BF16)
            for q in range(LCH):
                dst[q, h * B:(h + 1) * B, :] = ebuf[part * LCH + q] * keep

    spread_heads(lbuf_a, 0)

    def step_fn(i, carry):
        slot = lax.rem(i, RING)

        @pl.when(i >= STEPS - RING)
        def _():
            for k in range(EARLY // RING):
                s_copy((i - (STEPS - RING)) * (EARLY // RING) + k).start()

        for cp in w_copies(i, slot):
            cp.wait()

        def product(left, part, pair):
            rows = slice(part * DCH // 2, (part + 1) * DCH // 2)
            second = wbuf[slot, rows, 1] if pair == 0 else gbuf[slot, rows]
            right = jnp.concatenate([wbuf[slot, rows, 2 * pair].reshape(half, HD), second.reshape(half, HD)], axis=1)
            return dot(left, right)

        spread_heads(lbuf_b, 2 * i + 1)
        left_a = jnp.concatenate([lbuf_a[q] for q in range(LCH)], axis=1)
        first = [product(left_a, 0, pair) for pair in range(2)]
        spread_heads(lbuf_a, jnp.minimum(2 * i + 2, 2 * STEPS - 1))
        left_b = jnp.concatenate([lbuf_b[q] for q in range(LCH)], axis=1)
        for pair in range(2):
            acc[pair] += first[pair] + product(left_b, 1, pair)

        @pl.when(i + RING < STEPS)
        def _():
            for cp in w_copies(i + RING, slot):
                cp.start()
        return carry

    lax.fori_loop(0, STEPS, step_fn, 0)
    for b in range(EARLY, B):
        s_copy(b).start()

    for h in range(HL):
        rows = slice(h * B, (h + 1) * B)
        q = jax.nn.silu(acc[0, rows, 0:HD]).astype(BF16)
        k = jax.nn.silu(acc[0, rows, HD:2 * HD]).astype(BF16)
        v = jax.nn.silu(acc[1, rows, 0:HD]).astype(BF16)
        qk = jnp.concatenate([k, q], axis=0).astype(F32)
        both = jnp.transpose(qk).astype(BF16)
        kq_t[h] = jnp.concatenate([both[:, 0:B], both[:, B:]], axis=0)
        v_s[h] = v.astype(F32)

    brow = lax.broadcasted_iota(jnp.int32, (B, 2 * HD), 0)
    bcol = lax.broadcasted_iota(jnp.int32, (B, 2 * HD), 1) // HD

    def row_fn(i, carry):
        for r in range(2):
            s_copy(2 * i + r).wait()
        pick = jnp.where(brow == 2 * i + bcol, 1.0, 0.0).astype(BF16)
        for h in range(HL):
            kq = dot(kq_t[h], pick)
            decay = jnp.exp(jnp.full((1, HD), -slopes_ref[h], F32))
            for r in range(2):
                b = 2 * i + r
                lanes = slice(r * HD, (r + 1) * HD)
                new = decay * sbuf[b, h] + kq[0:HD, lanes] * v_s[h, pl.ds(b, 1), :]
                sbuf[b, h] = new
                o_s[b, h:h + 1, :] = jnp.sum(kq[HD:, lanes] * new, axis=0, keepdims=True)
        for r in range(2):
            o_copy(2 * i + r).start()
        return carry

    lax.fori_loop(0, B // 2, row_fn, 0)

    ss = jnp.zeros((B, HD), F32)
    for h in range(HL):
        o = o_s[:, h, :]
        ss = ss + o * o
    ss = jnp.sum(ss, axis=1, keepdims=True)
    ss_ref[...] = jnp.broadcast_to(ss, (B, HD))
    inv_own = lax.rsqrt(ss / (HL * HD) + EPS)
    for h in range(HL):
        gate = jax.nn.sigmoid(acc[1, h * B:(h + 1) * B, HD:2 * HD])
        og_ref[:, h * HD:(h + 1) * HD] = (o_s[:, h, :] * inv_own * onorm_ref[h:h + 1, :] * gate).astype(BF16)

    def drain(b, carry):
        o_copy(b).wait()
        return carry

    lax.fori_loop(0, B, drain, 0)


def lightning(hidden, g1, slopes, out_norm, lin_state, w_qkv, w_gate):
    return pl.pallas_call(
        lightning_kernel,
        out_shape=[jax.ShapeDtypeStruct((B, HL, HD, HD), F32), jax.ShapeDtypeStruct((B, HL * HD), BF16),
                   jax.ShapeDtypeStruct((B, HD), F32), jax.ShapeDtypeStruct((B, D), BF16)],
        in_specs=[any_spec()] * 7,
        out_specs=[any_spec(), vmem_spec(), vmem_spec(), vmem_spec()],
        scratch_shapes=[
            pltpu.VMEM((B, D), BF16),
            pltpu.VMEM((NC, HD), F32),
            pltpu.VMEM((HL, HD), F32),
            pltpu.SMEM((HL,), F32),
            pltpu.VMEM((RING, DCH, 3, HL, HD), BF16),
            pltpu.VMEM((RING, DCH, HL, HD), BF16),
            pltpu.VMEM((B, HL, HD, HD), F32),
            pltpu.VMEM((NC * B, HD), BF16),
            pltpu.VMEM((2 * STEPS * LCH, B, HD), BF16),
            pltpu.VMEM((LCH, HL * B, HD), BF16),
            pltpu.VMEM((LCH, HL * B, HD), BF16),
            pltpu.VMEM((2, HL * B, 2 * HD), F32),
            pltpu.VMEM((HL, 2 * HD, B), BF16),
            pltpu.VMEM((HL, B, HD), F32),
            pltpu.VMEM((B, HL, HD), F32),
            pltpu.SemaphoreType.DMA((4,)),
            pltpu.SemaphoreType.DMA((RING, 2)),
            pltpu.SemaphoreType.DMA((B,)),
            pltpu.SemaphoreType.DMA((B,)),
        ],
        compiler_params=pltpu.CompilerParams(vmem_limit_bytes=40 * MIB),
        name="lightning",
    )(hidden, g1, slopes, out_norm, lin_state, w_qkv, w_gate)


NCH = 4
CW = D // 2 // NCH


def peers():
    dp = lax.axis_index("dp")
    me = lax.axis_index("tp")
    core = lax.rem(me, 2)
    chip = me // 2
    mate = (dp, chip * 2 + (1 - core))
    across = (dp, (1 - chip) * 2 + core)
    return core, mate, across


def say_here(targets):
    barrier = pltpu.get_barrier_semaphore()
    for dev in targets:
        pl.semaphore_signal(barrier, inc=1, device_id=dev, device_id_type=MESH)


def await_peers(count):
    pl.semaphore_wait(pltpu.get_barrier_semaphore(), count)


def rcopy(src, dst, send, recv, dev):
    return pltpu.make_async_remote_copy(src_ref=src, dst_ref=dst, send_sem=send, recv_sem=recv,
                                        device_id=dev, device_id_type=MESH)


def exchange(left, wbuf, wwait, before_sends, pair_scale, mid_work, cross_scale, core, mate, across,
             a_send, a_recv, b_send, b_recv, total, sems, use, first=None):
    sa, ra, sb, rb, sc, rc = sems

    def product(half, j):
        wwait(half, j)
        buf, at = (wbuf, half * NCH + j) if first is None or j > 0 else (first, half)
        return jnp.concatenate([dot(left, buf[at, :, c:c + 2 * HD]) for c in range(0, CW, 2 * HD)], axis=1)

    a_copies = [rcopy(a_send.at[j], a_recv.at[j], sa.at[j], ra.at[j], mate) for j in range(NCH)]
    b_copies = [rcopy(b_send.at[j], b_recv.at[j], sb.at[j], rb.at[j], across) for j in range(NCH)]
    c_copies = [rcopy(total.at[core, j], total.at[core, j], sc.at[j], rc.at[j], mate) for j in range(NCH)]

    def send_across(j, scale):
        a_copies[j].wait_recv()
        b_send[j] = b_send[j] * scale[0] + a_recv[j] * scale[1] if scale else b_send[j] + a_recv[j]
        b_copies[j].start()

    scale = None
    for j in range(NCH):
        a_send[j] = product(1 - core, j)
        if j == 0:
            before_sends()
        a_copies[j].start()
        b_send[j] = product(core, j)
        if j == 1:
            scale = pair_scale()
        if j >= 1:
            send_across(j - 1, scale)
    send_across(NCH - 1, scale)
    mid_work()
    scale = cross_scale()
    for j in range(NCH):
        b_copies[j].wait_recv()
        total[core, j] = b_send[j] * scale[0] + b_recv[j] * scale[1] if scale else b_send[j] + b_recv[j]
        c_copies[j].start()
        if j >= 1:
            c_copies[j - 1].wait_recv()
            use(j - 1)
    c_copies[NCH - 1].wait_recv()
    use(NCH - 1)
    return a_copies + b_copies + c_copies


def exchange_scratch():
    return [
        pltpu.VMEM((2 * NCH, HL * HD, CW), BF16),
        pltpu.VMEM((NCH, B, CW), F32),
        pltpu.VMEM((NCH, B, CW), F32),
        pltpu.VMEM((NCH, B, CW), F32),
        pltpu.VMEM((NCH, B, CW), F32),
        pltpu.VMEM((2, NCH, B, CW), F32),
        pltpu.SemaphoreType.DMA((2 * NCH,)),
        pltpu.SemaphoreType.DMA((NCH,)),
        pltpu.SemaphoreType.DMA((NCH,)),
        pltpu.SemaphoreType.DMA((NCH,)),
        pltpu.SemaphoreType.DMA((NCH,)),
        pltpu.SemaphoreType.DMA((NCH,)),
        pltpu.SemaphoreType.DMA((NCH,)),
    ]


def out_weights(w_ref, wbuf, wsem, core, begin=0):
    def copy(half, j):
        at = half * NCH + j
        cols = pl.ds(pl.multiple_of(at * CW, CW), CW)
        return pltpu.make_async_copy(w_ref.at[:, cols], wbuf.at[at], wsem.at[at])

    def start():
        for j in range(begin, NCH):
            copy(1 - core, j).start()
            copy(core, j).start()

    def wait(half, j):
        if j >= begin:
            copy(half, j).wait()

    return start, wait


WA_ROWS = D * KV * (GQ + 2)
WA_CH = 32
WA_STEP = WA_ROWS // WA_CH
NJ = KV * (GQ + 2)


def mid_kernel(og_ref, ss_ref, h1_ref, g2_ref, alpha_ref, beta_ref, len_ref, wout_ref, wattn_ref,
               k_ref, v_ref, wnext_ref, q_ref, kn_ref, vn_ref, h2_ref, kbuf, vbuf, wnext,
               wbuf, a_send, a_recv, b_send, b_recv, total, wsem, sa, ra, sb, rb, sc, rc,
               wraw, wide, w2, ss_recv, ss_chip, wasem, ss_s, ss_r, csem):
    core, mate, across = peers()
    say_here((mate, across))
    start_w, wait_w = out_weights(wout_ref, wbuf, wsem, core)
    start_w()

    def wa_copy(i):
        return pltpu.make_async_copy(wattn_ref.at[pl.ds(i * WA_STEP, WA_STEP)], wraw.at[i], wasem.at[i])

    def wa_start(i, carry):
        wa_copy(i).start()
        return carry

    lax.fori_loop(0, WA_CH, wa_start, 0)
    caches = [pltpu.make_async_copy(k_ref, kbuf, csem.at[0]), pltpu.make_async_copy(v_ref, vbuf, csem.at[1])]
    caches += [pltpu.make_async_copy(wnext_ref.at[:, pl.ds(h * (D // 2), CW)], wnext.at[h], csem.at[2 + h]) for h in range(2)]
    for cp in caches:
        cp.start()
    ss_mate = rcopy(ss_ref, ss_recv.at[0], ss_s.at[0], ss_r.at[0], mate)
    ss_across = rcopy(ss_chip, ss_recv.at[1], ss_s.at[1], ss_r.at[1], across)

    def before_sends():
        await_peers(2)
        ss_mate.start()

    def root(total_sq, count):
        return jnp.minimum(jnp.sqrt(total_sq[:, 0:1] / count + EPS), 3e38)

    def pair_scale():
        ss_mate.wait_recv()
        both = ss_ref[...] + ss_recv[0]
        ss_chip[...] = both
        ss_across.start()
        inv = lax.rsqrt(both[:, 0:1] / (D // 2) + EPS)
        return root(ss_ref[...], D // 4) * inv, root(ss_recv[0], D // 4) * inv

    def cross_scale():
        ss_across.wait_recv()
        inv = lax.rsqrt((ss_chip[:, 0:1] + ss_recv[1, :, 0:1]) / D + EPS)
        return root(ss_chip[...], D // 2) * inv, root(ss_recv[1], D // 2) * inv

    def relayout():
        def body(i, carry):
            wa_copy(i).wait()
            wide[...] = wraw[i].astype(F32)
            for j in range(NJ):
                w2[j, pl.ds(pl.multiple_of(i * HD, HD), HD), :] = wide[pl.ds(j, HD, stride=NJ), :].astype(BF16)
            return carry
        lax.fori_loop(0, WA_CH, body, 0)

    alpha = alpha_ref[0]
    beta = beta_ref[0]
    squares = [jnp.zeros((B, HD), F32)]

    def use(j):
        for half in range(2):
            for p in range(CW // HD):
                cols = slice(half * (D // 2) + j * CW + p * HD, half * (D // 2) + j * CW + (p + 1) * HD)
                a1 = total[half, j, :, p * HD:(p + 1) * HD]
                m = (alpha * h1_ref[:, cols].astype(F32) + beta * a1).astype(BF16)
                h2_ref[:, cols] = m
                x = m.astype(F32)
                squares[0] = squares[0] + x * x

    sent = exchange(og_ref[...], wbuf, wait_w, before_sends, pair_scale, relayout, cross_scale, core, mate, across,
                    a_send, a_recv, b_send, b_recv, total, (sa, ra, sb, rb, sc, rc), use)
    sq = squares[0]
    inv2 = lax.rsqrt(jnp.sum(sq, axis=1, keepdims=True) / D + EPS)
    for c in range(NC):
        m = h2_ref[:, c * HD:(c + 1) * HD].astype(F32)
        h2_ref[:, c * HD:(c + 1) * HD] = (m * inv2 * g2_ref[c:c + 1, :]).astype(BF16)

    pos = jnp.zeros((B, HD), F32)
    row_i = lax.broadcasted_iota(jnp.int32, (B, HD), 0)
    for b in range(B):
        pos = jnp.where(row_i == b, jnp.full((B, HD), len_ref[b]).astype(F32), pos)
    lane = lax.broadcasted_iota(jnp.int32, (B, HD), 1)
    freq = jnp.exp((lane % 32).astype(F32) * (-2.0 * math.log(ROPE_BASE) / 64))
    ang = pos * freq
    rot = lane < 64
    cosv = jnp.where(rot, jnp.cos(ang), 1.0)
    sinv = jnp.sin(ang)
    sin_lo = jnp.where(lane < 32, -sinv, 0.0)
    sin_hi = jnp.where((lane >= 32) & rot, sinv, 0.0)

    def turn(x):
        return x * cosv + pltpu.roll(x, HD - 32, 1) * sin_lo + pltpu.roll(x, 32, 1) * sin_hi

    h2 = h2_ref[...]
    for j in range(GQ + 2):
        w = jnp.concatenate([w2[2 * j], w2[2 * j + 1]], axis=1)
        pr = dot(h2, w)
        for kv in range(KV):
            x = pr[:, kv * HD:(kv + 1) * HD]
            if j < GQ:
                q_ref[pl.ds(kv * GQ + j, B, stride=8), :] = turn(x).astype(BF16).astype(F32)
            elif j == GQ:
                kn_ref[kv] = turn(x).astype(BF16).astype(F32)
            else:
                vn_ref[kv] = x.astype(BF16).astype(F32)
    for cp in caches:
        cp.wait()
    for cp in sent + [ss_mate, ss_across]:
        cp.wait_send()


def middle(og, ss, h1, g2, alpha, beta, cache_len, w_out, w_attn, k_cache, v_cache, w_next):
    return pl.pallas_call(
        mid_kernel,
        out_shape=[jax.ShapeDtypeStruct((B * 8, HD), F32), jax.ShapeDtypeStruct((KV, B, HD), F32),
                   jax.ShapeDtypeStruct((KV, B, HD), F32), jax.ShapeDtypeStruct((B, D), BF16),
                   pltpu.VMEM((B, KV, T, HD), BF16), pltpu.VMEM((B, KV, T, HD), BF16),
                   pltpu.VMEM((2, HL * HD, CW), BF16)],
        in_specs=[vmem_spec(), vmem_spec(), vmem_spec(), vmem_spec(), smem_spec(), smem_spec(), smem_spec(),
                  any_spec(), any_spec(), any_spec(), any_spec(), any_spec()],
        out_specs=[vmem_spec()] * 7,
        scratch_shapes=exchange_scratch() + [
            pltpu.VMEM((WA_CH, WA_STEP, HD), BF16),
            pltpu.VMEM((WA_STEP, HD), F32),
            pltpu.VMEM((NJ, D, HD), BF16),
            pltpu.VMEM((2, B, HD), F32),
            pltpu.VMEM((B, HD), F32),
            pltpu.SemaphoreType.DMA((WA_CH,)),
            pltpu.SemaphoreType.DMA((2,)),
            pltpu.SemaphoreType.DMA((2,)),
            pltpu.SemaphoreType.DMA((4,)),
        ],
        compiler_params=pltpu.CompilerParams(vmem_limit_bytes=35 * MIB, collective_id=0, has_side_effects=True),
        name="middle",
    )(og, ss, h1, g2, alpha, beta, cache_len, w_out, w_attn, k_cache, v_cache, w_next)


ROWS = 4
ROWS_MM = 8


def attention_kernel(len_ref, q_ref, kn_ref, vn_ref, kin_ref, vin_ref, at_ref, ko_ref, vo_ref, kbuf, vbuf, osem):
    def outs(b):
        return (pltpu.make_async_copy(kbuf.at[b], ko_ref.at[b], osem.at[0, b]),
                pltpu.make_async_copy(vbuf.at[b], vo_ref.at[b], osem.at[1, b]))

    row8 = lax.broadcasted_iota(jnp.int32, (8, HD), 0)
    row16 = lax.broadcasted_iota(jnp.int32, (16, HD), 0)
    tpos = lax.broadcasted_iota(jnp.int32, (8, T), 1)

    def insert(i, carry):
        rows = [i * ROWS + r for r in range(ROWS)]
        for b in rows:
            p = len_ref[b]
            base = pl.multiple_of((p // 16) * 16, 16)
            hit = row16 == p - base
            for kv in range(KV):
                for buf, new in ((kbuf, kn_ref), (vbuf, vn_ref)):
                    old = buf[b, kv, pl.ds(base, 16), :].astype(F32)
                    buf[b, kv, pl.ds(base, 16), :] = jnp.where(hit, new[kv, pl.ds(b, 1), :], old).astype(BF16)
        for b in rows:
            for cp in outs(b):
                cp.start()
        return carry

    lax.fori_loop(0, B // ROWS, insert, 0)

    def body(i, carry):
        rows = [i * ROWS_MM + r for r in range(ROWS_MM)]
        lens = [len_ref[b] for b in rows]
        scores = []
        for b, p in zip(rows, lens):
            q = q_ref[pl.ds(b * 8, 8), :]
            q2 = jnp.concatenate([jnp.where(row8 < 4, q, 0.0), jnp.where(row8 < 4, 0.0, q)], axis=1).astype(BF16)
            k2 = jnp.concatenate([kbuf[b, 0], kbuf[b, 1]], axis=1)
            s = lax.dot_general(q2, k2, (((1,), (1,)), ((), ())), preferred_element_type=F32) * HD ** -0.5
            scores.append(jnp.where(tpos <= p, s, -jnp.inf))
        tops = [jnp.max(s, axis=1, keepdims=True) for s in scores]
        es = [jnp.exp(s - m) for s, m in zip(scores, tops)]
        sums = [jnp.sum(e, axis=1, keepdims=True) for e in es]
        prs = [(e / z).astype(BF16) for e, z in zip(es, sums)]
        for b, pr in zip(rows, prs):
            o = dot(pr, jnp.concatenate([vbuf[b, 0], vbuf[b, 1]], axis=1))
            at_ref[pl.ds(b * 8, 8), :] = jnp.where(row8 < 4, o[:, 0:HD], o[:, HD:])
        return carry

    lax.fori_loop(0, B // ROWS_MM, body, 0)

    def drain(b, carry):
        for cp in outs(b):
            cp.wait()
        return carry

    lax.fori_loop(0, B, drain, 0)


def attention(cache_len, q, kn, vn, kbuf, vbuf):
    return pl.pallas_call(
        attention_kernel,
        out_shape=[jax.ShapeDtypeStruct((B * 8, HD), F32), pltpu.HBM((B, KV, T, HD), BF16),
                   pltpu.HBM((B, KV, T, HD), BF16), pltpu.VMEM((B, KV, T, HD), BF16), pltpu.VMEM((B, KV, T, HD), BF16)],
        in_specs=[smem_spec(), vmem_spec(), vmem_spec(), vmem_spec(), vmem_spec(), vmem_spec()],
        out_specs=[vmem_spec(), any_spec(), any_spec(), vmem_spec(), vmem_spec()],
        input_output_aliases={4: 3, 5: 4},
        scratch_shapes=[pltpu.SemaphoreType.DMA((2, B))],
        compiler_params=pltpu.CompilerParams(vmem_limit_bytes=4 * MIB),
        name="attention",
    )(cache_len, q, kn, vn, kbuf, vbuf)[:3]


def last_kernel(at_ref, h2_ref, alpha_ref, beta_ref, wout_ref, first_ref, out_ref,
                wbuf, a_send, a_recv, b_send, b_recv, total, wsem, sa, ra, sb, rb, sc, rc):
    core, mate, across = peers()
    say_here((mate, across))
    start_w, wait_w = out_weights(wout_ref, wbuf, wsem, core, begin=1)
    start_w()
    left = jnp.concatenate([at_ref[pl.ds(j, B, stride=8), :].astype(BF16) for j in range(8)], axis=1)
    alpha = alpha_ref[1]
    beta = beta_ref[1]

    def use(j):
        for half in range(2):
            cols = slice(half * (D // 2) + j * CW, half * (D // 2) + (j + 1) * CW)
            out_ref[:, cols] = (alpha * h2_ref[:, cols].astype(F32) + beta * total[half, j]).astype(BF16)

    sent = exchange(left, wbuf, wait_w, lambda: await_peers(2), lambda: None, lambda: None, lambda: None, core, mate,
                    across, a_send, a_recv, b_send, b_recv, total, (sa, ra, sb, rb, sc, rc), use, first=first_ref)
    for cp in sent:
        cp.wait_send()


def last(at, h2, alpha, beta, w_out, w_first):
    return pl.pallas_call(
        last_kernel,
        out_shape=jax.ShapeDtypeStruct((B, D), BF16),
        in_specs=[vmem_spec(), vmem_spec(), smem_spec(), smem_spec(), any_spec(), vmem_spec()],
        out_specs=vmem_spec(),
        scratch_shapes=exchange_scratch(),
        compiler_params=pltpu.CompilerParams(vmem_limit_bytes=16 * MIB, collective_id=1, has_side_effects=True),
        name="last",
    )(at, h2, alpha, beta, w_out, w_first)


def solution(mesh):
    row_spec = P('dp', None)
    cache_spec = P('dp', 'tp', None, None)
    in_specs = (row_spec, P('dp'), cache_spec, cache_spec, cache_spec, P(None), P(None, None, 'tp', None),
                P(None, 'tp', None), P('tp'), P('tp', None), P('tp', None, None), P(None),
                P(None, 'tp', None, None), P('tp', None, None), P(None), P(None))
    out_specs = (row_spec, cache_spec, cache_spec, cache_spec)

    def local_step(hidden, cache_len, lin_state, k_cache, v_cache, norm_first, w_qkv, w_gate, slopes, out_norm,
                   w_out_lin, norm_second, w_attn, w_out_attn, mix_alpha, mix_beta):
        def hbm(x):
            return pltpu.with_memory_space_constraint(x, pltpu.HBM)

        g1 = norm_first.reshape(NC, HD)
        g2 = norm_second.reshape(NC, HD)
        wa = jnp.transpose(w_attn, (0, 2, 1, 3)).reshape(WA_ROWS, HD)
        state_out, og, ss, h1 = lightning(hbm(hidden), hbm(g1), hbm(slopes), hbm(out_norm), hbm(lin_state), hbm(w_qkv), hbm(w_gate))
        w_last = hbm(w_out_attn.reshape(HL * HD, D))
        q, kn, vn, h2, kbuf, vbuf, w_first = middle(og, ss, h1, g2, mix_alpha, mix_beta, cache_len,
                                                    hbm(w_out_lin.reshape(HL * HD, D)), hbm(wa), hbm(k_cache),
                                                    hbm(v_cache), w_last)
        at, k_out, v_out = attention(cache_len, q, kn, vn, kbuf, vbuf)
        hidden_out = last(at, h2, mix_alpha, mix_beta, w_last, w_first)
        return hidden_out, state_out, k_out, v_out

    return jax.shard_map(local_step, mesh=mesh, in_specs=in_specs, out_specs=out_specs, check_vma=False)
```

```python
import functools
import math

import jax
import jax.numpy as jnp
from jax import lax
from jax.experimental import pallas as pl
from jax.experimental.pallas import tpu as pltpu
from jax.sharding import PartitionSpec as P

EPS = 1e-5
ROPE_BASE = 10000000.0
MESH = pl.DeviceIdType.MESH
F32 = jnp.float32
BF16 = jnp.bfloat16
MIB = 1024 * 1024

B = 32
D = 4096
HL = 8
HD = 128
KV = 2
GQ = 4
T = 512
NC = D // HD

DCH = 512
STEPS = D // DCH
LCH = DCH * HL // 2 // HD
RING = 3
EARLY = 24


def any_spec():
    return pl.BlockSpec(memory_space=pl.ANY)


def vmem_spec():
    return pl.BlockSpec(memory_space=pltpu.VMEM)


def smem_spec():
    return pl.BlockSpec(memory_space=pltpu.SMEM)


def dot(a, b):
    return jnp.dot(a, b, preferred_element_type=F32)


def lightning_kernel(hid_hbm, g1_hbm, slopes_hbm, onorm_hbm, state_ref, wqkv_ref, wgate_ref,
                     sout_ref, og_ref, ss_ref, h1_ref, hid_ref, g1_ref, onorm_ref, slopes_ref,
                     wbuf, gbuf, sbuf, hstack, ebuf, lbuf_a, lbuf_b, acc, kq_t, v_s, o_s, psem, wsem, ssem, osem):
    def w_copies(step, slot):
        rows = pl.ds(step * DCH, DCH)
        return (pltpu.make_async_copy(wqkv_ref.at[rows], wbuf.at[slot], wsem.at[slot, 0]),
                pltpu.make_async_copy(wgate_ref.at[rows], gbuf.at[slot], wsem.at[slot, 1]))

    def s_copy(b):
        return pltpu.make_async_copy(state_ref.at[b], sbuf.at[b], ssem.at[b])

    def o_copy(b):
        return pltpu.make_async_copy(sbuf.at[b], sout_ref.at[b], osem.at[b])

    small = [pltpu.make_async_copy(src, dst, psem.at[n]) for n, (src, dst) in enumerate(
        ((hid_hbm, hid_ref), (g1_hbm, g1_ref), (onorm_hbm, onorm_ref), (slopes_hbm, slopes_ref)))]
    for cp in small:
        cp.start()
    for i in range(RING):
        for cp in w_copies(i, i):
            cp.start()
    for cp in small:
        cp.wait()

    sq = jnp.zeros((B, HD), F32)
    for c in range(NC):
        x = hid_ref[:, c * HD:(c + 1) * HD].astype(F32)
        sq = sq + x * x
    inv = lax.rsqrt(jnp.sum(sq, axis=1, keepdims=True) / D + EPS)
    rr = lax.broadcasted_iota(jnp.int32, (HD, 256), 1)
    dd = lax.broadcasted_iota(jnp.int32, (HD, 256), 0)
    for c in range(NC):
        x = hid_ref[:, c * HD:(c + 1) * HD].astype(F32)
        h1 = (x * inv * g1_ref[c:c + 1, :]).astype(BF16)
        h1_ref[:, c * HD:(c + 1) * HD] = h1
        hstack[c * B:(c + 1) * B, :] = h1
    for n in range(4):
        spread = jnp.where(rr // 8 + 32 * n == dd, 1.0, 0.0).astype(BF16)
        for c in range(NC // 8):
            e = dot(hstack[c * 256:(c + 1) * 256, :], spread).astype(BF16)
            for k in range(8):
                for m in range(2):
                    ebuf[(c * 8 + k) * 8 + n * 2 + m] = e[k * B:(k + 1) * B, m * HD:(m + 1) * HD]

    acc[...] = jnp.zeros_like(acc)
    half = DCH * HL // 2
    lane = lax.broadcasted_iota(jnp.int32, (B, HD), 1) % 8

    def spread_heads(dst, part):
        for h in range(HL):
            keep = jnp.where(lane == h, 1.0, 0.0).astype(BF16)
            for q in range(LCH):
                dst[q, h * B:(h + 1) * B, :] = ebuf[part * LCH + q] * keep

    spread_heads(lbuf_a, 0)

    def step_fn(i, carry):
        slot = lax.rem(i, RING)

        @pl.when(i >= STEPS - RING)
        def _():
            for k in range(EARLY // RING):
                s_copy((i - (STEPS - RING)) * (EARLY // RING) + k).start()

        for cp in w_copies(i, slot):
            cp.wait()

        def product(left, part, pair):
            rows = slice(part * DCH // 2, (part + 1) * DCH // 2)
            second = wbuf[slot, rows, 1] if pair == 0 else gbuf[slot, rows]
            right = jnp.concatenate([wbuf[slot, rows, 2 * pair].reshape(half, HD), second.reshape(half, HD)], axis=1)
            return dot(left, right)

        spread_heads(lbuf_b, 2 * i + 1)
        left_a = jnp.concatenate([lbuf_a[q] for q in range(LCH)], axis=1)
        first = [product(left_a, 0, pair) for pair in range(2)]
        spread_heads(lbuf_a, jnp.minimum(2 * i + 2, 2 * STEPS - 1))
        left_b = jnp.concatenate([lbuf_b[q] for q in range(LCH)], axis=1)
        for pair in range(2):
            acc[pair] += first[pair] + product(left_b, 1, pair)

        @pl.when(i + RING < STEPS)
        def _():
            for cp in w_copies(i + RING, slot):
                cp.start()
        return carry

    lax.fori_loop(0, STEPS, step_fn, 0)
    for b in range(EARLY, B):
        s_copy(b).start()

    for h in range(HL):
        rows = slice(h * B, (h + 1) * B)
        q = jax.nn.silu(acc[0, rows, 0:HD]).astype(BF16)
        k = jax.nn.silu(acc[0, rows, HD:2 * HD]).astype(BF16)
        v = jax.nn.silu(acc[1, rows, 0:HD]).astype(BF16)
        qk = jnp.concatenate([k, q], axis=0).astype(F32)
        both = jnp.transpose(qk).astype(BF16)
        kq_t[h] = jnp.concatenate([both[:, 0:B], both[:, B:]], axis=0)
        v_s[h] = v.astype(F32)

    brow = lax.broadcasted_iota(jnp.int32, (B, 2 * HD), 0)
    bcol = lax.broadcasted_iota(jnp.int32, (B, 2 * HD), 1) // HD

    def row_fn(i, carry):
        for r in range(2):
            s_copy(2 * i + r).wait()
        pick = jnp.where(brow == 2 * i + bcol, 1.0, 0.0).astype(BF16)
        for h in range(HL):
            kq = dot(kq_t[h], pick)
            decay = jnp.exp(jnp.full((1, HD), -slopes_ref[h], F32))
            for r in range(2):
                b = 2 * i + r
                lanes = slice(r * HD, (r + 1) * HD)
                new = decay * sbuf[b, h] + kq[0:HD, lanes] * v_s[h, pl.ds(b, 1), :]
                sbuf[b, h] = new
                o_s[b, h:h + 1, :] = jnp.sum(kq[HD:, lanes] * new, axis=0, keepdims=True)
        for r in range(2):
            o_copy(2 * i + r).start()
        return carry

    lax.fori_loop(0, B // 2, row_fn, 0)

    ss = jnp.zeros((B, HD), F32)
    for h in range(HL):
        o = o_s[:, h, :]
        ss = ss + o * o
    ss = jnp.sum(ss, axis=1, keepdims=True)
    ss_ref[...] = jnp.broadcast_to(ss, (B, HD))
    inv_own = lax.rsqrt(ss / (HL * HD) + EPS)
    for h in range(HL):
        gate = jax.nn.sigmoid(acc[1, h * B:(h + 1) * B, HD:2 * HD])
        og_ref[:, h * HD:(h + 1) * HD] = (o_s[:, h, :] * inv_own * onorm_ref[h:h + 1, :] * gate).astype(BF16)

    def drain(b, carry):
        o_copy(b).wait()
        return carry

    lax.fori_loop(0, B, drain, 0)


def lightning(hidden, g1, slopes, out_norm, lin_state, w_qkv, w_gate):
    return pl.pallas_call(
        lightning_kernel,
        out_shape=[jax.ShapeDtypeStruct((B, HL, HD, HD), F32), jax.ShapeDtypeStruct((B, HL * HD), BF16),
                   jax.ShapeDtypeStruct((B, HD), F32), jax.ShapeDtypeStruct((B, D), BF16)],
        in_specs=[any_spec()] * 7,
        out_specs=[any_spec(), vmem_spec(), vmem_spec(), vmem_spec()],
        scratch_shapes=[
            pltpu.VMEM((B, D), BF16),
            pltpu.VMEM((NC, HD), F32),
            pltpu.VMEM((HL, HD), F32),
            pltpu.SMEM((HL,), F32),
            pltpu.VMEM((RING, DCH, 3, HL, HD), BF16),
            pltpu.VMEM((RING, DCH, HL, HD), BF16),
            pltpu.VMEM((B, HL, HD, HD), F32),
            pltpu.VMEM((NC * B, HD), BF16),
            pltpu.VMEM((2 * STEPS * LCH, B, HD), BF16),
            pltpu.VMEM((LCH, HL * B, HD), BF16),
            pltpu.VMEM((LCH, HL * B, HD), BF16),
            pltpu.VMEM((2, HL * B, 2 * HD), F32),
            pltpu.VMEM((HL, 2 * HD, B), BF16),
            pltpu.VMEM((HL, B, HD), F32),
            pltpu.VMEM((B, HL, HD), F32),
            pltpu.SemaphoreType.DMA((4,)),
            pltpu.SemaphoreType.DMA((RING, 2)),
            pltpu.SemaphoreType.DMA((B,)),
            pltpu.SemaphoreType.DMA((B,)),
        ],
        compiler_params=pltpu.CompilerParams(vmem_limit_bytes=40 * MIB),
        name="lightning",
    )(hidden, g1, slopes, out_norm, lin_state, w_qkv, w_gate)


NCH = 8
CW = D // 2 // NCH


def peers():
    dp = lax.axis_index("dp")
    me = lax.axis_index("tp")
    core = lax.rem(me, 2)
    chip = me // 2
    mate = (dp, chip * 2 + (1 - core))
    across = (dp, (1 - chip) * 2 + core)
    return core, mate, across


def say_here(targets):
    barrier = pltpu.get_barrier_semaphore()
    for dev in targets:
        pl.semaphore_signal(barrier, inc=1, device_id=dev, device_id_type=MESH)


def await_peers(count):
    pl.semaphore_wait(pltpu.get_barrier_semaphore(), count)


def rcopy(src, dst, send, recv, dev):
    return pltpu.make_async_remote_copy(src_ref=src, dst_ref=dst, send_sem=send, recv_sem=recv,
                                        device_id=dev, device_id_type=MESH)


def exchange(left, wbuf, wwait, before_sends, pair_scale, mid_work, cross_scale, core, mate, across,
             a_send, a_recv, b_send, b_recv, total, sems, use, first=None):
    sa, ra, sb, rb, sc, rc = sems

    def product(half, j):
        wwait(half, j)
        buf, at = (wbuf, half * NCH + j) if first is None or j > 0 else (first, half)
        return jnp.concatenate([dot(left, buf[at, :, c:c + 2 * HD]) for c in range(0, CW, 2 * HD)], axis=1)

    a_copies = [rcopy(a_send.at[j], a_recv.at[j], sa.at[j], ra.at[j], mate) for j in range(NCH)]
    b_copies = [rcopy(b_send.at[j], b_recv.at[j], sb.at[j], rb.at[j], across) for j in range(NCH)]
    c_copies = [rcopy(total.at[core, j], total.at[core, j], sc.at[j], rc.at[j], mate) for j in range(NCH)]

    def send_across(j, scale):
        a_copies[j].wait_recv()
        b_send[j] = b_send[j] * scale[0] + a_recv[j] * scale[1] if scale else b_send[j] + a_recv[j]
        b_copies[j].start()

    scale = None
    for j in range(NCH):
        a_send[j] = product(1 - core, j)
        if j == 0:
            before_sends()
        a_copies[j].start()
        b_send[j] = product(core, j)
        if j == 1:
            scale = pair_scale()
        if j >= 1:
            send_across(j - 1, scale)
    send_across(NCH - 1, scale)
    mid_work()
    scale = cross_scale()
    for j in range(NCH):
        b_copies[j].wait_recv()
        total[core, j] = b_send[j] * scale[0] + b_recv[j] * scale[1] if scale else b_send[j] + b_recv[j]
        c_copies[j].start()
        if j >= 1:
            c_copies[j - 1].wait_recv()
            use(j - 1)
    c_copies[NCH - 1].wait_recv()
    use(NCH - 1)
    return a_copies + b_copies + c_copies


def exchange_scratch():
    return [
        pltpu.VMEM((2 * NCH, HL * HD, CW), BF16),
        pltpu.VMEM((NCH, B, CW), F32),
        pltpu.VMEM((NCH, B, CW), F32),
        pltpu.VMEM((NCH, B, CW), F32),
        pltpu.VMEM((NCH, B, CW), F32),
        pltpu.VMEM((2, NCH, B, CW), F32),
        pltpu.SemaphoreType.DMA((2 * NCH,)),
        pltpu.SemaphoreType.DMA((NCH,)),
        pltpu.SemaphoreType.DMA((NCH,)),
        pltpu.SemaphoreType.DMA((NCH,)),
        pltpu.SemaphoreType.DMA((NCH,)),
        pltpu.SemaphoreType.DMA((NCH,)),
        pltpu.SemaphoreType.DMA((NCH,)),
    ]


def out_weights(w_ref, wbuf, wsem, core, begin=0):
    def copy(half, j):
        at = half * NCH + j
        cols = pl.ds(pl.multiple_of(at * CW, CW), CW)
        return pltpu.make_async_copy(w_ref.at[:, cols], wbuf.at[at], wsem.at[at])

    def start():
        for j in range(begin, NCH):
            copy(1 - core, j).start()
            copy(core, j).start()

    def wait(half, j):
        if j >= begin:
            copy(half, j).wait()

    return start, wait


WA_ROWS = D * KV * (GQ + 2)
WA_CH = 32
WA_STEP = WA_ROWS // WA_CH
NJ = KV * (GQ + 2)


def mid_kernel(og_ref, ss_ref, h1_ref, g2_ref, alpha_hbm, beta_hbm, len_hbm, wout_ref, wattn_ref,
               k_ref, v_ref, wnext_ref, q_ref, kn_ref, vn_ref, h2_ref, kbuf, vbuf, wnext,
               wbuf, a_send, a_recv, b_send, b_recv, total, wsem, sa, ra, sb, rb, sc, rc,
               wraw, wide, w2, ss_recv, ss_chip, alpha_ref, beta_ref, len_ref, wasem, ss_s, ss_r, csem, psem):
    core, mate, across = peers()
    say_here((mate, across))
    scalars = [pltpu.make_async_copy(src, dst, psem.at[n]) for n, (src, dst) in enumerate(
        ((alpha_hbm, alpha_ref), (beta_hbm, beta_ref), (len_hbm, len_ref)))]
    for cp in scalars:
        cp.start()
    start_w, wait_w = out_weights(wout_ref, wbuf, wsem, core)
    start_w()

    def wa_copy(i):
        return pltpu.make_async_copy(wattn_ref.at[pl.ds(i * WA_STEP, WA_STEP)], wraw.at[i], wasem.at[i])

    def wa_start(i, carry):
        wa_copy(i).start()
        return carry

    lax.fori_loop(0, WA_CH, wa_start, 0)
    caches = [pltpu.make_async_copy(k_ref, kbuf, csem.at[0]), pltpu.make_async_copy(v_ref, vbuf, csem.at[1])]
    caches += [pltpu.make_async_copy(wnext_ref.at[:, pl.ds(h * (D // 2), CW)], wnext.at[h], csem.at[2 + h]) for h in range(2)]
    for cp in caches:
        cp.start()
    ss_mate = rcopy(ss_ref, ss_recv.at[0], ss_s.at[0], ss_r.at[0], mate)
    ss_across = rcopy(ss_chip, ss_recv.at[1], ss_s.at[1], ss_r.at[1], across)

    def before_sends():
        await_peers(2)
        ss_mate.start()

    def root(total_sq, count):
        return jnp.minimum(jnp.sqrt(total_sq[:, 0:1] / count + EPS), 3e38)

    def pair_scale():
        ss_mate.wait_recv()
        both = ss_ref[...] + ss_recv[0]
        ss_chip[...] = both
        ss_across.start()
        inv = lax.rsqrt(both[:, 0:1] / (D // 2) + EPS)
        return root(ss_ref[...], D // 4) * inv, root(ss_recv[0], D // 4) * inv

    def cross_scale():
        for cp in scalars:
            cp.wait()
        ss_across.wait_recv()
        inv = lax.rsqrt((ss_chip[:, 0:1] + ss_recv[1, :, 0:1]) / D + EPS)
        return root(ss_chip[...], D // 2) * inv, root(ss_recv[1], D // 2) * inv

    def relayout():
        def body(i, carry):
            wa_copy(i).wait()
            wide[...] = wraw[i].astype(F32)
            for j in range(NJ):
                w2[j, pl.ds(pl.multiple_of(i * HD, HD), HD), :] = wide[pl.ds(j, HD, stride=NJ), :].astype(BF16)
            return carry
        lax.fori_loop(0, WA_CH, body, 0)

    squares = [jnp.zeros((B, HD), F32)]

    def use(j):
        for half in range(2):
            for p in range(CW // HD):
                cols = slice(half * (D // 2) + j * CW + p * HD, half * (D // 2) + j * CW + (p + 1) * HD)
                a1 = total[half, j, :, p * HD:(p + 1) * HD]
                m = (alpha_ref[0] * h1_ref[:, cols].astype(F32) + beta_ref[0] * a1).astype(BF16)
                h2_ref[:, cols] = m
                x = m.astype(F32)
                squares[0] = squares[0] + x * x

    sent = exchange(og_ref[...], wbuf, wait_w, before_sends, pair_scale, relayout, cross_scale, core, mate, across,
                    a_send, a_recv, b_send, b_recv, total, (sa, ra, sb, rb, sc, rc), use)
    sq = squares[0]
    inv2 = lax.rsqrt(jnp.sum(sq, axis=1, keepdims=True) / D + EPS)
    for c in range(NC):
        m = h2_ref[:, c * HD:(c + 1) * HD].astype(F32)
        h2_ref[:, c * HD:(c + 1) * HD] = (m * inv2 * g2_ref[c:c + 1, :]).astype(BF16)

    pos = jnp.zeros((B, HD), F32)
    row_i = lax.broadcasted_iota(jnp.int32, (B, HD), 0)
    for b in range(B):
        pos = jnp.where(row_i == b, jnp.full((B, HD), len_ref[b]).astype(F32), pos)
    lane = lax.broadcasted_iota(jnp.int32, (B, HD), 1)
    freq = jnp.exp((lane % 32).astype(F32) * (-2.0 * math.log(ROPE_BASE) / 64))
    ang = pos * freq
    rot = lane < 64
    cosv = jnp.where(rot, jnp.cos(ang), 1.0)
    sinv = jnp.sin(ang)
    sin_lo = jnp.where(lane < 32, -sinv, 0.0)
    sin_hi = jnp.where((lane >= 32) & rot, sinv, 0.0)

    def turn(x):
        return x * cosv + pltpu.roll(x, HD - 32, 1) * sin_lo + pltpu.roll(x, 32, 1) * sin_hi

    h2 = h2_ref[...]
    for j in range(GQ + 2):
        w = jnp.concatenate([w2[2 * j], w2[2 * j + 1]], axis=1)
        pr = dot(h2, w)
        for kv in range(KV):
            x = pr[:, kv * HD:(kv + 1) * HD]
            if j < GQ:
                q_ref[pl.ds(kv * GQ + j, B, stride=8), :] = turn(x).astype(BF16).astype(F32)
            elif j == GQ:
                kn_ref[kv] = turn(x).astype(BF16).astype(F32)
            else:
                vn_ref[kv] = x.astype(BF16).astype(F32)
    for cp in caches:
        cp.wait()
    for cp in sent + [ss_mate, ss_across]:
        cp.wait_send()


def middle(og, ss, h1, g2, alpha, beta, cache_len, w_out, w_attn, k_cache, v_cache, w_next):
    return pl.pallas_call(
        mid_kernel,
        out_shape=[jax.ShapeDtypeStruct((B * 8, HD), F32), jax.ShapeDtypeStruct((KV, B, HD), F32),
                   jax.ShapeDtypeStruct((KV, B, HD), F32), jax.ShapeDtypeStruct((B, D), BF16),
                   pltpu.VMEM((B, KV, T, HD), BF16), pltpu.VMEM((B, KV, T, HD), BF16),
                   pltpu.VMEM((2, HL * HD, CW), BF16)],
        in_specs=[vmem_spec(), vmem_spec(), vmem_spec(), vmem_spec(), any_spec(), any_spec(), any_spec(),
                  any_spec(), any_spec(), any_spec(), any_spec(), any_spec()],
        out_specs=[vmem_spec()] * 7,
        scratch_shapes=exchange_scratch() + [
            pltpu.VMEM((WA_CH, WA_STEP, HD), BF16),
            pltpu.VMEM((WA_STEP, HD), F32),
            pltpu.VMEM((NJ, D, HD), BF16),
            pltpu.VMEM((2, B, HD), F32),
            pltpu.VMEM((B, HD), F32),
            pltpu.SMEM((2,), F32),
            pltpu.SMEM((2,), F32),
            pltpu.SMEM((B,), jnp.int32),
            pltpu.SemaphoreType.DMA((WA_CH,)),
            pltpu.SemaphoreType.DMA((2,)),
            pltpu.SemaphoreType.DMA((2,)),
            pltpu.SemaphoreType.DMA((4,)),
            pltpu.SemaphoreType.DMA((3,)),
        ],
        compiler_params=pltpu.CompilerParams(vmem_limit_bytes=35 * MIB, collective_id=0, has_side_effects=True),
        name="middle",
    )(og, ss, h1, g2, alpha, beta, cache_len, w_out, w_attn, k_cache, v_cache, w_next)


ROWS = 4
ROWS_MM = 8


def attention_kernel(len_ref, q_ref, kn_ref, vn_ref, kin_ref, vin_ref, at_ref, ko_ref, vo_ref, kbuf, vbuf, osem):
    def outs(b):
        return (pltpu.make_async_copy(kbuf.at[b], ko_ref.at[b], osem.at[0, b]),
                pltpu.make_async_copy(vbuf.at[b], vo_ref.at[b], osem.at[1, b]))

    row8 = lax.broadcasted_iota(jnp.int32, (8, HD), 0)
    row16 = lax.broadcasted_iota(jnp.int32, (16, HD), 0)
    tpos = lax.broadcasted_iota(jnp.int32, (8, T), 1)

    def insert(i, carry):
        rows = [i * ROWS + r for r in range(ROWS)]
        for b in rows:
            p = len_ref[b]
            base = pl.multiple_of((p // 16) * 16, 16)
            hit = row16 == p - base
            for kv in range(KV):
                for buf, new in ((kbuf, kn_ref), (vbuf, vn_ref)):
                    old = buf[b, kv, pl.ds(base, 16), :].astype(F32)
                    buf[b, kv, pl.ds(base, 16), :] = jnp.where(hit, new[kv, pl.ds(b, 1), :], old).astype(BF16)
        for b in rows:
            for cp in outs(b):
                cp.start()
        return carry

    lax.fori_loop(0, B // ROWS, insert, 0)

    def body(i, carry):
        rows = [i * ROWS_MM + r for r in range(ROWS_MM)]
        lens = [len_ref[b] for b in rows]
        scores = []
        for b, p in zip(rows, lens):
            q = q_ref[pl.ds(b * 8, 8), :]
            q2 = jnp.concatenate([jnp.where(row8 < 4, q, 0.0), jnp.where(row8 < 4, 0.0, q)], axis=1).astype(BF16)
            k2 = jnp.concatenate([kbuf[b, 0], kbuf[b, 1]], axis=1)
            s = lax.dot_general(q2, k2, (((1,), (1,)), ((), ())), preferred_element_type=F32) * HD ** -0.5
            scores.append(jnp.where(tpos <= p, s, -jnp.inf))
        tops = [jnp.max(s, axis=1, keepdims=True) for s in scores]
        es = [jnp.exp(s - m) for s, m in zip(scores, tops)]
        sums = [jnp.sum(e, axis=1, keepdims=True) for e in es]
        prs = [(e / z).astype(BF16) for e, z in zip(es, sums)]
        for b, pr in zip(rows, prs):
            o = dot(pr, jnp.concatenate([vbuf[b, 0], vbuf[b, 1]], axis=1))
            at_ref[pl.ds(b * 8, 8), :] = jnp.where(row8 < 4, o[:, 0:HD], o[:, HD:])
        return carry

    lax.fori_loop(0, B // ROWS_MM, body, 0)

    def drain(b, carry):
        for cp in outs(b):
            cp.wait()
        return carry

    lax.fori_loop(0, B, drain, 0)


def attention(cache_len, q, kn, vn, kbuf, vbuf):
    return pl.pallas_call(
        attention_kernel,
        out_shape=[jax.ShapeDtypeStruct((B * 8, HD), F32), pltpu.HBM((B, KV, T, HD), BF16),
                   pltpu.HBM((B, KV, T, HD), BF16), pltpu.VMEM((B, KV, T, HD), BF16), pltpu.VMEM((B, KV, T, HD), BF16)],
        in_specs=[smem_spec(), vmem_spec(), vmem_spec(), vmem_spec(), vmem_spec(), vmem_spec()],
        out_specs=[vmem_spec(), any_spec(), any_spec(), vmem_spec(), vmem_spec()],
        input_output_aliases={4: 3, 5: 4},
        scratch_shapes=[pltpu.SemaphoreType.DMA((2, B))],
        compiler_params=pltpu.CompilerParams(vmem_limit_bytes=4 * MIB),
        name="attention",
    )(cache_len, q, kn, vn, kbuf, vbuf)[:3]


def last_kernel(at_ref, h2_ref, alpha_hbm, beta_hbm, wout_ref, first_ref, out_ref,
                wbuf, a_send, a_recv, b_send, b_recv, total, wsem, sa, ra, sb, rb, sc, rc,
                alpha_ref, beta_ref, psem):
    core, mate, across = peers()
    say_here((mate, across))
    scalars = [pltpu.make_async_copy(alpha_hbm, alpha_ref, psem.at[0]), pltpu.make_async_copy(beta_hbm, beta_ref, psem.at[1])]
    for cp in scalars:
        cp.start()
    start_w, wait_w = out_weights(wout_ref, wbuf, wsem, core, begin=1)
    start_w()
    left = jnp.concatenate([at_ref[pl.ds(j, B, stride=8), :].astype(BF16) for j in range(8)], axis=1)
    def settle():
        for cp in scalars:
            cp.wait()

    def use(j):
        for half in range(2):
            cols = slice(half * (D // 2) + j * CW, half * (D // 2) + (j + 1) * CW)
            out_ref[:, cols] = (alpha_ref[1] * h2_ref[:, cols].astype(F32) + beta_ref[1] * total[half, j]).astype(BF16)

    sent = exchange(left, wbuf, wait_w, lambda: await_peers(2), lambda: None, settle, lambda: None, core, mate,
                    across, a_send, a_recv, b_send, b_recv, total, (sa, ra, sb, rb, sc, rc), use, first=first_ref)
    for cp in sent:
        cp.wait_send()


def last(at, h2, alpha, beta, w_out, w_first):
    return pl.pallas_call(
        last_kernel,
        out_shape=jax.ShapeDtypeStruct((B, D), BF16),
        in_specs=[vmem_spec(), vmem_spec(), any_spec(), any_spec(), any_spec(), vmem_spec()],
        out_specs=vmem_spec(),
        scratch_shapes=exchange_scratch() + [pltpu.SMEM((2,), F32), pltpu.SMEM((2,), F32), pltpu.SemaphoreType.DMA((2,))],
        compiler_params=pltpu.CompilerParams(vmem_limit_bytes=16 * MIB, collective_id=1, has_side_effects=True),
        name="last",
    )(at, h2, alpha, beta, w_out, w_first)


def solution(mesh):
    row_spec = P('dp', None)
    cache_spec = P('dp', 'tp', None, None)
    in_specs = (row_spec, P('dp'), cache_spec, cache_spec, cache_spec, P(None), P(None, None, 'tp', None),
                P(None, 'tp', None), P('tp'), P('tp', None), P('tp', None, None), P(None),
                P(None, 'tp', None, None), P('tp', None, None), P(None), P(None))
    out_specs = (row_spec, cache_spec, cache_spec, cache_spec)

    def local_step(hidden, cache_len, lin_state, k_cache, v_cache, norm_first, w_qkv, w_gate, slopes, out_norm,
                   w_out_lin, norm_second, w_attn, w_out_attn, mix_alpha, mix_beta):
        def hbm(x):
            return pltpu.with_memory_space_constraint(x, pltpu.HBM)

        g1 = norm_first.reshape(NC, HD)
        g2 = norm_second.reshape(NC, HD)
        wa = jnp.transpose(w_attn, (0, 2, 1, 3)).reshape(WA_ROWS, HD)
        state_out, og, ss, h1 = lightning(hbm(hidden), hbm(g1), hbm(slopes), hbm(out_norm), hbm(lin_state), hbm(w_qkv), hbm(w_gate))
        w_last = hbm(w_out_attn.reshape(HL * HD, D))
        q, kn, vn, h2, kbuf, vbuf, w_first = middle(og, ss, h1, g2, hbm(mix_alpha), hbm(mix_beta), hbm(cache_len),
                                                    hbm(w_out_lin.reshape(HL * HD, D)), hbm(wa), hbm(k_cache),
                                                    hbm(v_cache), w_last)
        at, k_out, v_out = attention(cache_len, q, kn, vn, kbuf, vbuf)
        hidden_out = last(at, h2, hbm(mix_alpha), hbm(mix_beta), w_last, w_first)
        return hidden_out, state_out, k_out, v_out

    return jax.shard_map(local_step, mesh=mesh, in_specs=in_specs, out_specs=out_specs, check_vma=False)
```

```python
import functools
import math

import jax
import jax.numpy as jnp
from jax import lax
from jax.experimental import pallas as pl
from jax.experimental.pallas import tpu as pltpu
from jax.sharding import PartitionSpec as P

EPS = 1e-5
ROPE_BASE = 10000000.0
MESH = pl.DeviceIdType.MESH
F32 = jnp.float32
BF16 = jnp.bfloat16
MIB = 1024 * 1024

B = 32
D = 4096
HL = 8
HD = 128
KV = 2
GQ = 4
T = 512
NC = D // HD

DCH = 512
STEPS = D // DCH
LCH = DCH * HL // 2 // HD
RING = 3
EARLY = 24


def any_spec():
    return pl.BlockSpec(memory_space=pl.ANY)


def vmem_spec():
    return pl.BlockSpec(memory_space=pltpu.VMEM)


def smem_spec():
    return pl.BlockSpec(memory_space=pltpu.SMEM)


def dot(a, b):
    return jnp.dot(a, b, preferred_element_type=F32)


def lightning_kernel(hid_hbm, g1_hbm, slopes_hbm, onorm_hbm, state_ref, wqkv_ref, wgate_ref,
                     sout_ref, og_ref, ss_ref, h1_ref, hid_ref, g1_ref, onorm_ref, slopes_ref,
                     wbuf, gbuf, sbuf, hstack, ebuf, lbuf_a, lbuf_b, acc, kq_t, v_s, o_s, psem, wsem, ssem, osem):
    def w_copies(step, slot):
        rows = pl.ds(step * DCH, DCH)
        return (pltpu.make_async_copy(wqkv_ref.at[rows], wbuf.at[slot], wsem.at[slot, 0]),
                pltpu.make_async_copy(wgate_ref.at[rows], gbuf.at[slot], wsem.at[slot, 1]))

    def s_copy(b):
        return pltpu.make_async_copy(state_ref.at[b], sbuf.at[b], ssem.at[b])

    def o_copy(b):
        return pltpu.make_async_copy(sbuf.at[b], sout_ref.at[b], osem.at[b])

    small = [pltpu.make_async_copy(src, dst, psem.at[n]) for n, (src, dst) in enumerate(
        ((hid_hbm, hid_ref), (g1_hbm, g1_ref), (onorm_hbm, onorm_ref), (slopes_hbm, slopes_ref)))]
    for cp in small:
        cp.start()
    for i in range(RING):
        for cp in w_copies(i, i):
            cp.start()
    for cp in small:
        cp.wait()

    sq = jnp.zeros((B, HD), F32)
    for c in range(NC):
        x = hid_ref[:, c * HD:(c + 1) * HD].astype(F32)
        sq = sq + x * x
    inv = lax.rsqrt(jnp.sum(sq, axis=1, keepdims=True) / D + EPS)
    rr = lax.broadcasted_iota(jnp.int32, (HD, 256), 1)
    dd = lax.broadcasted_iota(jnp.int32, (HD, 256), 0)
    for c in range(NC):
        x = hid_ref[:, c * HD:(c + 1) * HD].astype(F32)
        h1 = (x * inv * g1_ref[c:c + 1, :]).astype(BF16)
        h1_ref[:, c * HD:(c + 1) * HD] = h1
        hstack[c * B:(c + 1) * B, :] = h1
    for n in range(4):
        spread = jnp.where(rr // 8 + 32 * n == dd, 1.0, 0.0).astype(BF16)
        for c in range(NC // 8):
            e = dot(hstack[c * 256:(c + 1) * 256, :], spread).astype(BF16)
            for k in range(8):
                for m in range(2):
                    ebuf[(c * 8 + k) * 8 + n * 2 + m] = e[k * B:(k + 1) * B, m * HD:(m + 1) * HD]

    acc[...] = jnp.zeros_like(acc)
    half = DCH * HL // 2
    lane = lax.broadcasted_iota(jnp.int32, (B, HD), 1) % 8

    def spread_heads(dst, part):
        for h in range(HL):
            keep = jnp.where(lane == h, 1.0, 0.0).astype(BF16)
            for q in range(LCH):
                dst[q, h * B:(h + 1) * B, :] = ebuf[part * LCH + q] * keep

    spread_heads(lbuf_a, 0)

    def step_fn(i, carry):
        slot = lax.rem(i, RING)

        @pl.when(i >= STEPS - RING)
        def _():
            for k in range(EARLY // RING):
                s_copy((i - (STEPS - RING)) * (EARLY // RING) + k).start()

        for cp in w_copies(i, slot):
            cp.wait()

        def product(left, part, pair):
            rows = slice(part * DCH // 2, (part + 1) * DCH // 2)
            second = wbuf[slot, rows, 1] if pair == 0 else gbuf[slot, rows]
            right = jnp.concatenate([wbuf[slot, rows, 2 * pair].reshape(half, HD), second.reshape(half, HD)], axis=1)
            return dot(left, right)

        spread_heads(lbuf_b, 2 * i + 1)
        left_a = jnp.concatenate([lbuf_a[q] for q in range(LCH)], axis=1)
        first = [product(left_a, 0, pair) for pair in range(2)]
        spread_heads(lbuf_a, jnp.minimum(2 * i + 2, 2 * STEPS - 1))
        left_b = jnp.concatenate([lbuf_b[q] for q in range(LCH)], axis=1)
        for pair in range(2):
            acc[pair] += first[pair] + product(left_b, 1, pair)

        @pl.when(i + RING < STEPS)
        def _():
            for cp in w_copies(i + RING, slot):
                cp.start()
        return carry

    lax.fori_loop(0, STEPS, step_fn, 0)
    for b in range(EARLY, B):
        s_copy(b).start()

    for h in range(HL):
        rows = slice(h * B, (h + 1) * B)
        q = jax.nn.silu(acc[0, rows, 0:HD]).astype(BF16)
        k = jax.nn.silu(acc[0, rows, HD:2 * HD]).astype(BF16)
        v = jax.nn.silu(acc[1, rows, 0:HD]).astype(BF16)
        qk = jnp.concatenate([k, q], axis=0).astype(F32)
        both = jnp.transpose(qk).astype(BF16)
        kq_t[h] = jnp.concatenate([both[:, 0:B], both[:, B:]], axis=0)
        v_s[h] = v.astype(F32)

    brow = lax.broadcasted_iota(jnp.int32, (B, 2 * HD), 0)
    bcol = lax.broadcasted_iota(jnp.int32, (B, 2 * HD), 1) // HD

    def row_fn(i, carry):
        for r in range(2):
            s_copy(2 * i + r).wait()
        pick = jnp.where(brow == 2 * i + bcol, 1.0, 0.0).astype(BF16)
        for h in range(HL):
            kq = dot(kq_t[h], pick)
            decay = jnp.exp(jnp.full((1, HD), -slopes_ref[h], F32))
            for r in range(2):
                b = 2 * i + r
                lanes = slice(r * HD, (r + 1) * HD)
                new = decay * sbuf[b, h] + kq[0:HD, lanes] * v_s[h, pl.ds(b, 1), :]
                sbuf[b, h] = new
                o_s[b, h:h + 1, :] = jnp.sum(kq[HD:, lanes] * new, axis=0, keepdims=True)
        for r in range(2):
            o_copy(2 * i + r).start()
        return carry

    lax.fori_loop(0, B // 2, row_fn, 0)

    ss = jnp.zeros((B, HD), F32)
    for h in range(HL):
        o = o_s[:, h, :]
        ss = ss + o * o
    ss = jnp.sum(ss, axis=1, keepdims=True)
    ss_ref[...] = jnp.broadcast_to(ss, (B, HD))
    inv_own = lax.rsqrt(ss / (HL * HD) + EPS)
    for h in range(HL):
        gate = jax.nn.sigmoid(acc[1, h * B:(h + 1) * B, HD:2 * HD])
        og_ref[:, h * HD:(h + 1) * HD] = (o_s[:, h, :] * inv_own * onorm_ref[h:h + 1, :] * gate).astype(BF16)

    def drain(b, carry):
        o_copy(b).wait()
        return carry

    lax.fori_loop(0, B, drain, 0)


def lightning(hidden, g1, slopes, out_norm, lin_state, w_qkv, w_gate):
    return pl.pallas_call(
        lightning_kernel,
        out_shape=[jax.ShapeDtypeStruct((B, HL, HD, HD), F32), jax.ShapeDtypeStruct((B, HL * HD), BF16),
                   jax.ShapeDtypeStruct((B, HD), F32), jax.ShapeDtypeStruct((B, D), BF16)],
        in_specs=[any_spec()] * 7,
        out_specs=[any_spec(), vmem_spec(), vmem_spec(), vmem_spec()],
        scratch_shapes=[
            pltpu.VMEM((B, D), BF16),
            pltpu.VMEM((NC, HD), F32),
            pltpu.VMEM((HL, HD), F32),
            pltpu.SMEM((HL,), F32),
            pltpu.VMEM((RING, DCH, 3, HL, HD), BF16),
            pltpu.VMEM((RING, DCH, HL, HD), BF16),
            pltpu.VMEM((B, HL, HD, HD), F32),
            pltpu.VMEM((NC * B, HD), BF16),
            pltpu.VMEM((2 * STEPS * LCH, B, HD), BF16),
            pltpu.VMEM((LCH, HL * B, HD), BF16),
            pltpu.VMEM((LCH, HL * B, HD), BF16),
            pltpu.VMEM((2, HL * B, 2 * HD), F32),
            pltpu.VMEM((HL, 2 * HD, B), BF16),
            pltpu.VMEM((HL, B, HD), F32),
            pltpu.VMEM((B, HL, HD), F32),
            pltpu.SemaphoreType.DMA((4,)),
            pltpu.SemaphoreType.DMA((RING, 2)),
            pltpu.SemaphoreType.DMA((B,)),
            pltpu.SemaphoreType.DMA((B,)),
        ],
        compiler_params=pltpu.CompilerParams(vmem_limit_bytes=40 * MIB),
        name="lightning",
    )(hidden, g1, slopes, out_norm, lin_state, w_qkv, w_gate)


MID_CHUNKS = 4
LAST_CHUNKS = 8


def peers():
    dp = lax.axis_index("dp")
    me = lax.axis_index("tp")
    core = lax.rem(me, 2)
    chip = me // 2
    mate = (dp, chip * 2 + (1 - core))
    across = (dp, (1 - chip) * 2 + core)
    return core, mate, across


def say_here(targets):
    barrier = pltpu.get_barrier_semaphore()
    for dev in targets:
        pl.semaphore_signal(barrier, inc=1, device_id=dev, device_id_type=MESH)


def await_peers(count):
    pl.semaphore_wait(pltpu.get_barrier_semaphore(), count)


def rcopy(src, dst, send, recv, dev):
    return pltpu.make_async_remote_copy(src_ref=src, dst_ref=dst, send_sem=send, recv_sem=recv,
                                        device_id=dev, device_id_type=MESH)


def exchange(left, wbuf, wwait, before_sends, pair_scale, mid_work, cross_scale, core, mate, across,
             a_send, a_recv, b_send, b_recv, total, sems, use, nch, first=None):
    sa, ra, sb, rb, sc, rc = sems
    width = D // 2 // nch

    def product(half, j):
        wwait(half, j)
        buf, at = (wbuf, half * nch + j) if first is None or j > 0 else (first, half)
        return jnp.concatenate([dot(left, buf[at, :, c:c + 2 * HD]) for c in range(0, width, 2 * HD)], axis=1)

    a_copies = [rcopy(a_send.at[j], a_recv.at[j], sa.at[j], ra.at[j], mate) for j in range(nch)]
    b_copies = [rcopy(b_send.at[j], b_recv.at[j], sb.at[j], rb.at[j], across) for j in range(nch)]
    c_copies = [rcopy(total.at[core, j], total.at[core, j], sc.at[j], rc.at[j], mate) for j in range(nch)]

    def send_across(j, scale):
        a_copies[j].wait_recv()
        b_send[j] = b_send[j] * scale[0] + a_recv[j] * scale[1] if scale else b_send[j] + a_recv[j]
        b_copies[j].start()

    scale = None
    for j in range(nch):
        a_send[j] = product(1 - core, j)
        if j == 0:
            before_sends()
        a_copies[j].start()
        b_send[j] = product(core, j)
        if j == 1:
            scale = pair_scale()
        if j >= 1:
            send_across(j - 1, scale)
    send_across(nch - 1, scale)
    mid_work()
    scale = cross_scale()
    for j in range(nch):
        b_copies[j].wait_recv()
        total[core, j] = b_send[j] * scale[0] + b_recv[j] * scale[1] if scale else b_send[j] + b_recv[j]
        c_copies[j].start()
        if j >= 1:
            c_copies[j - 1].wait_recv()
            use(j - 1)
    c_copies[nch - 1].wait_recv()
    use(nch - 1)
    return a_copies + b_copies + c_copies


def exchange_scratch(nch):
    width = D // 2 // nch
    return [
        pltpu.VMEM((2 * nch, HL * HD, width), BF16),
        pltpu.VMEM((nch, B, width), F32),
        pltpu.VMEM((nch, B, width), F32),
        pltpu.VMEM((nch, B, width), F32),
        pltpu.VMEM((nch, B, width), F32),
        pltpu.VMEM((2, nch, B, width), F32),
        pltpu.SemaphoreType.DMA((2 * nch,)),
        pltpu.SemaphoreType.DMA((nch,)),
        pltpu.SemaphoreType.DMA((nch,)),
        pltpu.SemaphoreType.DMA((nch,)),
        pltpu.SemaphoreType.DMA((nch,)),
        pltpu.SemaphoreType.DMA((nch,)),
        pltpu.SemaphoreType.DMA((nch,)),
    ]


def out_weights(w_ref, wbuf, wsem, core, nch, begin=0):
    width = D // 2 // nch

    def copy(half, j):
        at = half * nch + j
        cols = pl.ds(pl.multiple_of(at * width, width), width)
        return pltpu.make_async_copy(w_ref.at[:, cols], wbuf.at[at], wsem.at[at])

    def start():
        for j in range(begin, nch):
            copy(1 - core, j).start()
            copy(core, j).start()

    def wait(half, j):
        if j >= begin:
            copy(half, j).wait()

    return start, wait


WA_ROWS = D * KV * (GQ + 2)
WA_CH = 32
WA_STEP = WA_ROWS // WA_CH
NJ = KV * (GQ + 2)


def mid_kernel(og_ref, ss_ref, h1_ref, g2_ref, alpha_hbm, beta_hbm, len_hbm, wout_ref, wattn_ref,
               k_ref, v_ref, wnext_ref, q_ref, kn_ref, vn_ref, h2_ref, kbuf, vbuf, wnext,
               wbuf, a_send, a_recv, b_send, b_recv, total, wsem, sa, ra, sb, rb, sc, rc,
               wraw, wide, w2, ss_recv, ss_chip, alpha_ref, beta_ref, len_ref, wasem, ss_s, ss_r, csem, psem):
    core, mate, across = peers()
    say_here((mate, across))
    scalars = [pltpu.make_async_copy(src, dst, psem.at[n]) for n, (src, dst) in enumerate(
        ((alpha_hbm, alpha_ref), (beta_hbm, beta_ref), (len_hbm, len_ref)))]
    for cp in scalars:
        cp.start()
    start_w, wait_w = out_weights(wout_ref, wbuf, wsem, core, MID_CHUNKS)
    start_w()

    def wa_copy(i):
        return pltpu.make_async_copy(wattn_ref.at[pl.ds(i * WA_STEP, WA_STEP)], wraw.at[i], wasem.at[i])

    def wa_start(i, carry):
        wa_copy(i).start()
        return carry

    lax.fori_loop(0, WA_CH, wa_start, 0)
    caches = [pltpu.make_async_copy(k_ref, kbuf, csem.at[0]), pltpu.make_async_copy(v_ref, vbuf, csem.at[1])]
    caches += [pltpu.make_async_copy(wnext_ref.at[:, pl.ds(h * (D // 2), D // 2 // LAST_CHUNKS)], wnext.at[h], csem.at[2 + h]) for h in range(2)]
    for cp in caches:
        cp.start()
    ss_mate = rcopy(ss_ref, ss_recv.at[0], ss_s.at[0], ss_r.at[0], mate)
    ss_across = rcopy(ss_chip, ss_recv.at[1], ss_s.at[1], ss_r.at[1], across)

    def before_sends():
        await_peers(2)
        ss_mate.start()

    def root(total_sq, count):
        return jnp.minimum(jnp.sqrt(total_sq[:, 0:1] / count + EPS), 3e38)

    def pair_scale():
        ss_mate.wait_recv()
        both = ss_ref[...] + ss_recv[0]
        ss_chip[...] = both
        ss_across.start()
        inv = lax.rsqrt(both[:, 0:1] / (D // 2) + EPS)
        return root(ss_ref[...], D // 4) * inv, root(ss_recv[0], D // 4) * inv

    def cross_scale():
        for cp in scalars:
            cp.wait()
        ss_across.wait_recv()
        inv = lax.rsqrt((ss_chip[:, 0:1] + ss_recv[1, :, 0:1]) / D + EPS)
        return root(ss_chip[...], D // 2) * inv, root(ss_recv[1], D // 2) * inv

    def relayout():
        def body(i, carry):
            wa_copy(i).wait()
            wide[...] = wraw[i].astype(F32)
            for j in range(NJ):
                w2[j, pl.ds(pl.multiple_of(i * HD, HD), HD), :] = wide[pl.ds(j, HD, stride=NJ), :].astype(BF16)
            return carry
        lax.fori_loop(0, WA_CH, body, 0)

    squares = [jnp.zeros((B, HD), F32)]

    def use(j):
        wide_cols = D // 2 // MID_CHUNKS
        for half in range(2):
            for p in range(wide_cols // HD):
                cols = slice(half * (D // 2) + j * wide_cols + p * HD, half * (D // 2) + j * wide_cols + (p + 1) * HD)
                a1 = total[half, j, :, p * HD:(p + 1) * HD]
                m = (alpha_ref[0] * h1_ref[:, cols].astype(F32) + beta_ref[0] * a1).astype(BF16)
                h2_ref[:, cols] = m
                x = m.astype(F32)
                squares[0] = squares[0] + x * x

    sent = exchange(og_ref[...], wbuf, wait_w, before_sends, pair_scale, relayout, cross_scale, core, mate, across,
                    a_send, a_recv, b_send, b_recv, total, (sa, ra, sb, rb, sc, rc), use, MID_CHUNKS)
    sq = squares[0]
    inv2 = lax.rsqrt(jnp.sum(sq, axis=1, keepdims=True) / D + EPS)
    for c in range(NC):
        m = h2_ref[:, c * HD:(c + 1) * HD].astype(F32)
        h2_ref[:, c * HD:(c + 1) * HD] = (m * inv2 * g2_ref[c:c + 1, :]).astype(BF16)

    pos = jnp.zeros((B, HD), F32)
    row_i = lax.broadcasted_iota(jnp.int32, (B, HD), 0)
    for b in range(B):
        pos = jnp.where(row_i == b, jnp.full((B, HD), len_ref[b]).astype(F32), pos)
    lane = lax.broadcasted_iota(jnp.int32, (B, HD), 1)
    freq = jnp.exp((lane % 32).astype(F32) * (-2.0 * math.log(ROPE_BASE) / 64))
    ang = pos * freq
    rot = lane < 64
    cosv = jnp.where(rot, jnp.cos(ang), 1.0)
    sinv = jnp.sin(ang)
    sin_lo = jnp.where(lane < 32, -sinv, 0.0)
    sin_hi = jnp.where((lane >= 32) & rot, sinv, 0.0)

    def turn(x):
        return x * cosv + pltpu.roll(x, HD - 32, 1) * sin_lo + pltpu.roll(x, 32, 1) * sin_hi

    h2 = h2_ref[...]
    for j in range(GQ + 2):
        w = jnp.concatenate([w2[2 * j], w2[2 * j + 1]], axis=1)
        pr = dot(h2, w)
        for kv in range(KV):
            x = pr[:, kv * HD:(kv + 1) * HD]
            if j < GQ:
                q_ref[pl.ds(kv * GQ + j, B, stride=8), :] = turn(x).astype(BF16).astype(F32)
            elif j == GQ:
                kn_ref[kv] = turn(x).astype(BF16).astype(F32)
            else:
                vn_ref[kv] = x.astype(BF16).astype(F32)
    for cp in caches:
        cp.wait()
    for cp in sent + [ss_mate, ss_across]:
        cp.wait_send()


def middle(og, ss, h1, g2, alpha, beta, cache_len, w_out, w_attn, k_cache, v_cache, w_next):
    return pl.pallas_call(
        mid_kernel,
        out_shape=[jax.ShapeDtypeStruct((B * 8, HD), F32), jax.ShapeDtypeStruct((KV, B, HD), F32),
                   jax.ShapeDtypeStruct((KV, B, HD), F32), jax.ShapeDtypeStruct((B, D), BF16),
                   pltpu.VMEM((B, KV, T, HD), BF16), pltpu.VMEM((B, KV, T, HD), BF16),
                   pltpu.VMEM((2, HL * HD, D // 2 // LAST_CHUNKS), BF16)],
        in_specs=[vmem_spec(), vmem_spec(), vmem_spec(), vmem_spec(), any_spec(), any_spec(), any_spec(),
                  any_spec(), any_spec(), any_spec(), any_spec(), any_spec()],
        out_specs=[vmem_spec()] * 7,
        scratch_shapes=exchange_scratch(MID_CHUNKS) + [
            pltpu.VMEM((WA_CH, WA_STEP, HD), BF16),
            pltpu.VMEM((WA_STEP, HD), F32),
            pltpu.VMEM((NJ, D, HD), BF16),
            pltpu.VMEM((2, B, HD), F32),
            pltpu.VMEM((B, HD), F32),
            pltpu.SMEM((2,), F32),
            pltpu.SMEM((2,), F32),
            pltpu.SMEM((B,), jnp.int32),
            pltpu.SemaphoreType.DMA((WA_CH,)),
            pltpu.SemaphoreType.DMA((2,)),
            pltpu.SemaphoreType.DMA((2,)),
            pltpu.SemaphoreType.DMA((4,)),
            pltpu.SemaphoreType.DMA((3,)),
        ],
        compiler_params=pltpu.CompilerParams(vmem_limit_bytes=35 * MIB, collective_id=0, has_side_effects=True),
        name="middle",
    )(og, ss, h1, g2, alpha, beta, cache_len, w_out, w_attn, k_cache, v_cache, w_next)


ROWS = 4
ROWS_MM = 8


def attention_kernel(len_ref, q_ref, kn_ref, vn_ref, kin_ref, vin_ref, at_ref, ko_ref, vo_ref, kbuf, vbuf, osem):
    def outs(b):
        return (pltpu.make_async_copy(kbuf.at[b], ko_ref.at[b], osem.at[0, b]),
                pltpu.make_async_copy(vbuf.at[b], vo_ref.at[b], osem.at[1, b]))

    row8 = lax.broadcasted_iota(jnp.int32, (8, HD), 0)
    row16 = lax.broadcasted_iota(jnp.int32, (16, HD), 0)
    tpos = lax.broadcasted_iota(jnp.int32, (8, T), 1)

    def insert(i, carry):
        rows = [i * ROWS + r for r in range(ROWS)]
        for b in rows:
            p = len_ref[b]
            base = pl.multiple_of((p // 16) * 16, 16)
            hit = row16 == p - base
            for kv in range(KV):
                for buf, new in ((kbuf, kn_ref), (vbuf, vn_ref)):
                    old = buf[b, kv, pl.ds(base, 16), :].astype(F32)
                    buf[b, kv, pl.ds(base, 16), :] = jnp.where(hit, new[kv, pl.ds(b, 1), :], old).astype(BF16)
        for b in rows:
            for cp in outs(b):
                cp.start()
        return carry

    lax.fori_loop(0, B // ROWS, insert, 0)

    def body(i, carry):
        rows = [i * ROWS_MM + r for r in range(ROWS_MM)]
        lens = [len_ref[b] for b in rows]
        scores = []
        for b, p in zip(rows, lens):
            q = q_ref[pl.ds(b * 8, 8), :]
            q2 = jnp.concatenate([jnp.where(row8 < 4, q, 0.0), jnp.where(row8 < 4, 0.0, q)], axis=1).astype(BF16)
            k2 = jnp.concatenate([kbuf[b, 0], kbuf[b, 1]], axis=1)
            s = lax.dot_general(q2, k2, (((1,), (1,)), ((), ())), preferred_element_type=F32) * HD ** -0.5
            scores.append(jnp.where(tpos <= p, s, -jnp.inf))
        tops = [jnp.max(s, axis=1, keepdims=True) for s in scores]
        es = [jnp.exp(s - m) for s, m in zip(scores, tops)]
        sums = [jnp.sum(e, axis=1, keepdims=True) for e in es]
        prs = [(e / z).astype(BF16) for e, z in zip(es, sums)]
        for b, pr in zip(rows, prs):
            o = dot(pr, jnp.concatenate([vbuf[b, 0], vbuf[b, 1]], axis=1))
            at_ref[pl.ds(b * 8, 8), :] = jnp.where(row8 < 4, o[:, 0:HD], o[:, HD:])
        return carry

    lax.fori_loop(0, B // ROWS_MM, body, 0)

    def drain(b, carry):
        for cp in outs(b):
            cp.wait()
        return carry

    lax.fori_loop(0, B, drain, 0)


def attention(cache_len, q, kn, vn, kbuf, vbuf):
    return pl.pallas_call(
        attention_kernel,
        out_shape=[jax.ShapeDtypeStruct((B * 8, HD), F32), pltpu.HBM((B, KV, T, HD), BF16),
                   pltpu.HBM((B, KV, T, HD), BF16), pltpu.VMEM((B, KV, T, HD), BF16), pltpu.VMEM((B, KV, T, HD), BF16)],
        in_specs=[smem_spec(), vmem_spec(), vmem_spec(), vmem_spec(), vmem_spec(), vmem_spec()],
        out_specs=[vmem_spec(), any_spec(), any_spec(), vmem_spec(), vmem_spec()],
        input_output_aliases={4: 3, 5: 4},
        scratch_shapes=[pltpu.SemaphoreType.DMA((2, B))],
        compiler_params=pltpu.CompilerParams(vmem_limit_bytes=4 * MIB),
        name="attention",
    )(cache_len, q, kn, vn, kbuf, vbuf)[:3]


def last_kernel(at_ref, h2_ref, alpha_hbm, beta_hbm, wout_ref, first_ref, out_ref,
                wbuf, a_send, a_recv, b_send, b_recv, total, wsem, sa, ra, sb, rb, sc, rc,
                alpha_ref, beta_ref, psem):
    core, mate, across = peers()
    say_here((mate, across))
    scalars = [pltpu.make_async_copy(alpha_hbm, alpha_ref, psem.at[0]), pltpu.make_async_copy(beta_hbm, beta_ref, psem.at[1])]
    for cp in scalars:
        cp.start()
    start_w, wait_w = out_weights(wout_ref, wbuf, wsem, core, LAST_CHUNKS, begin=1)
    start_w()
    left = jnp.concatenate([at_ref[pl.ds(j, B, stride=8), :].astype(BF16) for j in range(8)], axis=1)
    def settle():
        for cp in scalars:
            cp.wait()

    def use(j):
        for half in range(2):
            at = half * (D // 2) + j * (D // 2 // LAST_CHUNKS)
            cols = slice(at, at + D // 2 // LAST_CHUNKS)
            out_ref[:, cols] = (alpha_ref[1] * h2_ref[:, cols].astype(F32) + beta_ref[1] * total[half, j]).astype(BF16)

    sent = exchange(left, wbuf, wait_w, lambda: await_peers(2), lambda: None, settle, lambda: None, core, mate,
                    across, a_send, a_recv, b_send, b_recv, total, (sa, ra, sb, rb, sc, rc), use, LAST_CHUNKS, first=first_ref)
    for cp in sent:
        cp.wait_send()


def last(at, h2, alpha, beta, w_out, w_first):
    return pl.pallas_call(
        last_kernel,
        out_shape=jax.ShapeDtypeStruct((B, D), BF16),
        in_specs=[vmem_spec(), vmem_spec(), any_spec(), any_spec(), any_spec(), vmem_spec()],
        out_specs=vmem_spec(),
        scratch_shapes=exchange_scratch(LAST_CHUNKS) + [pltpu.SMEM((2,), F32), pltpu.SMEM((2,), F32), pltpu.SemaphoreType.DMA((2,))],
        compiler_params=pltpu.CompilerParams(vmem_limit_bytes=16 * MIB, collective_id=1, has_side_effects=True),
        name="last",
    )(at, h2, alpha, beta, w_out, w_first)


def solution(mesh):
    row_spec = P('dp', None)
    cache_spec = P('dp', 'tp', None, None)
    in_specs = (row_spec, P('dp'), cache_spec, cache_spec, cache_spec, P(None), P(None, None, 'tp', None),
                P(None, 'tp', None), P('tp'), P('tp', None), P('tp', None, None), P(None),
                P(None, 'tp', None, None), P('tp', None, None), P(None), P(None))
    out_specs = (row_spec, cache_spec, cache_spec, cache_spec)

    def local_step(hidden, cache_len, lin_state, k_cache, v_cache, norm_first, w_qkv, w_gate, slopes, out_norm,
                   w_out_lin, norm_second, w_attn, w_out_attn, mix_alpha, mix_beta):
        def hbm(x):
            return pltpu.with_memory_space_constraint(x, pltpu.HBM)

        g1 = norm_first.reshape(NC, HD)
        g2 = norm_second.reshape(NC, HD)
        wa = jnp.transpose(w_attn, (0, 2, 1, 3)).reshape(WA_ROWS, HD)
        state_out, og, ss, h1 = lightning(hbm(hidden), hbm(g1), hbm(slopes), hbm(out_norm), hbm(lin_state), hbm(w_qkv), hbm(w_gate))
        w_last = hbm(w_out_attn.reshape(HL * HD, D))
        q, kn, vn, h2, kbuf, vbuf, w_first = middle(og, ss, h1, g2, hbm(mix_alpha), hbm(mix_beta), hbm(cache_len),
                                                    hbm(w_out_lin.reshape(HL * HD, D)), hbm(wa), hbm(k_cache),
                                                    hbm(v_cache), w_last)
        at, k_out, v_out = attention(cache_len, q, kn, vn, kbuf, vbuf)
        hidden_out = last(at, h2, hbm(mix_alpha), hbm(mix_beta), w_last, w_first)
        return hidden_out, state_out, k_out, v_out

    return jax.shard_map(local_step, mesh=mesh, in_specs=in_specs, out_specs=out_specs, check_vma=False)
```

```python
import functools
import math

import jax
import jax.numpy as jnp
from jax import lax
from jax.experimental import pallas as pl
from jax.experimental.pallas import tpu as pltpu
from jax.sharding import PartitionSpec as P

EPS = 1e-5
ROPE_BASE = 10000000.0
MESH = pl.DeviceIdType.MESH
F32 = jnp.float32
BF16 = jnp.bfloat16
MIB = 1024 * 1024

B = 32
D = 4096
HL = 8
HD = 128
KV = 2
GQ = 4
T = 512
NC = D // HD

DCH = 512
STEPS = D // DCH
LCH = DCH * HL // 2 // HD
RING = 3
EARLY = 24


def any_spec():
    return pl.BlockSpec(memory_space=pl.ANY)


def vmem_spec():
    return pl.BlockSpec(memory_space=pltpu.VMEM)


def smem_spec():
    return pl.BlockSpec(memory_space=pltpu.SMEM)


def dot(a, b):
    return jnp.dot(a, b, preferred_element_type=F32)


def lightning_kernel(hid_hbm, g1_hbm, slopes_hbm, onorm_hbm, state_ref, wqkv_ref, wgate_ref,
                     sout_ref, og_ref, ss_ref, h1_ref, hid_ref, g1_ref, onorm_ref, slopes_ref,
                     wbuf, gbuf, sbuf, hstack, ebuf, lbuf_a, lbuf_b, acc, kq_t, v_s, o_s, psem, wsem, ssem, osem):
    def w_copies(step, slot):
        rows = pl.ds(step * DCH, DCH)
        return (pltpu.make_async_copy(wqkv_ref.at[rows], wbuf.at[slot], wsem.at[slot, 0]),
                pltpu.make_async_copy(wgate_ref.at[rows], gbuf.at[slot], wsem.at[slot, 1]))

    def s_copy(b):
        return pltpu.make_async_copy(state_ref.at[b], sbuf.at[b], ssem.at[b])

    def o_copy(b):
        return pltpu.make_async_copy(sbuf.at[b], sout_ref.at[b], osem.at[b])

    small = [pltpu.make_async_copy(src, dst, psem.at[n]) for n, (src, dst) in enumerate(
        ((hid_hbm, hid_ref), (g1_hbm, g1_ref), (onorm_hbm, onorm_ref), (slopes_hbm, slopes_ref)))]
    for cp in small:
        cp.start()
    for i in range(RING):
        for cp in w_copies(i, i):
            cp.start()
    for cp in small:
        cp.wait()

    sq = jnp.zeros((B, HD), F32)
    for c in range(NC):
        x = hid_ref[:, c * HD:(c + 1) * HD].astype(F32)
        sq = sq + x * x
    inv = lax.rsqrt(jnp.sum(sq, axis=1, keepdims=True) / D + EPS)
    rr = lax.broadcasted_iota(jnp.int32, (HD, 256), 1)
    dd = lax.broadcasted_iota(jnp.int32, (HD, 256), 0)
    for c in range(NC):
        x = hid_ref[:, c * HD:(c + 1) * HD].astype(F32)
        h1 = (x * inv * g1_ref[c:c + 1, :]).astype(BF16)
        h1_ref[:, c * HD:(c + 1) * HD] = h1
        hstack[c * B:(c + 1) * B, :] = h1
    for n in range(4):
        spread = jnp.where(rr // 8 + 32 * n == dd, 1.0, 0.0).astype(BF16)
        for c in range(NC // 8):
            e = dot(hstack[c * 256:(c + 1) * 256, :], spread).astype(BF16)
            for k in range(8):
                for m in range(2):
                    ebuf[(c * 8 + k) * 8 + n * 2 + m] = e[k * B:(k + 1) * B, m * HD:(m + 1) * HD]

    acc[...] = jnp.zeros_like(acc)
    half = DCH * HL // 2
    lane = lax.broadcasted_iota(jnp.int32, (B, HD), 1) % 8

    def spread_heads(dst, part):
        for h in range(HL):
            keep = jnp.where(lane == h, 1.0, 0.0).astype(BF16)
            for q in range(LCH):
                dst[q, h * B:(h + 1) * B, :] = ebuf[part * LCH + q] * keep

    spread_heads(lbuf_a, 0)

    def step_fn(i, carry):
        slot = lax.rem(i, RING)

        @pl.when(i >= STEPS - RING)
        def _():
            for k in range(EARLY // RING):
                s_copy((i - (STEPS - RING)) * (EARLY // RING) + k).start()

        for cp in w_copies(i, slot):
            cp.wait()

        def product(left, part, pair):
            rows = slice(part * DCH // 2, (part + 1) * DCH // 2)
            second = wbuf[slot, rows, 1] if pair == 0 else gbuf[slot, rows]
            right = jnp.concatenate([wbuf[slot, rows, 2 * pair].reshape(half, HD), second.reshape(half, HD)], axis=1)
            return dot(left, right)

        spread_heads(lbuf_b, 2 * i + 1)
        left_a = jnp.concatenate([lbuf_a[q] for q in range(LCH)], axis=1)
        first = [product(left_a, 0, pair) for pair in range(2)]
        spread_heads(lbuf_a, jnp.minimum(2 * i + 2, 2 * STEPS - 1))
        left_b = jnp.concatenate([lbuf_b[q] for q in range(LCH)], axis=1)
        for pair in range(2):
            acc[pair] += first[pair] + product(left_b, 1, pair)

        @pl.when(i + RING < STEPS)
        def _():
            for cp in w_copies(i + RING, slot):
                cp.start()
        return carry

    lax.fori_loop(0, STEPS, step_fn, 0)
    for b in range(EARLY, B):
        s_copy(b).start()

    for h in range(HL):
        rows = slice(h * B, (h + 1) * B)
        q = jax.nn.silu(acc[0, rows, 0:HD]).astype(BF16)
        k = jax.nn.silu(acc[0, rows, HD:2 * HD]).astype(BF16)
        v = jax.nn.silu(acc[1, rows, 0:HD]).astype(BF16)
        qk = jnp.concatenate([k, q], axis=0).astype(F32)
        both = jnp.transpose(qk).astype(BF16)
        kq_t[h] = jnp.concatenate([both[:, 0:B], both[:, B:]], axis=0)
        v_s[h] = v.astype(F32)

    brow = lax.broadcasted_iota(jnp.int32, (B, 2 * HD), 0)
    bcol = lax.broadcasted_iota(jnp.int32, (B, 2 * HD), 1) // HD

    def row_fn(i, carry):
        for r in range(2):
            s_copy(2 * i + r).wait()
        pick = jnp.where(brow == 2 * i + bcol, 1.0, 0.0).astype(BF16)
        for h in range(HL):
            kq = dot(kq_t[h], pick)
            decay = jnp.exp(jnp.full((1, HD), -slopes_ref[h], F32))
            for r in range(2):
                b = 2 * i + r
                lanes = slice(r * HD, (r + 1) * HD)
                new = decay * sbuf[b, h] + kq[0:HD, lanes] * v_s[h, pl.ds(b, 1), :]
                sbuf[b, h] = new
                o_s[b, h:h + 1, :] = jnp.sum(kq[HD:, lanes] * new, axis=0, keepdims=True)
        for r in range(2):
            o_copy(2 * i + r).start()
        return carry

    lax.fori_loop(0, B // 2, row_fn, 0)

    ss = jnp.zeros((B, HD), F32)
    for h in range(HL):
        o = o_s[:, h, :]
        ss = ss + o * o
    ss = jnp.sum(ss, axis=1, keepdims=True)
    ss_ref[...] = jnp.broadcast_to(ss, (B, HD))
    inv_own = lax.rsqrt(ss / (HL * HD) + EPS)
    for h in range(HL):
        gate = jax.nn.sigmoid(acc[1, h * B:(h + 1) * B, HD:2 * HD])
        og_ref[:, h * HD:(h + 1) * HD] = (o_s[:, h, :] * inv_own * onorm_ref[h:h + 1, :] * gate).astype(BF16)

    def drain(b, carry):
        o_copy(b).wait()
        return carry

    lax.fori_loop(0, B, drain, 0)


def lightning(hidden, g1, slopes, out_norm, lin_state, w_qkv, w_gate):
    return pl.pallas_call(
        lightning_kernel,
        out_shape=[jax.ShapeDtypeStruct((B, HL, HD, HD), F32), jax.ShapeDtypeStruct((B, HL * HD), BF16),
                   jax.ShapeDtypeStruct((B, HD), F32), jax.ShapeDtypeStruct((B, D), BF16)],
        in_specs=[any_spec()] * 7,
        out_specs=[any_spec(), vmem_spec(), vmem_spec(), vmem_spec()],
        scratch_shapes=[
            pltpu.VMEM((B, D), BF16),
            pltpu.VMEM((NC, HD), F32),
            pltpu.VMEM((HL, HD), F32),
            pltpu.SMEM((HL,), F32),
            pltpu.VMEM((RING, DCH, 3, HL, HD), BF16),
            pltpu.VMEM((RING, DCH, HL, HD), BF16),
            pltpu.VMEM((B, HL, HD, HD), F32),
            pltpu.VMEM((NC * B, HD), BF16),
            pltpu.VMEM((2 * STEPS * LCH, B, HD), BF16),
            pltpu.VMEM((LCH, HL * B, HD), BF16),
            pltpu.VMEM((LCH, HL * B, HD), BF16),
            pltpu.VMEM((2, HL * B, 2 * HD), F32),
            pltpu.VMEM((HL, 2 * HD, B), BF16),
            pltpu.VMEM((HL, B, HD), F32),
            pltpu.VMEM((B, HL, HD), F32),
            pltpu.SemaphoreType.DMA((4,)),
            pltpu.SemaphoreType.DMA((RING, 2)),
            pltpu.SemaphoreType.DMA((B,)),
            pltpu.SemaphoreType.DMA((B,)),
        ],
        compiler_params=pltpu.CompilerParams(vmem_limit_bytes=40 * MIB),
        name="lightning",
    )(hidden, g1, slopes, out_norm, lin_state, w_qkv, w_gate)


MID_CHUNKS = 4
LAST_CHUNKS = 8


def peers():
    dp = lax.axis_index("dp")
    me = lax.axis_index("tp")
    core = lax.rem(me, 2)
    chip = me // 2
    mate = (dp, chip * 2 + (1 - core))
    across = (dp, (1 - chip) * 2 + core)
    return core, mate, across


def say_here(targets):
    barrier = pltpu.get_barrier_semaphore()
    for dev in targets:
        pl.semaphore_signal(barrier, inc=1, device_id=dev, device_id_type=MESH)


def await_peers(count):
    pl.semaphore_wait(pltpu.get_barrier_semaphore(), count)


def rcopy(src, dst, send, recv, dev):
    return pltpu.make_async_remote_copy(src_ref=src, dst_ref=dst, send_sem=send, recv_sem=recv,
                                        device_id=dev, device_id_type=MESH)


def exchange(left, wbuf, wwait, before_sends, pair_scale, mid_work, cross_scale, core, mate, across,
             a_send, a_recv, b_send, b_recv, total, sems, use, nch, first=None):
    sa, ra, sb, rb, sc, rc = sems
    width = D // 2 // nch
    both = nch - 1
    rest = (nch - 1, nch)
    own = (1 - core) * (nch + 1)
    other = core * (nch + 1)

    def product(at, j, owner):
        wwait(at, j)
        buf, at = (wbuf, at) if first is None or j > 0 else (first, 1 - owner)
        return jnp.concatenate([dot(left, buf[at, :, c:c + 2 * HD]) for c in range(0, width, 2 * HD)], axis=1)

    a_copies = [rcopy(a_send.at[j], a_recv.at[j], sa.at[j], ra.at[j], mate) for j in range(nch + 1)]
    b_copies = [rcopy(b_send.at[j], b_recv.at[j], sb.at[j], rb.at[j], across) for j in range(nch + 1)]
    c_places = [own + j for j in range(both)] + list(rest)
    c_copies = [rcopy(total.at[at], total.at[at], sc.at[j], rc.at[j], mate) for j, at in enumerate(c_places)]

    def send_across(j, scale):
        a_copies[j].wait_recv()
        b_send[j] = b_send[j] * scale[0] + a_recv[j] * scale[1] if scale else b_send[j] + a_recv[j]
        b_copies[j].start()

    def finish(j, scale):
        b_copies[j].wait_recv()
        total[c_places[j]] = b_send[j] * scale[0] + b_recv[j] * scale[1] if scale else b_send[j] + b_recv[j]
        c_copies[j].start()

    pair = None
    for j in range(both):
        a_send[j] = product(other + j, j, 1 - core)
        if j == 0:
            before_sends()
        a_copies[j].start()
        b_send[j] = product(own + j, j, core)
        if j == 1:
            pair = pair_scale()
        if j >= 1:
            send_across(j - 1, pair)

    @pl.when(core == 0)
    def _():
        for j in rest:
            a_send[j] = product(j, j, 1)
            a_copies[j].start()

    @pl.when(core == 1)
    def _():
        for j in rest:
            b_send[j] = product(j, j, 1)

    send_across(both - 1, pair)

    @pl.when(core == 1)
    def _():
        for j in rest:
            send_across(j, pair)

    mid_work()
    cross = cross_scale()
    for j in range(both):
        finish(j, cross)
        if j >= 1:
            c_copies[j - 1].wait_recv()
            use((j - 1, nch + j))

    @pl.when(core == 1)
    def _():
        for j in rest:
            finish(j, cross)

    c_copies[both - 1].wait_recv()
    use((both - 1, nch + both))

    @pl.when(core == 0)
    def _():
        for j in rest:
            c_copies[j].wait_recv()

    use(rest)

    def settle_sends():
        for cp in a_copies[:both] + b_copies[:both] + c_copies[:both]:
            cp.wait_send()

        @pl.when(core == 0)
        def _():
            for j in rest:
                a_copies[j].wait_send()

        @pl.when(core == 1)
        def _():
            for j in rest:
                b_copies[j].wait_send()
                c_copies[j].wait_send()

    return settle_sends


def exchange_scratch(nch):
    width = D // 2 // nch
    return [
        pltpu.VMEM((2 * nch, HL * HD, width), BF16),
        pltpu.VMEM((nch + 1, B, width), F32),
        pltpu.VMEM((nch + 1, B, width), F32),
        pltpu.VMEM((nch + 1, B, width), F32),
        pltpu.VMEM((nch + 1, B, width), F32),
        pltpu.VMEM((2 * nch, B, width), F32),
        pltpu.SemaphoreType.DMA((2 * nch,)),
        pltpu.SemaphoreType.DMA((nch + 1,)),
        pltpu.SemaphoreType.DMA((nch + 1,)),
        pltpu.SemaphoreType.DMA((nch + 1,)),
        pltpu.SemaphoreType.DMA((nch + 1,)),
        pltpu.SemaphoreType.DMA((nch + 1,)),
        pltpu.SemaphoreType.DMA((nch + 1,)),
    ]


def out_weights(w_ref, wbuf, wsem, core, nch, begin=0):
    width = D // 2 // nch

    def copy(at):
        cols = pl.ds(pl.multiple_of(at * width, width), width)
        return pltpu.make_async_copy(w_ref.at[:, cols], wbuf.at[at], wsem.at[at])

    def start():
        for j in range(begin, nch - 1):
            copy(core * (nch + 1) + j).start()
            copy((1 - core) * (nch + 1) + j).start()
        for at in (nch - 1, nch):
            copy(at).start()

    def wait(at, j):
        if j >= begin:
            copy(at).wait()

    return start, wait


WA_ROWS = D * KV * (GQ + 2)
WA_CH = 32
WA_STEP = WA_ROWS // WA_CH
NJ = KV * (GQ + 2)


def mid_kernel(og_ref, ss_ref, h1_ref, g2_ref, alpha_hbm, beta_hbm, len_hbm, wout_ref, wattn_ref,
               k_ref, v_ref, wnext_ref, q_ref, kn_ref, vn_ref, h2_ref, kbuf, vbuf, wnext,
               wbuf, a_send, a_recv, b_send, b_recv, total, wsem, sa, ra, sb, rb, sc, rc,
               wraw, wide, w2, ss_recv, ss_chip, alpha_ref, beta_ref, len_ref, wasem, ss_s, ss_r, csem, psem):
    core, mate, across = peers()
    say_here((mate, across))
    scalars = [pltpu.make_async_copy(src, dst, psem.at[n]) for n, (src, dst) in enumerate(
        ((alpha_hbm, alpha_ref), (beta_hbm, beta_ref), (len_hbm, len_ref)))]
    for cp in scalars:
        cp.start()
    start_w, wait_w = out_weights(wout_ref, wbuf, wsem, core, MID_CHUNKS)
    start_w()

    def wa_copy(i):
        return pltpu.make_async_copy(wattn_ref.at[pl.ds(i * WA_STEP, WA_STEP)], wraw.at[i], wasem.at[i])

    def wa_start(i, carry):
        wa_copy(i).start()
        return carry

    lax.fori_loop(0, WA_CH, wa_start, 0)
    caches = [pltpu.make_async_copy(k_ref, kbuf, csem.at[0]), pltpu.make_async_copy(v_ref, vbuf, csem.at[1])]
    caches += [pltpu.make_async_copy(wnext_ref.at[:, pl.ds(h * (LAST_CHUNKS + 1) * (D // 2 // LAST_CHUNKS), D // 2 // LAST_CHUNKS)], wnext.at[h], csem.at[2 + h]) for h in range(2)]
    for cp in caches:
        cp.start()
    ss_mate = rcopy(ss_ref, ss_recv.at[0], ss_s.at[0], ss_r.at[0], mate)
    ss_across = rcopy(ss_chip, ss_recv.at[1], ss_s.at[1], ss_r.at[1], across)

    def before_sends():
        await_peers(2)
        ss_mate.start()

    def root(total_sq, count):
        return jnp.minimum(jnp.sqrt(total_sq[:, 0:1] / count + EPS), 3e38)

    def pair_scale():
        ss_mate.wait_recv()
        both = ss_ref[...] + ss_recv[0]
        ss_chip[...] = both
        ss_across.start()
        inv = lax.rsqrt(both[:, 0:1] / (D // 2) + EPS)
        return root(ss_ref[...], D // 4) * inv, root(ss_recv[0], D // 4) * inv

    def cross_scale():
        for cp in scalars:
            cp.wait()
        ss_across.wait_recv()
        inv = lax.rsqrt((ss_chip[:, 0:1] + ss_recv[1, :, 0:1]) / D + EPS)
        return root(ss_chip[...], D // 2) * inv, root(ss_recv[1], D // 2) * inv

    def relayout():
        def body(i, carry):
            wa_copy(i).wait()
            wide[...] = wraw[i].astype(F32)
            for j in range(NJ):
                w2[j, pl.ds(pl.multiple_of(i * HD, HD), HD), :] = wide[pl.ds(j, HD, stride=NJ), :].astype(BF16)
            return carry
        lax.fori_loop(0, WA_CH, body, 0)

    squares = [jnp.zeros((B, HD), F32)]

    def use(chunks):
        wide_cols = D // 2 // MID_CHUNKS
        for at in chunks:
            for p in range(wide_cols // HD):
                cols = slice(at * wide_cols + p * HD, at * wide_cols + (p + 1) * HD)
                a1 = total[at, :, p * HD:(p + 1) * HD]
                m = (alpha_ref[0] * h1_ref[:, cols].astype(F32) + beta_ref[0] * a1).astype(BF16)
                h2_ref[:, cols] = m
                x = m.astype(F32)
                squares[0] = squares[0] + x * x

    settle_sends = exchange(og_ref[...], wbuf, wait_w, before_sends, pair_scale, relayout, cross_scale, core, mate, across,
                    a_send, a_recv, b_send, b_recv, total, (sa, ra, sb, rb, sc, rc), use, MID_CHUNKS)
    sq = squares[0]
    inv2 = lax.rsqrt(jnp.sum(sq, axis=1, keepdims=True) / D + EPS)
    for c in range(NC):
        m = h2_ref[:, c * HD:(c + 1) * HD].astype(F32)
        h2_ref[:, c * HD:(c + 1) * HD] = (m * inv2 * g2_ref[c:c + 1, :]).astype(BF16)

    pos = jnp.zeros((B, HD), F32)
    row_i = lax.broadcasted_iota(jnp.int32, (B, HD), 0)
    for b in range(B):
        pos = jnp.where(row_i == b, jnp.full((B, HD), len_ref[b]).astype(F32), pos)
    lane = lax.broadcasted_iota(jnp.int32, (B, HD), 1)
    freq = jnp.exp((lane % 32).astype(F32) * (-2.0 * math.log(ROPE_BASE) / 64))
    ang = pos * freq
    rot = lane < 64
    cosv = jnp.where(rot, jnp.cos(ang), 1.0)
    sinv = jnp.sin(ang)
    sin_lo = jnp.where(lane < 32, -sinv, 0.0)
    sin_hi = jnp.where((lane >= 32) & rot, sinv, 0.0)

    def turn(x):
        return x * cosv + pltpu.roll(x, HD - 32, 1) * sin_lo + pltpu.roll(x, 32, 1) * sin_hi

    h2 = h2_ref[...]
    for j in range(GQ + 2):
        w = jnp.concatenate([w2[2 * j], w2[2 * j + 1]], axis=1)
        pr = dot(h2, w)
        for kv in range(KV):
            x = pr[:, kv * HD:(kv + 1) * HD]
            if j < GQ:
                q_ref[pl.ds(kv * GQ + j, B, stride=8), :] = turn(x).astype(BF16).astype(F32)
            elif j == GQ:
                kn_ref[kv] = turn(x).astype(BF16).astype(F32)
            else:
                vn_ref[kv] = x.astype(BF16).astype(F32)
    for cp in caches:
        cp.wait()
    settle_sends()
    for cp in (ss_mate, ss_across):
        cp.wait_send()


def middle(og, ss, h1, g2, alpha, beta, cache_len, w_out, w_attn, k_cache, v_cache, w_next):
    return pl.pallas_call(
        mid_kernel,
        out_shape=[jax.ShapeDtypeStruct((B * 8, HD), F32), jax.ShapeDtypeStruct((KV, B, HD), F32),
                   jax.ShapeDtypeStruct((KV, B, HD), F32), jax.ShapeDtypeStruct((B, D), BF16),
                   pltpu.VMEM((B, KV, T, HD), BF16), pltpu.VMEM((B, KV, T, HD), BF16),
                   pltpu.VMEM((2, HL * HD, D // 2 // LAST_CHUNKS), BF16)],
        in_specs=[vmem_spec(), vmem_spec(), vmem_spec(), vmem_spec(), any_spec(), any_spec(), any_spec(),
                  any_spec(), any_spec(), any_spec(), any_spec(), any_spec()],
        out_specs=[vmem_spec()] * 7,
        scratch_shapes=exchange_scratch(MID_CHUNKS) + [
            pltpu.VMEM((WA_CH, WA_STEP, HD), BF16),
            pltpu.VMEM((WA_STEP, HD), F32),
            pltpu.VMEM((NJ, D, HD), BF16),
            pltpu.VMEM((2, B, HD), F32),
            pltpu.VMEM((B, HD), F32),
            pltpu.SMEM((2,), F32),
            pltpu.SMEM((2,), F32),
            pltpu.SMEM((B,), jnp.int32),
            pltpu.SemaphoreType.DMA((WA_CH,)),
            pltpu.SemaphoreType.DMA((2,)),
            pltpu.SemaphoreType.DMA((2,)),
            pltpu.SemaphoreType.DMA((4,)),
            pltpu.SemaphoreType.DMA((3,)),
        ],
        compiler_params=pltpu.CompilerParams(vmem_limit_bytes=35 * MIB, collective_id=0, has_side_effects=True),
        name="middle",
    )(og, ss, h1, g2, alpha, beta, cache_len, w_out, w_attn, k_cache, v_cache, w_next)


ROWS = 4
ROWS_MM = 8


def attention_kernel(len_ref, q_ref, kn_ref, vn_ref, kin_ref, vin_ref, at_ref, ko_ref, vo_ref, kbuf, vbuf, osem):
    def outs(b):
        return (pltpu.make_async_copy(kbuf.at[b], ko_ref.at[b], osem.at[0, b]),
                pltpu.make_async_copy(vbuf.at[b], vo_ref.at[b], osem.at[1, b]))

    row8 = lax.broadcasted_iota(jnp.int32, (8, HD), 0)
    row16 = lax.broadcasted_iota(jnp.int32, (16, HD), 0)
    tpos = lax.broadcasted_iota(jnp.int32, (8, T), 1)

    def insert(i, carry):
        rows = [i * ROWS + r for r in range(ROWS)]
        for b in rows:
            p = len_ref[b]
            base = pl.multiple_of((p // 16) * 16, 16)
            hit = row16 == p - base
            for kv in range(KV):
                for buf, new in ((kbuf, kn_ref), (vbuf, vn_ref)):
                    old = buf[b, kv, pl.ds(base, 16), :].astype(F32)
                    buf[b, kv, pl.ds(base, 16), :] = jnp.where(hit, new[kv, pl.ds(b, 1), :], old).astype(BF16)
        for b in rows:
            for cp in outs(b):
                cp.start()
        return carry

    lax.fori_loop(0, B // ROWS, insert, 0)

    def body(i, carry):
        rows = [i * ROWS_MM + r for r in range(ROWS_MM)]
        lens = [len_ref[b] for b in rows]
        scores = []
        for b, p in zip(rows, lens):
            q = q_ref[pl.ds(b * 8, 8), :]
            q2 = jnp.concatenate([jnp.where(row8 < 4, q, 0.0), jnp.where(row8 < 4, 0.0, q)], axis=1).astype(BF16)
            k2 = jnp.concatenate([kbuf[b, 0], kbuf[b, 1]], axis=1)
            s = lax.dot_general(q2, k2, (((1,), (1,)), ((), ())), preferred_element_type=F32) * HD ** -0.5
            scores.append(jnp.where(tpos <= p, s, -jnp.inf))
        tops = [jnp.max(s, axis=1, keepdims=True) for s in scores]
        es = [jnp.exp(s - m) for s, m in zip(scores, tops)]
        sums = [jnp.sum(e, axis=1, keepdims=True) for e in es]
        prs = [(e / z).astype(BF16) for e, z in zip(es, sums)]
        for b, pr in zip(rows, prs):
            o = dot(pr, jnp.concatenate([vbuf[b, 0], vbuf[b, 1]], axis=1))
            at_ref[pl.ds(b * 8, 8), :] = jnp.where(row8 < 4, o[:, 0:HD], o[:, HD:])
        return carry

    lax.fori_loop(0, B // ROWS_MM, body, 0)

    def drain(b, carry):
        for cp in outs(b):
            cp.wait()
        return carry

    lax.fori_loop(0, B, drain, 0)


def attention(cache_len, q, kn, vn, kbuf, vbuf):
    return pl.pallas_call(
        attention_kernel,
        out_shape=[jax.ShapeDtypeStruct((B * 8, HD), F32), pltpu.HBM((B, KV, T, HD), BF16),
                   pltpu.HBM((B, KV, T, HD), BF16), pltpu.VMEM((B, KV, T, HD), BF16), pltpu.VMEM((B, KV, T, HD), BF16)],
        in_specs=[smem_spec(), vmem_spec(), vmem_spec(), vmem_spec(), vmem_spec(), vmem_spec()],
        out_specs=[vmem_spec(), any_spec(), any_spec(), vmem_spec(), vmem_spec()],
        input_output_aliases={4: 3, 5: 4},
        scratch_shapes=[pltpu.SemaphoreType.DMA((2, B))],
        compiler_params=pltpu.CompilerParams(vmem_limit_bytes=4 * MIB),
        name="attention",
    )(cache_len, q, kn, vn, kbuf, vbuf)[:3]


def last_kernel(at_ref, h2_ref, alpha_hbm, beta_hbm, wout_ref, first_ref, out_ref,
                wbuf, a_send, a_recv, b_send, b_recv, total, wsem, sa, ra, sb, rb, sc, rc,
                alpha_ref, beta_ref, psem):
    core, mate, across = peers()
    say_here((mate, across))
    scalars = [pltpu.make_async_copy(alpha_hbm, alpha_ref, psem.at[0]), pltpu.make_async_copy(beta_hbm, beta_ref, psem.at[1])]
    for cp in scalars:
        cp.start()
    start_w, wait_w = out_weights(wout_ref, wbuf, wsem, core, LAST_CHUNKS, begin=1)
    start_w()
    left = jnp.concatenate([at_ref[pl.ds(j, B, stride=8), :].astype(BF16) for j in range(8)], axis=1)
    def settle():
        for cp in scalars:
            cp.wait()

    def use(chunks):
        for at in chunks:
            cols = slice(at * (D // 2 // LAST_CHUNKS), (at + 1) * (D // 2 // LAST_CHUNKS))
            out_ref[:, cols] = (alpha_ref[1] * h2_ref[:, cols].astype(F32) + beta_ref[1] * total[at]).astype(BF16)

    settle_sends = exchange(left, wbuf, wait_w, lambda: await_peers(2), lambda: None, settle, lambda: None, core, mate,
                    across, a_send, a_recv, b_send, b_recv, total, (sa, ra, sb, rb, sc, rc), use, LAST_CHUNKS, first=first_ref)
    settle_sends()


def last(at, h2, alpha, beta, w_out, w_first):
    return pl.pallas_call(
        last_kernel,
        out_shape=jax.ShapeDtypeStruct((B, D), BF16),
        in_specs=[vmem_spec(), vmem_spec(), any_spec(), any_spec(), any_spec(), vmem_spec()],
        out_specs=vmem_spec(),
        scratch_shapes=exchange_scratch(LAST_CHUNKS) + [pltpu.SMEM((2,), F32), pltpu.SMEM((2,), F32), pltpu.SemaphoreType.DMA((2,))],
        compiler_params=pltpu.CompilerParams(vmem_limit_bytes=16 * MIB, collective_id=1, has_side_effects=True),
        name="last",
    )(at, h2, alpha, beta, w_out, w_first)


def solution(mesh):
    row_spec = P('dp', None)
    cache_spec = P('dp', 'tp', None, None)
    in_specs = (row_spec, P('dp'), cache_spec, cache_spec, cache_spec, P(None), P(None, None, 'tp', None),
                P(None, 'tp', None), P('tp'), P('tp', None), P('tp', None, None), P(None),
                P(None, 'tp', None, None), P('tp', None, None), P(None), P(None))
    out_specs = (row_spec, cache_spec, cache_spec, cache_spec)

    def local_step(hidden, cache_len, lin_state, k_cache, v_cache, norm_first, w_qkv, w_gate, slopes, out_norm,
                   w_out_lin, norm_second, w_attn, w_out_attn, mix_alpha, mix_beta):
        def hbm(x):
            return pltpu.with_memory_space_constraint(x, pltpu.HBM)

        g1 = norm_first.reshape(NC, HD)
        g2 = norm_second.reshape(NC, HD)
        wa = jnp.transpose(w_attn, (0, 2, 1, 3)).reshape(WA_ROWS, HD)
        state_out, og, ss, h1 = lightning(hbm(hidden), hbm(g1), hbm(slopes), hbm(out_norm), hbm(lin_state), hbm(w_qkv), hbm(w_gate))
        w_last = hbm(w_out_attn.reshape(HL * HD, D))
        q, kn, vn, h2, kbuf, vbuf, w_first = middle(og, ss, h1, g2, hbm(mix_alpha), hbm(mix_beta), hbm(cache_len),
                                                    hbm(w_out_lin.reshape(HL * HD, D)), hbm(wa), hbm(k_cache),
                                                    hbm(v_cache), w_last)
        at, k_out, v_out = attention(cache_len, q, kn, vn, kbuf, vbuf)
        hidden_out = last(at, h2, hbm(mix_alpha), hbm(mix_beta), w_last, w_first)
        return hidden_out, state_out, k_out, v_out

    return jax.shard_map(local_step, mesh=mesh, in_specs=in_specs, out_specs=out_specs, check_vma=False)
```

```python
import functools
import math

import jax
import jax.numpy as jnp
from jax import lax
from jax.experimental import pallas as pl
from jax.experimental.pallas import tpu as pltpu
from jax.sharding import PartitionSpec as P

EPS = 1e-5
ROPE_BASE = 10000000.0
MESH = pl.DeviceIdType.MESH
F32 = jnp.float32
BF16 = jnp.bfloat16
MIB = 1024 * 1024

B = 32
D = 4096
HL = 8
HD = 128
KV = 2
GQ = 4
T = 512
NC = D // HD

DCH = 512
STEPS = D // DCH
LCH = DCH * HL // 2 // HD
RING = 3
EARLY = 30


def any_spec():
    return pl.BlockSpec(memory_space=pl.ANY)


def vmem_spec():
    return pl.BlockSpec(memory_space=pltpu.VMEM)


def smem_spec():
    return pl.BlockSpec(memory_space=pltpu.SMEM)


def dot(a, b):
    return jnp.dot(a, b, preferred_element_type=F32)


def lightning_kernel(hid_hbm, g1_hbm, slopes_hbm, onorm_hbm, state_ref, wqkv_ref, wgate_ref,
                     sout_ref, og_ref, ss_ref, h1_ref, hid_ref, g1_ref, onorm_ref, slopes_ref,
                     wbuf, gbuf, sbuf, hstack, ebuf, lbuf_a, lbuf_b, acc, kq_t, v_s, o_s, psem, wsem, ssem, osem):
    def w_copies(step, slot):
        rows = pl.ds(step * DCH, DCH)
        return (pltpu.make_async_copy(wqkv_ref.at[rows], wbuf.at[slot], wsem.at[slot, 0]),
                pltpu.make_async_copy(wgate_ref.at[rows], gbuf.at[slot], wsem.at[slot, 1]))

    def s_copy(b):
        return pltpu.make_async_copy(state_ref.at[b], sbuf.at[b], ssem.at[b])

    def o_copy(b):
        return pltpu.make_async_copy(sbuf.at[b], sout_ref.at[b], osem.at[b])

    small = [pltpu.make_async_copy(src, dst, psem.at[n]) for n, (src, dst) in enumerate(
        ((hid_hbm, hid_ref), (g1_hbm, g1_ref), (onorm_hbm, onorm_ref), (slopes_hbm, slopes_ref)))]
    for cp in small:
        cp.start()
    for i in range(RING):
        for cp in w_copies(i, i):
            cp.start()
    for cp in small:
        cp.wait()

    sq = jnp.zeros((B, HD), F32)
    for c in range(NC):
        x = hid_ref[:, c * HD:(c + 1) * HD].astype(F32)
        sq = sq + x * x
    inv = lax.rsqrt(jnp.sum(sq, axis=1, keepdims=True) / D + EPS)
    rr = lax.broadcasted_iota(jnp.int32, (HD, 256), 1)
    dd = lax.broadcasted_iota(jnp.int32, (HD, 256), 0)
    for c in range(NC):
        x = hid_ref[:, c * HD:(c + 1) * HD].astype(F32)
        h1 = (x * inv * g1_ref[c:c + 1, :]).astype(BF16)
        h1_ref[:, c * HD:(c + 1) * HD] = h1
        hstack[c * B:(c + 1) * B, :] = h1
    for n in range(4):
        spread = jnp.where(rr // 8 + 32 * n == dd, 1.0, 0.0).astype(BF16)
        for c in range(NC // 8):
            e = dot(hstack[c * 256:(c + 1) * 256, :], spread).astype(BF16)
            for k in range(8):
                for m in range(2):
                    ebuf[(c * 8 + k) * 8 + n * 2 + m] = e[k * B:(k + 1) * B, m * HD:(m + 1) * HD]

    acc[...] = jnp.zeros_like(acc)
    half = DCH * HL // 2
    lane = lax.broadcasted_iota(jnp.int32, (B, HD), 1) % 8

    def spread_heads(dst, part):
        for h in range(HL):
            keep = jnp.where(lane == h, 1.0, 0.0).astype(BF16)
            for q in range(LCH):
                dst[q, h * B:(h + 1) * B, :] = ebuf[part * LCH + q] * keep

    spread_heads(lbuf_a, 0)

    def step_fn(i, carry):
        slot = lax.rem(i, RING)

        @pl.when(i >= STEPS - RING)
        def _():
            for k in range(EARLY // RING):
                s_copy((i - (STEPS - RING)) * (EARLY // RING) + k).start()

        for cp in w_copies(i, slot):
            cp.wait()

        def product(left, part, pair):
            rows = slice(part * DCH // 2, (part + 1) * DCH // 2)
            second = wbuf[slot, rows, 1] if pair == 0 else gbuf[slot, rows]
            right = jnp.concatenate([wbuf[slot, rows, 2 * pair].reshape(half, HD), second.reshape(half, HD)], axis=1)
            return dot(left, right)

        spread_heads(lbuf_b, 2 * i + 1)
        left_a = jnp.concatenate([lbuf_a[q] for q in range(LCH)], axis=1)
        first = [product(left_a, 0, pair) for pair in range(2)]
        spread_heads(lbuf_a, jnp.minimum(2 * i + 2, 2 * STEPS - 1))
        left_b = jnp.concatenate([lbuf_b[q] for q in range(LCH)], axis=1)
        for pair in range(2):
            acc[pair] += first[pair] + product(left_b, 1, pair)

        @pl.when(i + RING < STEPS)
        def _():
            for cp in w_copies(i + RING, slot):
                cp.start()
        return carry

    lax.fori_loop(0, STEPS, step_fn, 0)
    for b in range(EARLY, B):
        s_copy(b).start()

    for h in range(HL):
        rows = slice(h * B, (h + 1) * B)
        q = jax.nn.silu(acc[0, rows, 0:HD]).astype(BF16)
        k = jax.nn.silu(acc[0, rows, HD:2 * HD]).astype(BF16)
        v = jax.nn.silu(acc[1, rows, 0:HD]).astype(BF16)
        qk = jnp.concatenate([k, q], axis=0).astype(F32)
        both = jnp.transpose(qk).astype(BF16)
        kq_t[h] = jnp.concatenate([both[:, 0:B], both[:, B:]], axis=0)
        v_s[h] = v.astype(F32)

    brow = lax.broadcasted_iota(jnp.int32, (B, 2 * HD), 0)
    bcol = lax.broadcasted_iota(jnp.int32, (B, 2 * HD), 1) // HD

    def row_fn(i, carry):
        for r in range(2):
            s_copy(2 * i + r).wait()
        pick = jnp.where(brow == 2 * i + bcol, 1.0, 0.0).astype(BF16)
        for h in range(HL):
            kq = dot(kq_t[h], pick)
            decay = jnp.exp(jnp.full((1, HD), -slopes_ref[h], F32))
            for r in range(2):
                b = 2 * i + r
                lanes = slice(r * HD, (r + 1) * HD)
                new = decay * sbuf[b, h] + kq[0:HD, lanes] * v_s[h, pl.ds(b, 1), :]
                sbuf[b, h] = new
                o_s[b, h:h + 1, :] = jnp.sum(kq[HD:, lanes] * new, axis=0, keepdims=True)
        for r in range(2):
            o_copy(2 * i + r).start()
        return carry

    lax.fori_loop(0, B // 2, row_fn, 0)

    ss = jnp.zeros((B, HD), F32)
    for h in range(HL):
        o = o_s[:, h, :]
        ss = ss + o * o
    ss = jnp.sum(ss, axis=1, keepdims=True)
    ss_ref[...] = jnp.broadcast_to(ss, (B, HD))
    inv_own = lax.rsqrt(ss / (HL * HD) + EPS)
    for h in range(HL):
        gate = jax.nn.sigmoid(acc[1, h * B:(h + 1) * B, HD:2 * HD])
        og_ref[:, h * HD:(h + 1) * HD] = (o_s[:, h, :] * inv_own * onorm_ref[h:h + 1, :] * gate).astype(BF16)

    def drain(b, carry):
        o_copy(b).wait()
        return carry

    lax.fori_loop(0, B, drain, 0)


def lightning(hidden, g1, slopes, out_norm, lin_state, w_qkv, w_gate):
    return pl.pallas_call(
        lightning_kernel,
        out_shape=[jax.ShapeDtypeStruct((B, HL, HD, HD), F32), jax.ShapeDtypeStruct((B, HL * HD), BF16),
                   jax.ShapeDtypeStruct((B, HD), F32), jax.ShapeDtypeStruct((B, D), BF16)],
        in_specs=[any_spec()] * 7,
        out_specs=[any_spec(), vmem_spec(), vmem_spec(), vmem_spec()],
        scratch_shapes=[
            pltpu.VMEM((B, D), BF16),
            pltpu.VMEM((NC, HD), F32),
            pltpu.VMEM((HL, HD), F32),
            pltpu.SMEM((HL,), F32),
            pltpu.VMEM((RING, DCH, 3, HL, HD), BF16),
            pltpu.VMEM((RING, DCH, HL, HD), BF16),
            pltpu.VMEM((B, HL, HD, HD), F32),
            pltpu.VMEM((NC * B, HD), BF16),
            pltpu.VMEM((2 * STEPS * LCH, B, HD), BF16),
            pltpu.VMEM((LCH, HL * B, HD), BF16),
            pltpu.VMEM((LCH, HL * B, HD), BF16),
            pltpu.VMEM((2, HL * B, 2 * HD), F32),
            pltpu.VMEM((HL, 2 * HD, B), BF16),
            pltpu.VMEM((HL, B, HD), F32),
            pltpu.VMEM((B, HL, HD), F32),
            pltpu.SemaphoreType.DMA((4,)),
            pltpu.SemaphoreType.DMA((RING, 2)),
            pltpu.SemaphoreType.DMA((B,)),
            pltpu.SemaphoreType.DMA((B,)),
        ],
        compiler_params=pltpu.CompilerParams(vmem_limit_bytes=40 * MIB),
        name="lightning",
    )(hidden, g1, slopes, out_norm, lin_state, w_qkv, w_gate)


MID_CHUNKS = 4
LAST_CHUNKS = 8


def peers():
    dp = lax.axis_index("dp")
    me = lax.axis_index("tp")
    core = lax.rem(me, 2)
    chip = me // 2
    mate = (dp, chip * 2 + (1 - core))
    across = (dp, (1 - chip) * 2 + core)
    return core, mate, across


def say_here(targets):
    barrier = pltpu.get_barrier_semaphore()
    for dev in targets:
        pl.semaphore_signal(barrier, inc=1, device_id=dev, device_id_type=MESH)


def await_peers(count):
    pl.semaphore_wait(pltpu.get_barrier_semaphore(), count)


def rcopy(src, dst, send, recv, dev):
    return pltpu.make_async_remote_copy(src_ref=src, dst_ref=dst, send_sem=send, recv_sem=recv,
                                        device_id=dev, device_id_type=MESH)


def exchange(left, wbuf, wwait, before_sends, pair_scale, mid_work, cross_scale, core, mate, across,
             a_send, a_recv, b_send, b_recv, total, sems, use, nch, first=None):
    sa, ra, sb, rb, sc, rc = sems
    width = D // 2 // nch
    both = nch - 1
    rest = (nch - 1, nch)
    own = (1 - core) * (nch + 1)
    other = core * (nch + 1)

    def product(at, j, owner):
        wwait(at, j)
        buf, at = (wbuf, at) if first is None or j > 0 else (first, 1 - owner)
        return jnp.concatenate([dot(left, buf[at, :, c:c + 2 * HD]) for c in range(0, width, 2 * HD)], axis=1)

    a_copies = [rcopy(a_send.at[j], a_recv.at[j], sa.at[j], ra.at[j], mate) for j in range(nch + 1)]
    b_copies = [rcopy(b_send.at[j], b_recv.at[j], sb.at[j], rb.at[j], across) for j in range(nch + 1)]
    c_places = [own + j for j in range(both)] + list(rest)
    c_copies = [rcopy(total.at[at], total.at[at], sc.at[j], rc.at[j], mate) for j, at in enumerate(c_places)]

    def send_across(j, scale):
        a_copies[j].wait_recv()
        b_send[j] = b_send[j] * scale[0] + a_recv[j] * scale[1] if scale else b_send[j] + a_recv[j]
        b_copies[j].start()

    def finish(j, scale):
        b_copies[j].wait_recv()
        total[c_places[j]] = b_send[j] * scale[0] + b_recv[j] * scale[1] if scale else b_send[j] + b_recv[j]
        c_copies[j].start()

    pair = None
    for j in range(both):
        a_send[j] = product(other + j, j, 1 - core)
        if j == 0:
            before_sends()
        a_copies[j].start()
        b_send[j] = product(own + j, j, core)
        if j == 1:
            pair = pair_scale()
        if j >= 1:
            send_across(j - 1, pair)

    @pl.when(core == 0)
    def _():
        for j in rest:
            a_send[j] = product(j, j, 1)
            a_copies[j].start()

    @pl.when(core == 1)
    def _():
        for j in rest:
            b_send[j] = product(j, j, 1)

    send_across(both - 1, pair)

    @pl.when(core == 1)
    def _():
        for j in rest:
            send_across(j, pair)

    mid_work()
    cross = cross_scale()
    for j in range(both):
        finish(j, cross)
        if j >= 1:
            c_copies[j - 1].wait_recv()
            use((j - 1, nch + j))

    @pl.when(core == 1)
    def _():
        for j in rest:
            finish(j, cross)

    c_copies[both - 1].wait_recv()
    use((both - 1, nch + both))

    @pl.when(core == 0)
    def _():
        for j in rest:
            c_copies[j].wait_recv()

    use(rest)

    def settle_sends():
        for cp in a_copies[:both] + b_copies[:both] + c_copies[:both]:
            cp.wait_send()

        @pl.when(core == 0)
        def _():
            for j in rest:
                a_copies[j].wait_send()

        @pl.when(core == 1)
        def _():
            for j in rest:
                b_copies[j].wait_send()
                c_copies[j].wait_send()

    return settle_sends


def exchange_scratch(nch):
    width = D // 2 // nch
    return [
        pltpu.VMEM((2 * nch, HL * HD, width), BF16),
        pltpu.VMEM((nch + 1, B, width), F32),
        pltpu.VMEM((nch + 1, B, width), F32),
        pltpu.VMEM((nch + 1, B, width), F32),
        pltpu.VMEM((nch + 1, B, width), F32),
        pltpu.VMEM((2 * nch, B, width), F32),
        pltpu.SemaphoreType.DMA((2 * nch,)),
        pltpu.SemaphoreType.DMA((nch + 1,)),
        pltpu.SemaphoreType.DMA((nch + 1,)),
        pltpu.SemaphoreType.DMA((nch + 1,)),
        pltpu.SemaphoreType.DMA((nch + 1,)),
        pltpu.SemaphoreType.DMA((nch + 1,)),
        pltpu.SemaphoreType.DMA((nch + 1,)),
    ]


def out_weights(w_ref, wbuf, wsem, core, nch, begin=0):
    width = D // 2 // nch

    def copy(at):
        cols = pl.ds(pl.multiple_of(at * width, width), width)
        return pltpu.make_async_copy(w_ref.at[:, cols], wbuf.at[at], wsem.at[at])

    def start():
        for j in range(begin, nch - 1):
            copy(core * (nch + 1) + j).start()
            copy((1 - core) * (nch + 1) + j).start()
        for at in (nch - 1, nch):
            copy(at).start()

    def wait(at, j):
        if j >= begin:
            copy(at).wait()

    return start, wait


WA_ROWS = D * KV * (GQ + 2)
WA_CH = 32
WA_STEP = WA_ROWS // WA_CH
NJ = KV * (GQ + 2)


def mid_kernel(og_ref, ss_ref, h1_ref, g2_ref, alpha_hbm, beta_hbm, len_hbm, wout_ref, wattn_ref,
               k_ref, v_ref, wnext_ref, q_ref, kn_ref, vn_ref, h2_ref, kbuf, vbuf, wnext,
               wbuf, a_send, a_recv, b_send, b_recv, total, wsem, sa, ra, sb, rb, sc, rc,
               wraw, wide, w2, ss_recv, ss_chip, alpha_ref, beta_ref, len_ref, wasem, ss_s, ss_r, csem, psem):
    core, mate, across = peers()
    say_here((mate, across))
    scalars = [pltpu.make_async_copy(src, dst, psem.at[n]) for n, (src, dst) in enumerate(
        ((alpha_hbm, alpha_ref), (beta_hbm, beta_ref), (len_hbm, len_ref)))]
    for cp in scalars:
        cp.start()
    start_w, wait_w = out_weights(wout_ref, wbuf, wsem, core, MID_CHUNKS)
    start_w()

    def wa_copy(i):
        return pltpu.make_async_copy(wattn_ref.at[pl.ds(i * WA_STEP, WA_STEP)], wraw.at[i], wasem.at[i])

    def wa_start(i, carry):
        wa_copy(i).start()
        return carry

    lax.fori_loop(0, WA_CH, wa_start, 0)
    caches = [pltpu.make_async_copy(k_ref, kbuf, csem.at[0]), pltpu.make_async_copy(v_ref, vbuf, csem.at[1])]
    caches += [pltpu.make_async_copy(wnext_ref.at[:, pl.ds(h * (LAST_CHUNKS + 1) * (D // 2 // LAST_CHUNKS), D // 2 // LAST_CHUNKS)], wnext.at[h], csem.at[2 + h]) for h in range(2)]
    for cp in caches:
        cp.start()
    ss_mate = rcopy(ss_ref, ss_recv.at[0], ss_s.at[0], ss_r.at[0], mate)
    ss_across = rcopy(ss_chip, ss_recv.at[1], ss_s.at[1], ss_r.at[1], across)

    def before_sends():
        await_peers(2)
        ss_mate.start()

    def root(total_sq, count):
        return jnp.minimum(jnp.sqrt(total_sq[:, 0:1] / count + EPS), 3e38)

    def pair_scale():
        ss_mate.wait_recv()
        both = ss_ref[...] + ss_recv[0]
        ss_chip[...] = both
        ss_across.start()
        inv = lax.rsqrt(both[:, 0:1] / (D // 2) + EPS)
        return root(ss_ref[...], D // 4) * inv, root(ss_recv[0], D // 4) * inv

    def cross_scale():
        for cp in scalars:
            cp.wait()
        ss_across.wait_recv()
        inv = lax.rsqrt((ss_chip[:, 0:1] + ss_recv[1, :, 0:1]) / D + EPS)
        return root(ss_chip[...], D // 2) * inv, root(ss_recv[1], D // 2) * inv

    def relayout():
        def body(i, carry):
            wa_copy(i).wait()
            wide[...] = wraw[i].astype(F32)
            for j in range(NJ):
                w2[j, pl.ds(pl.multiple_of(i * HD, HD), HD), :] = wide[pl.ds(j, HD, stride=NJ), :].astype(BF16)
            return carry
        lax.fori_loop(0, WA_CH, body, 0)

    squares = [jnp.zeros((B, HD), F32)]

    def use(chunks):
        wide_cols = D // 2 // MID_CHUNKS
        for at in chunks:
            for p in range(wide_cols // HD):
                cols = slice(at * wide_cols + p * HD, at * wide_cols + (p + 1) * HD)
                a1 = total[at, :, p * HD:(p + 1) * HD]
                m = (alpha_ref[0] * h1_ref[:, cols].astype(F32) + beta_ref[0] * a1).astype(BF16)
                h2_ref[:, cols] = m
                x = m.astype(F32)
                squares[0] = squares[0] + x * x

    settle_sends = exchange(og_ref[...], wbuf, wait_w, before_sends, pair_scale, relayout, cross_scale, core, mate, across,
                    a_send, a_recv, b_send, b_recv, total, (sa, ra, sb, rb, sc, rc), use, MID_CHUNKS)
    sq = squares[0]
    inv2 = lax.rsqrt(jnp.sum(sq, axis=1, keepdims=True) / D + EPS)
    for c in range(NC):
        m = h2_ref[:, c * HD:(c + 1) * HD].astype(F32)
        h2_ref[:, c * HD:(c + 1) * HD] = (m * inv2 * g2_ref[c:c + 1, :]).astype(BF16)

    pos = jnp.zeros((B, HD), F32)
    row_i = lax.broadcasted_iota(jnp.int32, (B, HD), 0)
    for b in range(B):
        pos = jnp.where(row_i == b, jnp.full((B, HD), len_ref[b]).astype(F32), pos)
    lane = lax.broadcasted_iota(jnp.int32, (B, HD), 1)
    freq = jnp.exp((lane % 32).astype(F32) * (-2.0 * math.log(ROPE_BASE) / 64))
    ang = pos * freq
    rot = lane < 64
    cosv = jnp.where(rot, jnp.cos(ang), 1.0)
    sinv = jnp.sin(ang)
    sin_lo = jnp.where(lane < 32, -sinv, 0.0)
    sin_hi = jnp.where((lane >= 32) & rot, sinv, 0.0)

    def turn(x):
        return x * cosv + pltpu.roll(x, HD - 32, 1) * sin_lo + pltpu.roll(x, 32, 1) * sin_hi

    h2 = h2_ref[...]
    for j in range(GQ + 2):
        w = jnp.concatenate([w2[2 * j], w2[2 * j + 1]], axis=1)
        pr = dot(h2, w)
        for kv in range(KV):
            x = pr[:, kv * HD:(kv + 1) * HD]
            if j < GQ:
                q_ref[pl.ds(kv * GQ + j, B, stride=8), :] = turn(x).astype(BF16).astype(F32)
            elif j == GQ:
                kn_ref[kv] = turn(x).astype(BF16).astype(F32)
            else:
                vn_ref[kv] = x.astype(BF16).astype(F32)
    for cp in caches:
        cp.wait()
    settle_sends()
    for cp in (ss_mate, ss_across):
        cp.wait_send()


def middle(og, ss, h1, g2, alpha, beta, cache_len, w_out, w_attn, k_cache, v_cache, w_next):
    return pl.pallas_call(
        mid_kernel,
        out_shape=[jax.ShapeDtypeStruct((B * 8, HD), F32), jax.ShapeDtypeStruct((KV, B, HD), F32),
                   jax.ShapeDtypeStruct((KV, B, HD), F32), jax.ShapeDtypeStruct((B, D), BF16),
                   pltpu.VMEM((B, KV, T, HD), BF16), pltpu.VMEM((B, KV, T, HD), BF16),
                   pltpu.VMEM((2, HL * HD, D // 2 // LAST_CHUNKS), BF16)],
        in_specs=[vmem_spec(), vmem_spec(), vmem_spec(), vmem_spec(), any_spec(), any_spec(), any_spec(),
                  any_spec(), any_spec(), any_spec(), any_spec(), any_spec()],
        out_specs=[vmem_spec()] * 7,
        scratch_shapes=exchange_scratch(MID_CHUNKS) + [
            pltpu.VMEM((WA_CH, WA_STEP, HD), BF16),
            pltpu.VMEM((WA_STEP, HD), F32),
            pltpu.VMEM((NJ, D, HD), BF16),
            pltpu.VMEM((2, B, HD), F32),
            pltpu.VMEM((B, HD), F32),
            pltpu.SMEM((2,), F32),
            pltpu.SMEM((2,), F32),
            pltpu.SMEM((B,), jnp.int32),
            pltpu.SemaphoreType.DMA((WA_CH,)),
            pltpu.SemaphoreType.DMA((2,)),
            pltpu.SemaphoreType.DMA((2,)),
            pltpu.SemaphoreType.DMA((4,)),
            pltpu.SemaphoreType.DMA((3,)),
        ],
        compiler_params=pltpu.CompilerParams(vmem_limit_bytes=35 * MIB, collective_id=0, has_side_effects=True),
        name="middle",
    )(og, ss, h1, g2, alpha, beta, cache_len, w_out, w_attn, k_cache, v_cache, w_next)


ROWS = 4
ROWS_MM = 16


def attention_kernel(len_ref, q_ref, kn_ref, vn_ref, kin_ref, vin_ref, at_ref, ko_ref, vo_ref, kbuf, vbuf, osem):
    def outs(b):
        return (pltpu.make_async_copy(kbuf.at[b], ko_ref.at[b], osem.at[0, b]),
                pltpu.make_async_copy(vbuf.at[b], vo_ref.at[b], osem.at[1, b]))

    row8 = lax.broadcasted_iota(jnp.int32, (8, HD), 0)
    row16 = lax.broadcasted_iota(jnp.int32, (16, HD), 0)
    tpos = lax.broadcasted_iota(jnp.int32, (8, T), 1)

    def insert(i, carry):
        rows = [i * ROWS + r for r in range(ROWS)]
        for b in rows:
            p = len_ref[b]
            base = pl.multiple_of((p // 16) * 16, 16)
            hit = row16 == p - base
            for kv in range(KV):
                for buf, new in ((kbuf, kn_ref), (vbuf, vn_ref)):
                    old = buf[b, kv, pl.ds(base, 16), :].astype(F32)
                    buf[b, kv, pl.ds(base, 16), :] = jnp.where(hit, new[kv, pl.ds(b, 1), :], old).astype(BF16)
        for b in rows:
            for cp in outs(b):
                cp.start()
        return carry

    lax.fori_loop(0, B // ROWS, insert, 0)

    def body(i, carry):
        rows = [i * ROWS_MM + r for r in range(ROWS_MM)]
        lens = [len_ref[b] for b in rows]
        scores = []
        for b, p in zip(rows, lens):
            q = q_ref[pl.ds(b * 8, 8), :]
            q2 = jnp.concatenate([jnp.where(row8 < 4, q, 0.0), jnp.where(row8 < 4, 0.0, q)], axis=1).astype(BF16)
            k2 = jnp.concatenate([kbuf[b, 0], kbuf[b, 1]], axis=1)
            s = lax.dot_general(q2, k2, (((1,), (1,)), ((), ())), preferred_element_type=F32) * HD ** -0.5
            scores.append(jnp.where(tpos <= p, s, -jnp.inf))
        tops = [jnp.max(s, axis=1, keepdims=True) for s in scores]
        es = [jnp.exp(s - m) for s, m in zip(scores, tops)]
        sums = [jnp.sum(e, axis=1, keepdims=True) for e in es]
        prs = [(e / z).astype(BF16) for e, z in zip(es, sums)]
        for b, pr in zip(rows, prs):
            o = dot(pr, jnp.concatenate([vbuf[b, 0], vbuf[b, 1]], axis=1))
            at_ref[pl.ds(b * 8, 8), :] = jnp.where(row8 < 4, o[:, 0:HD], o[:, HD:])
        return carry

    lax.fori_loop(0, B // ROWS_MM, body, 0)

    def drain(b, carry):
        for cp in outs(b):
            cp.wait()
        return carry

    lax.fori_loop(0, B, drain, 0)


def attention(cache_len, q, kn, vn, kbuf, vbuf):
    return pl.pallas_call(
        attention_kernel,
        out_shape=[jax.ShapeDtypeStruct((B * 8, HD), F32), pltpu.HBM((B, KV, T, HD), BF16),
                   pltpu.HBM((B, KV, T, HD), BF16), pltpu.VMEM((B, KV, T, HD), BF16), pltpu.VMEM((B, KV, T, HD), BF16)],
        in_specs=[smem_spec(), vmem_spec(), vmem_spec(), vmem_spec(), vmem_spec(), vmem_spec()],
        out_specs=[vmem_spec(), any_spec(), any_spec(), vmem_spec(), vmem_spec()],
        input_output_aliases={4: 3, 5: 4},
        scratch_shapes=[pltpu.SemaphoreType.DMA((2, B))],
        compiler_params=pltpu.CompilerParams(vmem_limit_bytes=4 * MIB),
        name="attention",
    )(cache_len, q, kn, vn, kbuf, vbuf)[:3]


def last_kernel(at_ref, h2_ref, alpha_hbm, beta_hbm, wout_ref, first_ref, out_ref,
                wbuf, a_send, a_recv, b_send, b_recv, total, wsem, sa, ra, sb, rb, sc, rc,
                alpha_ref, beta_ref, psem):
    core, mate, across = peers()
    say_here((mate, across))
    scalars = [pltpu.make_async_copy(alpha_hbm, alpha_ref, psem.at[0]), pltpu.make_async_copy(beta_hbm, beta_ref, psem.at[1])]
    for cp in scalars:
        cp.start()
    start_w, wait_w = out_weights(wout_ref, wbuf, wsem, core, LAST_CHUNKS, begin=1)
    start_w()
    left = jnp.concatenate([at_ref[pl.ds(j, B, stride=8), :].astype(BF16) for j in range(8)], axis=1)
    def settle():
        for cp in scalars:
            cp.wait()

    def use(chunks):
        for at in chunks:
            cols = slice(at * (D // 2 // LAST_CHUNKS), (at + 1) * (D // 2 // LAST_CHUNKS))
            out_ref[:, cols] = (alpha_ref[1] * h2_ref[:, cols].astype(F32) + beta_ref[1] * total[at]).astype(BF16)

    settle_sends = exchange(left, wbuf, wait_w, lambda: await_peers(2), lambda: None, settle, lambda: None, core, mate,
                    across, a_send, a_recv, b_send, b_recv, total, (sa, ra, sb, rb, sc, rc), use, LAST_CHUNKS, first=first_ref)
    settle_sends()


def last(at, h2, alpha, beta, w_out, w_first):
    return pl.pallas_call(
        last_kernel,
        out_shape=jax.ShapeDtypeStruct((B, D), BF16),
        in_specs=[vmem_spec(), vmem_spec(), any_spec(), any_spec(), any_spec(), vmem_spec()],
        out_specs=vmem_spec(),
        scratch_shapes=exchange_scratch(LAST_CHUNKS) + [pltpu.SMEM((2,), F32), pltpu.SMEM((2,), F32), pltpu.SemaphoreType.DMA((2,))],
        compiler_params=pltpu.CompilerParams(vmem_limit_bytes=16 * MIB, collective_id=1, has_side_effects=True),
        name="last",
    )(at, h2, alpha, beta, w_out, w_first)


def solution(mesh):
    row_spec = P('dp', None)
    cache_spec = P('dp', 'tp', None, None)
    in_specs = (row_spec, P('dp'), cache_spec, cache_spec, cache_spec, P(None), P(None, None, 'tp', None),
                P(None, 'tp', None), P('tp'), P('tp', None), P('tp', None, None), P(None),
                P(None, 'tp', None, None), P('tp', None, None), P(None), P(None))
    out_specs = (row_spec, cache_spec, cache_spec, cache_spec)

    def local_step(hidden, cache_len, lin_state, k_cache, v_cache, norm_first, w_qkv, w_gate, slopes, out_norm,
                   w_out_lin, norm_second, w_attn, w_out_attn, mix_alpha, mix_beta):
        def hbm(x):
            return pltpu.with_memory_space_constraint(x, pltpu.HBM)

        g1 = norm_first.reshape(NC, HD)
        g2 = norm_second.reshape(NC, HD)
        wa = jnp.transpose(w_attn, (0, 2, 1, 3)).reshape(WA_ROWS, HD)
        state_out, og, ss, h1 = lightning(hbm(hidden), hbm(g1), hbm(slopes), hbm(out_norm), hbm(lin_state), hbm(w_qkv), hbm(w_gate))
        w_last = hbm(w_out_attn.reshape(HL * HD, D))
        q, kn, vn, h2, kbuf, vbuf, w_first = middle(og, ss, h1, g2, hbm(mix_alpha), hbm(mix_beta), hbm(cache_len),
                                                    hbm(w_out_lin.reshape(HL * HD, D)), hbm(wa), hbm(k_cache),
                                                    hbm(v_cache), w_last)
        at, k_out, v_out = attention(cache_len, q, kn, vn, kbuf, vbuf)
        hidden_out = last(at, h2, hbm(mix_alpha), hbm(mix_beta), w_last, w_first)
        return hidden_out, state_out, k_out, v_out

    return jax.shard_map(local_step, mesh=mesh, in_specs=in_specs, out_specs=out_specs, check_vma=False)
```
